16 devices in a mesh: dp: 2 (over y, z), tp: 8 (over x, core).
Axes of the slice: x: 4, y: 2, z: 1, core: 2. Of those that a mesh axis runs over, the one named last changes fastest.
The devices are a block of a 4x4x8 slice.
Arguments:
- queries: bfloat16 [256, 256], P(('dp', 'tp')), parts along dimension 0
- w_first: bfloat16 [256, 1024], replicated
- w_second: bfloat16 [1024, 256], replicated
- catalogue: bfloat16 [262144, 256], P('tp')
- log_q: float32 [262144], P('tp')
- labels: int32 [256], P(('dp', 'tp')), parts along dimension 0
Outputs:
- output 1: float32 [2], P('dp'), parts along dimension 0
- output 2: bfloat16 [524288, 256], P(('dp', 'tp')), parts along dimension 0
- output 3: bfloat16 [512, 1024], P('dp'), parts along dimension 0
- output 4: bfloat16 [2048, 256], P('dp'), parts along dimension 0
There are 2 independent parts. The reference program is written for one: setup_inputs(seed, part) draws one part's arguments, and reference() takes and returns one part's arrays. A program takes and returns all parts, laid end to end along the dimension named above; an argument that names none is the same for every part.
All inputs are finite; a program needn't handle non-finite values.
Results may differ from the reference program's by a relative error of at most 0.00349722.
Values are sent between devices in bfloat16 or wider.
A program may use at most 768 MiB of HBM per device.

```python
import math
import jax
import jax.numpy as jnp
from jax import lax

QUERIES = 128
ROW_BLOCK = 16
IN_DIM = 256
HID_DIM = 1024
EMB_DIM = 256
NUM_ITEMS = 262144


def setup_inputs(seed: int = 0, part: int = 0) -> dict:
    base_key = jax.random.key(seed)
    shared_keys = jax.random.split(base_key, 4)
    part_keys = jax.random.split(jax.random.fold_in(base_key, part), 2)
    queries = jax.random.normal(part_keys[0], (QUERIES, IN_DIM), jnp.float32).astype(jnp.bfloat16)
    w_first = (jax.random.normal(shared_keys[0], (IN_DIM, HID_DIM), jnp.float32) * (1.0 / IN_DIM) ** 0.5).astype(jnp.bfloat16)
    w_second = (jax.random.normal(shared_keys[1], (HID_DIM, EMB_DIM), jnp.float32) * (2.0 / HID_DIM) ** 0.5).astype(jnp.bfloat16)
    catalogue = (jax.random.normal(shared_keys[2], (NUM_ITEMS, EMB_DIM), jnp.float32) * (36.0 / EMB_DIM) ** 0.5).astype(jnp.bfloat16)
    log_q = jax.random.normal(shared_keys[3], (NUM_ITEMS,), jnp.float32) - math.log(NUM_ITEMS)
    labels = jax.random.randint(part_keys[1], (QUERIES,), 0, NUM_ITEMS, jnp.int32)
    return {"queries": queries, "w_first": w_first, "w_second": w_second, "catalogue": catalogue, "log_q": log_q, "labels": labels}


def reference(queries, w_first, w_second, catalogue, log_q, labels):
    pre_act = jnp.dot(queries, w_first, preferred_element_type=jnp.float32)
    hidden = jnp.maximum(pre_act, 0.0).astype(jnp.bfloat16)
    query_emb = jnp.dot(hidden, w_second, preferred_element_type=jnp.float32).astype(jnp.bfloat16)
    num_blocks = QUERIES // ROW_BLOCK
    item_ids = jnp.arange(NUM_ITEMS, dtype=jnp.int32)

    def block_step(grad_items, block_in):
        block_rows, row_labels = block_in
        logits = jnp.dot(block_rows, catalogue.T, preferred_element_type=jnp.float32) - log_q[None, :]
        row_max = jnp.max(logits, axis=1, keepdims=True)
        exp_all = jnp.exp(logits - row_max)
        sum_exp = jnp.sum(exp_all, axis=1, keepdims=True)
        label_hit = item_ids[None, :] == row_labels[:, None]
        target = jnp.sum(jnp.where(label_hit, logits, 0.0), axis=1)
        losses = row_max[:, 0] + jnp.log(sum_exp[:, 0]) - target
        soft_prob = exp_all / sum_exp
        grad_logits = (jnp.where(label_hit, soft_prob - 1.0, soft_prob) / QUERIES).astype(jnp.bfloat16)
        grad_items = grad_items + jnp.dot(grad_logits.T, block_rows, preferred_element_type=jnp.float32)
        grad_rows = jnp.dot(grad_logits, catalogue, preferred_element_type=jnp.float32)
        return grad_items, (losses, grad_rows)

    init_items = jnp.zeros((NUM_ITEMS, EMB_DIM), jnp.float32)
    grad_items, (losses, grad_rows) = lax.scan(block_step, init_items, (query_emb.reshape(num_blocks, ROW_BLOCK, EMB_DIM), labels.reshape(num_blocks, ROW_BLOCK)))
    mean_loss = jnp.mean(losses).reshape(1)
    grad_emb = grad_rows.reshape(QUERIES, EMB_DIM).astype(jnp.bfloat16)
    grad_second = jnp.dot(hidden.T, grad_emb, preferred_element_type=jnp.float32).astype(jnp.bfloat16)
    grad_hidden = jnp.dot(grad_emb, w_second.T, preferred_element_type=jnp.float32)
    grad_pre = jnp.where(pre_act > 0.0, grad_hidden, 0.0).astype(jnp.bfloat16)
    grad_first = jnp.dot(queries.T, grad_pre, preferred_element_type=jnp.float32).astype(jnp.bfloat16)
    return mean_loss, grad_items.astype(jnp.bfloat16), grad_first, grad_second
```

```python
import functools

import jax
import jax.numpy as jnp
from jax import lax
from jax.experimental import pallas as pl
from jax.experimental.pallas import tpu as pltpu
from jax.sharding import PartitionSpec as P

F32, BF16 = jnp.float32, jnp.bfloat16
MESH = pl.DeviceIdType.MESH
LANES = 128
FIRST_TILE = 4096
SECOND_TILE = 4096
LOAD_TILE = 2048
OUT_TILE = 2048
OUT_SLOTS = 4
LOWEST = -3.0e38


def dot(a, b, contract):
    return lax.dot_general(a, b, ((contract[:1], contract[1:]), ((), ())), preferred_element_type=F32)


def loss_kernel(n, q_hbm, w1_hbm, w2_hbm, cat_hbm, lq_hbm, labels,
                g_ref, x_ref, dx_ref, h_ref, a_ref, q_ref, w2_ref, loss_ref,
                cat, ez, lq, w1, lab, d, m_run, s_run, t_run, m_hist, stats, part, pieces,
                load_sem, cat_sem, send_sem, q_sem, lab_sem, stat_sem, part_sem, dx_sem):
    me = lax.axis_index("tp")
    own = q_hbm.shape[0]
    rows = own * n
    items = cat_hbm.shape[0]
    my_rows = pl.ds(pl.multiple_of(me * own, own), own)

    q_load = pltpu.make_async_copy(q_hbm, q_ref.at[my_rows], load_sem.at[0])
    w1_load = pltpu.make_async_copy(w1_hbm, w1, load_sem.at[1])
    w2_load = pltpu.make_async_copy(w2_hbm, w2_ref, load_sem.at[2])
    lq_load = pltpu.make_async_copy(lq_hbm, lq, load_sem.at[3])
    q_load.start()
    barrier = pltpu.get_barrier_semaphore()
    peers = [lax.rem(me + k, n) for k in range(1, n)]
    for p in peers:
        pl.semaphore_signal(barrier, inc=1, device_id={"tp": p}, device_id_type=MESH)
    w1_load.start()
    w2_load.start()
    lq_load.start()
    for j in range(items // LOAD_TILE):
        part_rows = pl.ds(j * LOAD_TILE, LOAD_TILE)
        pltpu.make_async_copy(cat_hbm.at[part_rows], cat.at[part_rows], cat_sem.at[j]).start()
    for r in range(own):
        lab[pl.ds(me * own + r, 1), :] = jnp.full((1, LANES), labels[r], jnp.int32)
    pl.semaphore_wait(barrier, n - 1)

    def exchange(src, dst, stage, recv_sem):
        copies = []
        for k, p in enumerate(peers):
            copy = pltpu.make_async_remote_copy(
                src_ref=src(p), dst_ref=dst, send_sem=send_sem.at[stage, k], recv_sem=recv_sem.at[me],
                device_id={"tp": p}, device_id_type=MESH)
            copy.start()
            copies.append(copy)
        return copies

    def arrive(dst_of, recv_sem):
        for p in peers:
            ref = dst_of(p)
            pltpu.make_async_copy(ref, ref, recv_sem.at[p]).wait()

    def rows_of(p):
        return pl.ds(pl.multiple_of(p * own, own), own)

    lab_sends = exchange(lambda p: lab.at[my_rows], lab.at[my_rows], 0, lab_sem)
    q_load.wait()
    q_sends = exchange(lambda p: q_ref.at[my_rows], q_ref.at[my_rows], 1, q_sem)
    m_run[...] = jnp.full(m_run.shape, LOWEST, F32)
    s_run[...] = jnp.zeros(s_run.shape, F32)
    t_run[...] = jnp.zeros(t_run.shape, F32)
    w1_load.wait()
    w2_load.wait()
    lq_load.wait()
    arrive(lambda p: lab.at[rows_of(p)], lab_sem)
    d[...] = lab[...] - me * items - lax.broadcasted_iota(jnp.int32, d.shape, 1)
    arrive(lambda p: q_ref.at[rows_of(p)], q_sem)

    a = dot(q_ref[...], w1[...], (1, 0))
    a_ref[...] = a
    h_ref[...] = jnp.maximum(a, 0.0).astype(BF16)
    x_ref[...] = dot(h_ref[...], w2_ref[...], (1, 0)).astype(BF16)

    def first_pass(i, carry):
        for j in range(FIRST_TILE // LOAD_TILE):
            k = i * (FIRST_TILE // LOAD_TILE) + j
            part_rows = pl.ds(pl.multiple_of(k * LOAD_TILE, LOAD_TILE), LOAD_TILE)
            pltpu.make_async_copy(cat_hbm.at[part_rows], cat.at[part_rows], cat_sem.at[k]).wait()
        base = pl.multiple_of(i * FIRST_TILE, FIRST_TILE)
        z = dot(x_ref[...], cat[pl.ds(base, FIRST_TILE), :], (1, 1)) - lq[:, pl.ds(base, FIRST_TILE)]
        m_old = m_run[...]
        m = m_old
        for c in range(FIRST_TILE // LANES):
            m = jnp.maximum(m, z[:, c * LANES:(c + 1) * LANES])
        s = s_run[...] * jnp.exp(m_old - m)
        t = t_run[...]
        dd = d[...]
        for c in range(FIRST_TILE // LANES):
            zc = z[:, c * LANES:(c + 1) * LANES]
            e = jnp.exp(zc - m)
            s = s + e
            t = jnp.where(dd == base + c * LANES, zc, t)
            ez[:, pl.ds(pl.multiple_of(base + c * LANES, LANES), LANES)] = e
        m_run[...] = m
        m_hist[i] = m
        s_run[...] = s
        t_run[...] = t
        return carry

    lax.fori_loop(0, items // FIRST_TILE, first_pass, 0)

    m_t = m_run[...].T
    m_row = jnp.max(m_t, axis=0, keepdims=True)
    s_row = jnp.sum(s_run[...].T * jnp.exp(m_t - m_row), axis=0, keepdims=True)
    t_row = jnp.sum(t_run[...].T, axis=0, keepdims=True)
    sub = lax.broadcasted_iota(jnp.int32, (8, LANES), 0)
    stats[me] = jnp.where(sub == 0, m_row, jnp.where(sub == 1, s_row, t_row))
    stat_sends = exchange(lambda p: stats.at[me], stats.at[me], 2, stat_sem)
    arrive(lambda p: stats.at[p], stat_sem)
    big = stats[0, 0:1, :]
    for p in range(1, n):
        big = jnp.maximum(big, stats[p, 0:1, :])
    total = jnp.zeros_like(big)
    target = jnp.zeros_like(big)
    for p in range(n):
        total = total + stats[p, 1:2, :] * jnp.exp(stats[p, 0:1, :] - big)
        target = target + stats[p, 2:3, :]
    loss_ref[...] = jnp.sum(big + jnp.log(total) - target, axis=1, keepdims=True) / rows
    big_col = jnp.broadcast_to(big, (rows, LANES)).T
    inv_col = jnp.broadcast_to(1.0 / (total * rows), (rows, LANES)).T

    part[...] = jnp.zeros(part.shape, F32)

    def second_pass(i, carry):
        base = pl.multiple_of(i * SECOND_TILE, SECOND_TILE)
        dd = d[...]
        for f in range(SECOND_TILE // FIRST_TILE):
            scale = jnp.exp(m_hist[i * (SECOND_TILE // FIRST_TILE) + f] - big_col) * inv_col
            for c in range(f * FIRST_TILE // LANES, (f + 1) * FIRST_TILE // LANES):
                cols = pl.ds(pl.multiple_of(base + c * LANES, LANES), LANES)
                g = ez[:, cols] * scale
                g = g - jnp.where(dd == base + c * LANES, 1.0 / rows, 0.0)
                g_ref[:, cols] = g.astype(BF16)
        part[...] += dot(g_ref[:, pl.ds(base, SECOND_TILE)], cat[pl.ds(base, SECOND_TILE), :], (1, 0))
        return carry

    lax.fori_loop(0, items // SECOND_TILE, second_pass, 0)

    part_sends = exchange(lambda p: part.at[rows_of(p)], pieces.at[me], 3, part_sem)
    pieces[me] = part[my_rows, :]
    arrive(lambda p: pieces.at[p], part_sem)
    acc = pieces[0]
    for p in range(1, n):
        acc = acc + pieces[p]
    dx_ref[my_rows, :] = acc.astype(BF16)
    dx_sends = exchange(lambda p: dx_ref.at[my_rows], dx_ref.at[my_rows], 4, dx_sem)
    arrive(lambda p: dx_ref.at[rows_of(p)], dx_sem)
    for copy in lab_sends + q_sends + stat_sends + part_sends + dx_sends:
        copy.wait_send()


def grad_kernel(g_ref, x_ref, dx_ref, h_ref, a_ref, q_ref, w2_ref, loss_ref,
                loss_hbm, de_hbm, dw1_hbm, dw2_hbm, stage, dw1, dw2, out_sem, sem):
    items = de_hbm.shape[0]
    steps = items // OUT_TILE
    pltpu.make_async_copy(loss_ref, loss_hbm, sem.at[0]).start()

    def out_copy(i, slot):
        at = pl.ds(pl.multiple_of(i * OUT_TILE, OUT_TILE), OUT_TILE)
        return pltpu.make_async_copy(stage.at[slot], de_hbm.at[at], out_sem.at[slot])

    def step(i, carry):
        slot = lax.rem(i, OUT_SLOTS)

        @pl.when(i >= OUT_SLOTS)
        def _():
            out_copy(i - OUT_SLOTS, slot).wait()

        base = pl.multiple_of(i * OUT_TILE, OUT_TILE)
        stage[slot] = dot(g_ref[:, pl.ds(base, OUT_TILE)], x_ref[...], (0, 0)).astype(BF16)
        out_copy(i, slot).start()
        return carry

    lax.fori_loop(0, OUT_SLOTS, step, 0)
    dx = dx_ref[...]
    dw2[...] = dot(h_ref[...], dx, (0, 0)).astype(BF16)
    pltpu.make_async_copy(dw2, dw2_hbm, sem.at[2]).start()
    dh = dot(dx, w2_ref[...], (1, 1))
    da = jnp.where(a_ref[...] > 0.0, dh, 0.0).astype(BF16)
    dw1[...] = dot(q_ref[...], da, (0, 0)).astype(BF16)
    pltpu.make_async_copy(dw1, dw1_hbm, sem.at[1]).start()
    lax.fori_loop(OUT_SLOTS, steps, step, 0)
    for i in range(steps - OUT_SLOTS, steps):
        out_copy(i, i % OUT_SLOTS).wait()
    pltpu.make_async_copy(loss_ref, loss_hbm, sem.at[0]).wait()
    pltpu.make_async_copy(dw1, dw1_hbm, sem.at[1]).wait()
    pltpu.make_async_copy(dw2, dw2_hbm, sem.at[2]).wait()


def solution(mesh):
    n = mesh.shape["tp"]

    def local_step(queries, w_first, w_second, catalogue, log_q, labels):
        own, d_in = queries.shape
        hid, emb = w_second.shape
        items = catalogue.shape[0]
        rows = own * n
        hbm = pl.BlockSpec(memory_space=pl.ANY)
        vmem = pl.BlockSpec(memory_space=pltpu.VMEM)
        dma = pltpu.SemaphoreType.DMA
        held = pl.pallas_call(
            functools.partial(loss_kernel, n),
            name="loss_kernel",
            out_shape=[
                pltpu.VMEM((rows, items), BF16),
                pltpu.VMEM((rows, emb), BF16),
                pltpu.VMEM((rows, emb), BF16),
                pltpu.VMEM((rows, hid), BF16),
                pltpu.VMEM((rows, hid), F32),
                pltpu.VMEM((rows, d_in), BF16),
                pltpu.VMEM((hid, emb), BF16),
                pltpu.VMEM((1, 1), F32),
            ],
            in_specs=[hbm] * 5 + [pl.BlockSpec(memory_space=pltpu.SMEM)],
            out_specs=[vmem] * 8,
            scratch_shapes=[
                pltpu.VMEM((items, emb), BF16),
                pltpu.VMEM((rows, items), F32),
                pltpu.VMEM((1, items), F32),
                pltpu.VMEM((d_in, hid), BF16),
                pltpu.VMEM((rows, LANES), jnp.int32),
                pltpu.VMEM((rows, LANES), jnp.int32),
                pltpu.VMEM((rows, LANES), F32),
                pltpu.VMEM((rows, LANES), F32),
                pltpu.VMEM((rows, LANES), F32),
                pltpu.VMEM((items // FIRST_TILE, rows, LANES), F32),
                pltpu.VMEM((n, 8, LANES), F32),
                pltpu.VMEM((rows, emb), F32),
                pltpu.VMEM((n, own, emb), F32),
                dma((4,)),
                dma((items // LOAD_TILE,)),
                dma((5, n - 1)),
                dma((n,)),
                dma((n,)),
                dma((n,)),
                dma((n,)),
                dma((n,)),
            ],
            compiler_params=pltpu.CompilerParams(collective_id=0, has_side_effects=True, vmem_limit_bytes=46 << 20),
        )(queries, w_first, w_second, catalogue, log_q.reshape(1, items), labels)
        loss, grad_items, grad_first, grad_second = pl.pallas_call(
            grad_kernel,
            name="grad_kernel",
            out_shape=[
                jax.ShapeDtypeStruct((1, 1), F32),
                jax.ShapeDtypeStruct((items, emb), BF16),
                jax.ShapeDtypeStruct((d_in, hid), BF16),
                jax.ShapeDtypeStruct((hid, emb), BF16),
            ],
            in_specs=[vmem] * 8,
            out_specs=[hbm] * 4,
            scratch_shapes=[
                pltpu.VMEM((OUT_SLOTS, OUT_TILE, emb), BF16),
                pltpu.VMEM((d_in, hid), BF16),
                pltpu.VMEM((hid, emb), BF16),
                dma((OUT_SLOTS,)),
                dma((3,)),
            ],
            compiler_params=pltpu.CompilerParams(vmem_limit_bytes=40 << 20),
        )(*held)
        return loss.reshape(1), grad_items, grad_first, grad_second

    row_spec = P(("dp", "tp"), None)
    return jax.shard_map(
        local_step, mesh=mesh,
        in_specs=(row_spec, P(None, None), P(None, None), P("tp", None), P("tp"), P(("dp", "tp"))),
        out_specs=(P("dp"), row_spec, P("dp", None), P("dp", None)), check_vma=False)
```

```python
import functools

import jax
import jax.numpy as jnp
from jax import lax
from jax.experimental import pallas as pl
from jax.experimental.pallas import tpu as pltpu
from jax.sharding import PartitionSpec as P

F32, BF16 = jnp.float32, jnp.bfloat16
MESH = pl.DeviceIdType.MESH
LANES = 128
TILE = 4096
DOT_TILE = 1024
GROUP = 32
SECOND_TILE = 8192
LOAD_TILE = 2048
OUT_TILE = 2048
OUT_SLOTS = 4
LOWEST = -3.0e38


def dot(a, b, contract):
    return lax.dot_general(a, b, ((contract[:1], contract[1:]), ((), ())), preferred_element_type=F32)


def loss_kernel(n, q_hbm, w1_hbm, w2_hbm, cat_hbm, lq_hbm, lab_hbm,
                g_ref, x_ref, dx_ref, h_ref, a_ref, q_ref, w2_ref, loss_ref,
                cat, ez, z_even, z_odd, lq, w1, labels, lab, d, m_run, s_run, t_run, m_hist, stats, part, pieces,
                load_sem, cat_sem, send_sem, q_sem, lab_sem, stat_sem, part_sem, dx_sem):
    me = lax.axis_index("tp")
    own = q_hbm.shape[0]
    rows = own * n
    items = cat_hbm.shape[0]
    tiles = items // TILE
    chunks = TILE // LANES
    my_rows = pl.ds(pl.multiple_of(me * own, own), own)

    q_load = pltpu.make_async_copy(q_hbm, q_ref.at[my_rows], load_sem.at[0])
    w1_load = pltpu.make_async_copy(w1_hbm, w1, load_sem.at[1])
    w2_load = pltpu.make_async_copy(w2_hbm, w2_ref, load_sem.at[2])
    lq_load = pltpu.make_async_copy(lq_hbm, lq, load_sem.at[3])
    lab_load = pltpu.make_async_copy(lab_hbm, labels, load_sem.at[4])
    barrier = pltpu.get_barrier_semaphore()
    peers = [lax.rem(me + k, n) for k in range(1, n)]
    for p in peers:
        pl.semaphore_signal(barrier, inc=1, device_id={"tp": p}, device_id_type=MESH)
    for load in (q_load, lab_load, w1_load, w2_load, lq_load):
        load.start()
    lab_load.wait()
    for r in range(own):
        lab[pl.ds(me * own + r, 1), :] = jnp.full((1, LANES), labels[r], jnp.int32)
    with jax.named_scope("wload"):
        w1_load.wait()
        w2_load.wait()
        lq_load.wait()

    def cat_copy(k):
        part_rows = pl.ds(pl.multiple_of(k * LOAD_TILE, LOAD_TILE), LOAD_TILE)
        return pltpu.make_async_copy(cat_hbm.at[part_rows], cat.at[part_rows], cat_sem.at[k])

    for k in range(items // LOAD_TILE):
        cat_copy(k).start()
    q_load.wait()
    with jax.named_scope("bar"):
        pl.semaphore_wait(barrier, n - 1)

    def exchange(src, dst, stage, recv_sem):
        copies = []
        for k, p in enumerate(peers):
            copy = pltpu.make_async_remote_copy(
                src_ref=src(p), dst_ref=dst, send_sem=send_sem.at[stage, k], recv_sem=recv_sem.at[me],
                device_id={"tp": p}, device_id_type=MESH)
            copy.start()
            copies.append(copy)
        return copies

    def arrive(dst_of, recv_sem):
        for p in peers:
            ref = dst_of(p)
            pltpu.make_async_copy(ref, ref, recv_sem.at[p]).wait()

    def rows_of(p):
        return pl.ds(pl.multiple_of(p * own, own), own)

    q_sends = exchange(lambda p: q_ref.at[my_rows], q_ref.at[my_rows], 1, q_sem)
    lab_sends = exchange(lambda p: lab.at[my_rows], lab.at[my_rows], 0, lab_sem)
    m_run[...] = jnp.full(m_run.shape, LOWEST, F32)
    s_run[...] = jnp.zeros(s_run.shape, F32)
    t_run[...] = jnp.zeros(t_run.shape, F32)
    part[...] = jnp.zeros(part.shape, F32)
    with jax.named_scope("qgather"):
        arrive(lambda p: q_ref.at[rows_of(p)], q_sem)


    with jax.named_scope("tower"):
        a = dot(q_ref[...], w1[...], (1, 0))
        a_ref[...] = a
        h_ref[...] = jnp.maximum(a, 0.0).astype(BF16)
        x_ref[...] = dot(h_ref[...], w2_ref[...], (1, 0)).astype(BF16)
        arrive(lambda p: lab.at[rows_of(p)], lab_sem)

    local = lab[...] - me * items
    lane = lax.broadcasted_iota(jnp.int32, d.shape, 1)
    d[...] = local - lane

    def logits(i, z_ref):
        for j in range(TILE // LOAD_TILE):
            cat_copy(i * (TILE // LOAD_TILE) + j).wait()
        x = x_ref[...]
        m = m_run[...]
        for j in range(TILE // DOT_TILE):
            base = pl.multiple_of(i * TILE + j * DOT_TILE, DOT_TILE)
            z = dot(x, cat[pl.ds(base, DOT_TILE), :], (1, 1)) - lq[:, pl.ds(base, DOT_TILE)]
            for c in range(DOT_TILE // LANES):
                zc = z[:, c * LANES:(c + 1) * LANES]
                z_ref[j * (DOT_TILE // LANES) + c] = zc
                m = jnp.maximum(m, zc)
        m_run[...] = m
        m_hist[i + 1] = m

    def weigh(i, z_ref):
        for r in range(0, rows, GROUP):
            at = slice(r, r + GROUP)
            m = m_hist[i + 1, at, :]
            s = s_run[at, :] * jnp.exp(m_hist[i, at, :] - m)
            t = t_run[at, :]
            dd = d[at, :] - i * TILE
            for c in range(chunks):
                zc = z_ref[c, at, :]
                e = jnp.exp(zc - m)
                s = s + e
                t = jnp.where(dd == c * LANES, zc, t)
                ez[i * chunks + c, at, :] = e
            s_run[at, :] = s
            t_run[at, :] = t

    with jax.named_scope("pass1a"):
        m_hist[0] = m_run[...]
        logits(0, z_even)

    def first_pass(j, carry):
        logits(2 * j + 1, z_odd)
        weigh(2 * j, z_even)
        logits(2 * j + 2, z_even)
        weigh(2 * j + 1, z_odd)
        return carry

    with jax.named_scope("pass1b"):
        lax.fori_loop(0, tiles // 2 - 1, first_pass, 0)

    with jax.named_scope("pass1c"):
        logits(tiles - 1, z_odd)
        weigh(tiles - 2, z_even)
        weigh(tiles - 1, z_odd)


    m_t = m_run[...].T
    m_row = jnp.max(m_t, axis=0, keepdims=True)
    s_row = jnp.sum(s_run[...].T * jnp.exp(m_t - m_row), axis=0, keepdims=True)
    t_row = jnp.sum(t_run[...].T, axis=0, keepdims=True)
    sub = lax.broadcasted_iota(jnp.int32, (8, LANES), 0)
    stats[me] = jnp.where(sub == 0, m_row, jnp.where(sub == 1, s_row, t_row))
    stat_sends = exchange(lambda p: stats.at[me], stats.at[me], 2, stat_sem)
    with jax.named_scope("statwait"):
        arrive(lambda p: stats.at[p], stat_sem)

    big = stats[0, 0:1, :]
    for p in range(1, n):
        big = jnp.maximum(big, stats[p, 0:1, :])
    total = jnp.zeros_like(big)
    target = jnp.zeros_like(big)
    for p in range(n):
        total = total + stats[p, 1:2, :] * jnp.exp(stats[p, 0:1, :] - big)
        target = target + stats[p, 2:3, :]
    loss_ref[...] = jnp.broadcast_to(
        jnp.sum(big + jnp.log(total) - target, axis=1, keepdims=True) / rows, loss_ref.shape)
    inv = 1.0 / (total * rows)
    big_col = jnp.broadcast_to(big, (rows, LANES)).T
    inv_col = jnp.broadcast_to(inv, (rows, LANES)).T
    hit_col = jnp.broadcast_to(jnp.exp(target - big) * inv - 1.0 / rows, (rows, LANES)).T.astype(BF16)
    home = jnp.where(local - local // LANES * LANES == lane, local // LANES, -1)
    home = jnp.where((local >= 0) & (local < items), home, -1).astype(F32)

    def second_pass(i, carry):
        gs = []
        for f in range(SECOND_TILE // TILE):
            tile = i * (SECOND_TILE // TILE) + f
            scale = jnp.exp(m_hist[tile + 1] - big_col) * inv_col
            here = (home - (tile * chunks).astype(F32)).astype(BF16)
            for c in range(chunks):
                g = (ez[tile * chunks + c] * scale).astype(BF16)
                g = jnp.where(here == jnp.bfloat16(c), hit_col, g)
                g_ref[tile * chunks + c] = g
                gs.append(g)
        base = pl.multiple_of(i * SECOND_TILE, SECOND_TILE)
        part[...] += dot(jnp.concatenate(gs, axis=1), cat[pl.ds(base, SECOND_TILE), :], (1, 0))
        return carry

    with jax.named_scope("pass2"):
        lax.fori_loop(0, items // SECOND_TILE, second_pass, 0)


    part_sends = exchange(lambda p: part.at[rows_of(p)], pieces.at[me], 3, part_sem)
    pieces[me] = part[my_rows, :]
    with jax.named_scope("rswait"):
        arrive(lambda p: pieces.at[p], part_sem)

    acc = pieces[0]
    for p in range(1, n):
        acc = acc + pieces[p]
    dx_ref[my_rows, :] = acc.astype(BF16)
    dx_sends = exchange(lambda p: dx_ref.at[my_rows], dx_ref.at[my_rows], 4, dx_sem)
    with jax.named_scope("agwait"):
        arrive(lambda p: dx_ref.at[rows_of(p)], dx_sem)

    for copy in lab_sends + q_sends + stat_sends + part_sends + dx_sends:
        copy.wait_send()


def grad_kernel(g_ref, x_ref, dx_ref, h_ref, a_ref, q_ref, w2_ref, loss_ref,
                loss_hbm, de_hbm, dw1_hbm, dw2_hbm, loss, stage, dw1, dw2, out_sem, sem):
    items = de_hbm.shape[0]
    steps = items // OUT_TILE
    loss[...] = loss_ref[0:1, 0:1]
    loss_copy = pltpu.make_async_copy(loss, loss_hbm, sem.at[0])
    loss_copy.start()

    def out_copy(i, slot):
        at = pl.ds(pl.multiple_of(i * OUT_TILE, OUT_TILE), OUT_TILE)
        return pltpu.make_async_copy(stage.at[slot], de_hbm.at[at], out_sem.at[slot])

    def step(i, carry):
        slot = lax.rem(i, OUT_SLOTS)

        @pl.when(i >= OUT_SLOTS)
        def _():
            out_copy(i - OUT_SLOTS, slot).wait()

        count = OUT_TILE // LANES
        g = jnp.concatenate([g_ref[i * count + c] for c in range(count)], axis=1)
        stage[slot] = dot(g, x_ref[...], (0, 0)).astype(BF16)
        out_copy(i, slot).start()
        return carry

    with jax.named_scope("de1"):
        lax.fori_loop(0, OUT_SLOTS, step, 0)

    dx = dx_ref[...]
    dw2[...] = dot(h_ref[...], dx, (0, 0)).astype(BF16)
    pltpu.make_async_copy(dw2, dw2_hbm, sem.at[2]).start()
    dh = dot(dx, w2_ref[...], (1, 1))
    da = jnp.where(a_ref[...] > 0.0, dh, 0.0).astype(BF16)
    dw1[...] = dot(q_ref[...], da, (0, 0)).astype(BF16)
    pltpu.make_async_copy(dw1, dw1_hbm, sem.at[1]).start()
    with jax.named_scope("de2"):
        lax.fori_loop(OUT_SLOTS, steps, step, 0)

    with jax.named_scope("outwait"):
        for i in range(steps - OUT_SLOTS, steps):
            out_copy(i, i % OUT_SLOTS).wait()
        loss_copy.wait()
        pltpu.make_async_copy(dw1, dw1_hbm, sem.at[1]).wait()
        pltpu.make_async_copy(dw2, dw2_hbm, sem.at[2]).wait()


def solution(mesh):
    n = mesh.shape["tp"]

    def local_step(queries, w_first, w_second, catalogue, log_q, labels):
        own, d_in = queries.shape
        hid, emb = w_second.shape
        items = catalogue.shape[0]
        rows = own * n
        hbm = pl.BlockSpec(memory_space=pl.ANY)
        vmem = pl.BlockSpec(memory_space=pltpu.VMEM)
        dma = pltpu.SemaphoreType.DMA
        held = pl.pallas_call(
            functools.partial(loss_kernel, n),
            name="loss_kernel",
            out_shape=[
                pltpu.VMEM((items // LANES, rows, LANES), BF16),
                pltpu.VMEM((rows, emb), BF16),
                pltpu.VMEM((rows, emb), BF16),
                pltpu.VMEM((rows, hid), BF16),
                pltpu.VMEM((rows, hid), F32),
                pltpu.VMEM((rows, d_in), BF16),
                pltpu.VMEM((hid, emb), BF16),
                pltpu.VMEM((8, LANES), F32),
            ],
            in_specs=[hbm] * 6,
            out_specs=[vmem] * 8,
            scratch_shapes=[
                pltpu.VMEM((items, emb), BF16),
                pltpu.VMEM((items // LANES, rows, LANES), F32),
                pltpu.VMEM((TILE // LANES, rows, LANES), F32),
                pltpu.VMEM((TILE // LANES, rows, LANES), F32),
                pltpu.VMEM((1, items), F32),
                pltpu.VMEM((d_in, hid), BF16),
                pltpu.SMEM((own,), jnp.int32),
                pltpu.VMEM((rows, LANES), jnp.int32),
                pltpu.VMEM((rows, LANES), jnp.int32),
                pltpu.VMEM((rows, LANES), F32),
                pltpu.VMEM((rows, LANES), F32),
                pltpu.VMEM((rows, LANES), F32),
                pltpu.VMEM((items // TILE + 1, rows, LANES), F32),
                pltpu.VMEM((n, 8, LANES), F32),
                pltpu.VMEM((rows, emb), F32),
                pltpu.VMEM((n, own, emb), F32),
                dma((5,)),
                dma((items // LOAD_TILE,)),
                dma((5, n - 1)),
                dma((n,)),
                dma((n,)),
                dma((n,)),
                dma((n,)),
                dma((n,)),
            ],
            compiler_params=pltpu.CompilerParams(collective_id=0, has_side_effects=True, vmem_limit_bytes=50 << 20),
        )(queries, w_first, w_second, catalogue, log_q.reshape(1, items), labels)
        loss, grad_items, grad_first, grad_second = pl.pallas_call(
            grad_kernel,
            name="grad_kernel",
            out_shape=[
                jax.ShapeDtypeStruct((1, 1), F32),
                jax.ShapeDtypeStruct((items, emb), BF16),
                jax.ShapeDtypeStruct((d_in, hid), BF16),
                jax.ShapeDtypeStruct((hid, emb), BF16),
            ],
            in_specs=[vmem] * 8,
            out_specs=[hbm] * 4,
            scratch_shapes=[
                pltpu.VMEM((1, 1), F32),
                pltpu.VMEM((OUT_SLOTS, OUT_TILE, emb), BF16),
                pltpu.VMEM((d_in, hid), BF16),
                pltpu.VMEM((hid, emb), BF16),
                dma((OUT_SLOTS,)),
                dma((3,)),
            ],
            compiler_params=pltpu.CompilerParams(vmem_limit_bytes=40 << 20),
        )(*held)
        return loss.reshape(1), grad_items, grad_first, grad_second

    row_spec = P(("dp", "tp"), None)
    return jax.shard_map(
        local_step, mesh=mesh,
        in_specs=(row_spec, P(None, None), P(None, None), P("tp", None), P("tp"), P(("dp", "tp"))),
        out_specs=(P("dp"), row_spec, P("dp", None), P("dp", None)), check_vma=False)
```

```python
import functools

import jax
import jax.numpy as jnp
from jax import lax
from jax.experimental import pallas as pl
from jax.experimental.pallas import tpu as pltpu
from jax.sharding import PartitionSpec as P

F32, BF16 = jnp.float32, jnp.bfloat16
MESH = pl.DeviceIdType.MESH
LANES = 128
TILE = 4096
DOT_TILE = 512
GROUP = 16
SECOND_TILE = 8192
LOAD_TILE = 2048
OUT_TILE = 4096
EARLY = 5
LOWEST = -3.0e38


def dot(a, b, contract):
    return lax.dot_general(a, b, ((contract[:1], contract[1:]), ((), ())), preferred_element_type=F32)


def loss_kernel(n, q_hbm, w1_hbm, w2_hbm, cat_hbm, lq_hbm, lab_hbm,
                cat, dx_ref, h_ref, a_ref, q_ref, w2_ref, loss_ref,
                x_ref, g_ref, ez, z_even, z_odd, lq, w1, labels, lab, d, m_run, s_run, t_run, m_hist, stats, part, pieces,
                load_sem, cat_sem, send_sem, q_sem, lab_sem, stat_sem, part_sem, dx_sem):
    me = lax.axis_index("tp")
    own = q_hbm.shape[0]
    rows = own * n
    items = cat_hbm.shape[0]
    tiles = items // TILE
    chunks = TILE // LANES
    my_rows = pl.ds(pl.multiple_of(me * own, own), own)

    q_load = pltpu.make_async_copy(q_hbm, q_ref.at[my_rows], load_sem.at[0])
    w1_load = pltpu.make_async_copy(w1_hbm, w1, load_sem.at[1])
    w2_load = pltpu.make_async_copy(w2_hbm, w2_ref, load_sem.at[2])
    lq_load = pltpu.make_async_copy(lq_hbm, lq, load_sem.at[3])
    lab_load = pltpu.make_async_copy(lab_hbm, labels, load_sem.at[4])
    barrier = pltpu.get_barrier_semaphore()
    peers = [lax.rem(me + k, n) for k in range(1, n)]
    for p in peers:
        pl.semaphore_signal(barrier, inc=1, device_id={"tp": p}, device_id_type=MESH)
    for load in (q_load, lab_load, w1_load, w2_load, lq_load):
        load.start()
    lab_load.wait()
    for r in range(own):
        lab[pl.ds(me * own + r, 1), :] = jnp.full((1, LANES), labels[r], jnp.int32)
    with jax.named_scope("wload"):
        w1_load.wait()
        w2_load.wait()
        lq_load.wait()

    def cat_copy(k):
        part_rows = pl.ds(pl.multiple_of(k * LOAD_TILE, LOAD_TILE), LOAD_TILE)
        return pltpu.make_async_copy(cat_hbm.at[part_rows], cat.at[part_rows], cat_sem.at[k])

    for k in range(items // LOAD_TILE):
        cat_copy(k).start()
    q_load.wait()
    with jax.named_scope("bar"):
        pl.semaphore_wait(barrier, n - 1)

    def exchange(src, dst, stage, recv_sem):
        copies = []
        for k, p in enumerate(peers):
            copy = pltpu.make_async_remote_copy(
                src_ref=src(p), dst_ref=dst, send_sem=send_sem.at[stage, k], recv_sem=recv_sem.at[me],
                device_id={"tp": p}, device_id_type=MESH)
            copy.start()
            copies.append(copy)
        return copies

    def arrive(dst_of, recv_sem):
        for p in peers:
            ref = dst_of(p)
            pltpu.make_async_copy(ref, ref, recv_sem.at[p]).wait()

    def rows_of(p):
        return pl.ds(pl.multiple_of(p * own, own), own)

    q_sends = exchange(lambda p: q_ref.at[my_rows], q_ref.at[my_rows], 1, q_sem)
    lab_sends = exchange(lambda p: lab.at[my_rows], lab.at[my_rows], 0, lab_sem)
    m_run[...] = jnp.full(m_run.shape, LOWEST, F32)
    s_run[...] = jnp.zeros(s_run.shape, F32)
    t_run[...] = jnp.zeros(t_run.shape, F32)
    part[...] = jnp.zeros(part.shape, F32)
    with jax.named_scope("qgather"):
        arrive(lambda p: q_ref.at[rows_of(p)], q_sem)


    with jax.named_scope("tower"):
        a = dot(q_ref[...], w1[...], (1, 0))
        a_ref[...] = a
        h_ref[...] = jnp.maximum(a, 0.0).astype(BF16)
        x_ref[...] = dot(h_ref[...], w2_ref[...], (1, 0)).astype(BF16)
        arrive(lambda p: lab.at[rows_of(p)], lab_sem)

    local = lab[...] - me * items
    lane = lax.broadcasted_iota(jnp.int32, d.shape, 1)
    d[...] = local - lane

    def logits(i, z_ref):
        for j in range(TILE // DOT_TILE):
            base = pl.multiple_of(i * TILE + j * DOT_TILE, DOT_TILE)
            z = dot(x_ref[...], cat[pl.ds(base, DOT_TILE), :], (1, 1)) - lq[:, pl.ds(base, DOT_TILE)]
            m = m_run[...]
            for c in range(DOT_TILE // LANES):
                zc = z[:, c * LANES:(c + 1) * LANES]
                z_ref[j * (DOT_TILE // LANES) + c] = zc
                m = jnp.maximum(m, zc)
            m_run[...] = m
            yield
        m_hist[i + 1] = m

    def weigh(i, z_ref):
        for r in range(0, rows, GROUP):
            at = slice(r, r + GROUP)
            m = m_hist[i + 1, at, :]
            s = s_run[at, :] * jnp.exp(m_hist[i, at, :] - m)
            t = t_run[at, :]
            dd = d[at, :] - i * TILE
            for c in range(chunks):
                zc = z_ref[c, at, :]
                e = jnp.exp(zc - m)
                s = s + e
                t = jnp.where(dd == c * LANES, zc, t)
                ez[i * chunks + c, at, :] = e
            s_run[at, :] = s
            t_run[at, :] = t
            yield

    def arrived(i):
        for j in range(TILE // LOAD_TILE):
            cat_copy(i * (TILE // LOAD_TILE) + j).wait()

    def together(*parts):
        parts = list(parts)
        while parts:
            parts = [p for p in parts if next(p, parts) is not parts]

    with jax.named_scope("pass1a"):
        m_hist[0] = m_run[...]
        arrived(0)
        together(logits(0, z_even))

    def first_pass(j, carry):
        arrived(2 * j + 1)
        arrived(2 * j + 2)
        together(logits(2 * j + 1, z_odd), weigh(2 * j, z_even))
        together(logits(2 * j + 2, z_even), weigh(2 * j + 1, z_odd))
        return carry

    with jax.named_scope("pass1b"):
        lax.fori_loop(0, tiles // 2 - 1, first_pass, 0)

    with jax.named_scope("pass1c"):
        arrived(tiles - 1)
        together(logits(tiles - 1, z_odd), weigh(tiles - 2, z_even))
        together(weigh(tiles - 1, z_odd))


    m_t = m_run[...].T
    m_row = jnp.max(m_t, axis=0, keepdims=True)
    s_row = jnp.sum(s_run[...].T * jnp.exp(m_t - m_row), axis=0, keepdims=True)
    t_row = jnp.sum(t_run[...].T, axis=0, keepdims=True)
    sub = lax.broadcasted_iota(jnp.int32, (8, LANES), 0)
    stats[me] = jnp.where(sub == 0, m_row, jnp.where(sub == 1, s_row, t_row))
    stat_sends = exchange(lambda p: stats.at[me], stats.at[me], 2, stat_sem)
    with jax.named_scope("statwait"):
        arrive(lambda p: stats.at[p], stat_sem)

    big = stats[0, 0:1, :]
    for p in range(1, n):
        big = jnp.maximum(big, stats[p, 0:1, :])
    total = jnp.zeros_like(big)
    target = jnp.zeros_like(big)
    for p in range(n):
        total = total + stats[p, 1:2, :] * jnp.exp(stats[p, 0:1, :] - big)
        target = target + stats[p, 2:3, :]
    loss_ref[...] = jnp.broadcast_to(
        jnp.sum(big + jnp.log(total) - target, axis=1, keepdims=True) / rows, loss_ref.shape)
    inv = 1.0 / (total * rows)
    big_col = jnp.broadcast_to(big, (rows, LANES)).T
    inv_col = jnp.broadcast_to(inv, (rows, LANES)).T
    hit_col = jnp.broadcast_to(jnp.exp(target - big) * inv - 1.0 / rows, (rows, LANES)).T.astype(BF16)
    home = jnp.where(local - local // LANES * LANES == lane, local // LANES, -1)
    home = jnp.where((local >= 0) & (local < items), home, -1).astype(F32)

    def second_pass(i, carry):
        gs = []
        for f in range(SECOND_TILE // TILE):
            tile = i * (SECOND_TILE // TILE) + f
            scale = jnp.exp(m_hist[tile + 1] - big_col) * inv_col
            here = (home - (tile * chunks).astype(F32)).astype(BF16)
            for c in range(chunks):
                g = (ez[tile * chunks + c] * scale).astype(BF16)
                g = jnp.where(here == jnp.bfloat16(c), hit_col, g)
                g_ref[tile * chunks + c] = g
                gs.append(g)
        base = pl.multiple_of(i * SECOND_TILE, SECOND_TILE)
        part[...] += dot(jnp.concatenate(gs, axis=1), cat[pl.ds(base, SECOND_TILE), :], (1, 0))
        return carry

    with jax.named_scope("pass2"):
        lax.fori_loop(0, items // SECOND_TILE, second_pass, 0)


    part_sends = exchange(lambda p: part.at[rows_of(p)], pieces.at[me], 3, part_sem)
    pieces[me] = part[my_rows, :]

    def item_grads(i, carry):
        count = OUT_TILE // LANES
        g = jnp.concatenate([g_ref[i * count + c] for c in range(count)], axis=1)
        cat[pl.ds(pl.multiple_of(i * OUT_TILE, OUT_TILE), OUT_TILE), :] = dot(g, x_ref[...], (0, 0)).astype(BF16)
        return carry

    with jax.named_scope("de1"):
        lax.fori_loop(0, EARLY, item_grads, 0)

    with jax.named_scope("rswait"):
        arrive(lambda p: pieces.at[p], part_sem)

    acc = pieces[0]
    for p in range(1, n):
        acc = acc + pieces[p]
    dx_ref[my_rows, :] = acc.astype(BF16)
    dx_sends = exchange(lambda p: dx_ref.at[my_rows], dx_ref.at[my_rows], 4, dx_sem)
    with jax.named_scope("de2"):
        lax.fori_loop(EARLY, items // OUT_TILE, item_grads, 0)

    with jax.named_scope("agwait"):
        arrive(lambda p: dx_ref.at[rows_of(p)], dx_sem)

    for copy in lab_sends + q_sends + stat_sends + part_sends + dx_sends:
        copy.wait_send()


def grad_kernel(de_ref, dx_ref, h_ref, a_ref, q_ref, w2_ref, loss_ref,
                loss_hbm, de_hbm, dw1_hbm, dw2_hbm, loss, dw1, dw2, out_sem, sem):
    copies = []
    for k in range(de_hbm.shape[0] // LOAD_TILE):
        at = pl.ds(k * LOAD_TILE, LOAD_TILE)
        copies.append(pltpu.make_async_copy(de_ref.at[at], de_hbm.at[at], out_sem.at[k]))
        copies[-1].start()
    with jax.named_scope("bwd"):
        dx = dx_ref[...]
        dw2[...] = dot(h_ref[...], dx, (0, 0)).astype(BF16)
        dh = dot(dx, w2_ref[...], (1, 1))
        da = jnp.where(a_ref[...] > 0.0, dh, 0.0).astype(BF16)
        dw1[...] = dot(q_ref[...], da, (0, 0)).astype(BF16)
        loss[...] = loss_ref[0:1, 0:1]
        copies.append(pltpu.make_async_copy(loss, loss_hbm, sem.at[0]))
        copies.append(pltpu.make_async_copy(dw1, dw1_hbm, sem.at[1]))
        copies.append(pltpu.make_async_copy(dw2, dw2_hbm, sem.at[2]))
        for copy in copies[-3:]:
            copy.start()

    for copy in copies:
        copy.wait()


def solution(mesh):
    n = mesh.shape["tp"]

    def local_step(queries, w_first, w_second, catalogue, log_q, labels):
        own, d_in = queries.shape
        hid, emb = w_second.shape
        items = catalogue.shape[0]
        rows = own * n
        hbm = pl.BlockSpec(memory_space=pl.ANY)
        vmem = pl.BlockSpec(memory_space=pltpu.VMEM)
        dma = pltpu.SemaphoreType.DMA
        held = pl.pallas_call(
            functools.partial(loss_kernel, n),
            name="loss_kernel",
            out_shape=[
                pltpu.VMEM((items, emb), BF16),
                pltpu.VMEM((rows, emb), BF16),
                pltpu.VMEM((rows, hid), BF16),
                pltpu.VMEM((rows, hid), F32),
                pltpu.VMEM((rows, d_in), BF16),
                pltpu.VMEM((hid, emb), BF16),
                pltpu.VMEM((8, LANES), F32),
            ],
            in_specs=[hbm] * 6,
            out_specs=[vmem] * 7,
            scratch_shapes=[
                pltpu.VMEM((rows, emb), BF16),
                pltpu.VMEM((items // LANES, rows, LANES), BF16),
                pltpu.VMEM((items // LANES, rows, LANES), F32),
                pltpu.VMEM((TILE // LANES, rows, LANES), F32),
                pltpu.VMEM((TILE // LANES, rows, LANES), F32),
                pltpu.VMEM((1, items), F32),
                pltpu.VMEM((d_in, hid), BF16),
                pltpu.SMEM((own,), jnp.int32),
                pltpu.VMEM((rows, LANES), jnp.int32),
                pltpu.VMEM((rows, LANES), jnp.int32),
                pltpu.VMEM((rows, LANES), F32),
                pltpu.VMEM((rows, LANES), F32),
                pltpu.VMEM((rows, LANES), F32),
                pltpu.VMEM((items // TILE + 1, rows, LANES), F32),
                pltpu.VMEM((n, 8, LANES), F32),
                pltpu.VMEM((rows, emb), F32),
                pltpu.VMEM((n, own, emb), F32),
                dma((5,)),
                dma((items // LOAD_TILE,)),
                dma((5, n - 1)),
                dma((n,)),
                dma((n,)),
                dma((n,)),
                dma((n,)),
                dma((n,)),
            ],
            compiler_params=pltpu.CompilerParams(collective_id=0, has_side_effects=True, vmem_limit_bytes=44 << 20),
        )(queries, w_first, w_second, catalogue, log_q.reshape(1, items), labels)
        loss, grad_items, grad_first, grad_second = pl.pallas_call(
            grad_kernel,
            name="grad_kernel",
            out_shape=[
                jax.ShapeDtypeStruct((1, 1), F32),
                jax.ShapeDtypeStruct((items, emb), BF16),
                jax.ShapeDtypeStruct((d_in, hid), BF16),
                jax.ShapeDtypeStruct((hid, emb), BF16),
            ],
            in_specs=[vmem] * 7,
            out_specs=[hbm] * 4,
            scratch_shapes=[
                pltpu.VMEM((1, 1), F32),
                pltpu.VMEM((d_in, hid), BF16),
                pltpu.VMEM((hid, emb), BF16),
                dma((items // LOAD_TILE,)),
                dma((3,)),
            ],
            compiler_params=pltpu.CompilerParams(vmem_limit_bytes=24 << 20),
        )(*held)
        return loss.reshape(1), grad_items, grad_first, grad_second

    row_spec = P(("dp", "tp"), None)
    return jax.shard_map(
        local_step, mesh=mesh,
        in_specs=(row_spec, P(None, None), P(None, None), P("tp", None), P("tp"), P(("dp", "tp"))),
        out_specs=(P("dp"), row_spec, P("dp", None), P("dp", None)), check_vma=False)
```

```python
import functools

import jax
import jax.numpy as jnp
from jax import lax
from jax.experimental import pallas as pl
from jax.experimental.pallas import tpu as pltpu
from jax.sharding import PartitionSpec as P

F32, BF16 = jnp.float32, jnp.bfloat16
MESH = pl.DeviceIdType.MESH
LANES = 128
TILE = 4096
DOT_TILE = 512
GROUP = 16
SECOND_TILE = 8192
LOAD_TILE = 2048
OUT_TILE = 4096
EARLY = 5
LOWEST = -3.0e38


def dot(a, b, contract):
    return lax.dot_general(a, b, ((contract[:1], contract[1:]), ((), ())), preferred_element_type=F32)


def loss_kernel(n, q_hbm, w1_hbm, w2_hbm, cat_hbm, lq_hbm, lab_hbm,
                cat, dx_ref, h_ref, a_ref, q_ref, w2_ref, loss_ref,
                x_ref, g_ref, ez, z_even, z_odd, lq, w1, labels, lab, d, m_run, s_run, t_run, m_hist, stats, targets, part, pieces,
                load_sem, cat_sem, send_sem, q_sem, lab_sem, stat_sem, target_sem, part_sem, dx_sem):
    me = lax.axis_index("tp")
    own = q_hbm.shape[0]
    rows = own * n
    items = cat_hbm.shape[0]
    tiles = items // TILE
    chunks = TILE // LANES
    my_rows = pl.ds(pl.multiple_of(me * own, own), own)

    q_load = pltpu.make_async_copy(q_hbm, q_ref.at[my_rows], load_sem.at[0])
    w1_load = pltpu.make_async_copy(w1_hbm, w1, load_sem.at[1])
    w2_load = pltpu.make_async_copy(w2_hbm, w2_ref, load_sem.at[2])
    lq_load = pltpu.make_async_copy(lq_hbm, lq, load_sem.at[3])
    lab_load = pltpu.make_async_copy(lab_hbm, labels, load_sem.at[4])
    barrier = pltpu.get_barrier_semaphore()
    peers = [lax.rem(me + k, n) for k in range(1, n)]
    for p in peers:
        pl.semaphore_signal(barrier, inc=1, device_id={"tp": p}, device_id_type=MESH)
    for load in (q_load, w1_load, w2_load, lq_load, lab_load):
        load.start()

    def cat_copy(k):
        part_rows = pl.ds(pl.multiple_of(k * LOAD_TILE, LOAD_TILE), LOAD_TILE)
        return pltpu.make_async_copy(cat_hbm.at[part_rows], cat.at[part_rows], cat_sem.at[k])

    with jax.named_scope("bar"):
        pl.semaphore_wait(barrier, n - 1)

    def exchange(src, dst, stage, recv_sem):
        copies = []
        for k, p in enumerate(peers):
            copy = pltpu.make_async_remote_copy(
                src_ref=src(p), dst_ref=dst, send_sem=send_sem.at[stage, k], recv_sem=recv_sem.at[me],
                device_id={"tp": p}, device_id_type=MESH)
            copy.start()
            copies.append(copy)
        return copies

    def arrive(dst_of, recv_sem):
        for p in peers:
            ref = dst_of(p)
            pltpu.make_async_copy(ref, ref, recv_sem.at[p]).wait()

    def rows_of(p):
        return pl.ds(pl.multiple_of(p * own, own), own)

    q_load.wait()
    q_sends = exchange(lambda p: q_ref.at[my_rows], q_ref.at[my_rows], 1, q_sem)
    with jax.named_scope("wload"):
        w1_load.wait()
        w2_load.wait()
        lq_load.wait()
        for k in range(items // LOAD_TILE):
            cat_copy(k).start()

    lab_load.wait()
    for r in range(own):
        lab[pl.ds(me * own + r, 1), :] = jnp.full((1, LANES), labels[r], jnp.int32)
    m_run[...] = jnp.full(m_run.shape, LOWEST, F32)
    s_run[...] = jnp.zeros(s_run.shape, F32)
    part[...] = jnp.zeros(part.shape, F32)
    lab_sends = exchange(lambda p: lab.at[my_rows], lab.at[my_rows], 0, lab_sem)
    with jax.named_scope("qgather"):
        arrive(lambda p: q_ref.at[rows_of(p)], q_sem)


    with jax.named_scope("tower"):
        a = dot(q_ref[...], w1[...], (1, 0))
        a_ref[...] = a
        h_ref[...] = jnp.maximum(a, 0.0).astype(BF16)
        x_ref[...] = dot(h_ref[...], w2_ref[...], (1, 0)).astype(BF16)
        arrive(lambda p: lab.at[rows_of(p)], lab_sem)

    local = lab[...] - me * items
    lane = lax.broadcasted_iota(jnp.int32, lab.shape, 1)
    d[...] = local - lane

    def logits(i, z_ref):
        for j in range(TILE // DOT_TILE):
            base = pl.multiple_of(i * TILE + j * DOT_TILE, DOT_TILE)
            z = dot(x_ref[...], cat[pl.ds(base, DOT_TILE), :], (1, 1)) - lq[:, pl.ds(base, DOT_TILE)]
            m = m_run[...]
            for c in range(DOT_TILE // LANES):
                zc = z[:, c * LANES:(c + 1) * LANES]
                z_ref[j * (DOT_TILE // LANES) + c] = zc
                ez[i * chunks + j * (DOT_TILE // LANES) + c] = zc
                m = jnp.maximum(m, zc)
            m_run[...] = m
            yield
        m_hist[i + 1] = m

    def weigh(i, z_ref):
        for r in range(0, rows, GROUP):
            at = slice(r, r + GROUP)
            m = m_hist[i + 1, at, :]
            s = s_run[at, :] * jnp.exp(m_hist[i, at, :] - m)
            for c in range(chunks):
                s = s + jnp.exp(z_ref[c, at, :] - m)
            s_run[at, :] = s
            yield

    def arrived(i):
        for j in range(TILE // LOAD_TILE):
            cat_copy(i * (TILE // LOAD_TILE) + j).wait()

    def together(*parts):
        parts = list(parts)
        while parts:
            parts = [p for p in parts if next(p, parts) is not parts]

    with jax.named_scope("pass1a"):
        m_hist[0] = m_run[...]
        arrived(0)
        together(logits(0, z_even))

    def first_pass(j, carry):
        arrived(2 * j + 1)
        arrived(2 * j + 2)
        together(logits(2 * j + 1, z_odd), weigh(2 * j, z_even))
        together(logits(2 * j + 2, z_even), weigh(2 * j + 1, z_odd))
        return carry

    with jax.named_scope("pass1b"):
        lax.fori_loop(0, tiles // 2 - 1, first_pass, 0)

    with jax.named_scope("pass1c"):
        arrived(tiles - 1)
        together(logits(tiles - 1, z_odd), weigh(tiles - 2, z_even))
        together(weigh(tiles - 1, z_odd))


    m_t = m_run[...].T
    m_row = jnp.max(m_t, axis=0, keepdims=True)
    s_row = jnp.sum(s_run[...].T * jnp.exp(m_t - m_row), axis=0, keepdims=True)
    sub = lax.broadcasted_iota(jnp.int32, (8, LANES), 0)
    stats[me] = jnp.where(sub == 0, m_row, s_row)
    stat_sends = exchange(lambda p: stats.at[me], stats.at[me], 2, stat_sem)
    t_run[...] = jnp.zeros(t_run.shape, F32)

    def weights(i, carry):
        for r in range(0, rows, GROUP):
            at = slice(r, r + GROUP)
            m = m_run[at, :]
            t = t_run[at, :]
            dd = d[at, :] - i * TILE
            for c in range(chunks):
                zc = ez[i * chunks + c, at, :]
                t = jnp.where(dd == c * LANES, zc, t)
                ez[i * chunks + c, at, :] = jnp.exp(zc - m)
            t_run[at, :] = t
        return carry

    with jax.named_scope("weights"):
        lax.fori_loop(0, tiles, weights, 0)

    t_col = jnp.broadcast_to(jnp.sum(t_run[...], axis=1, keepdims=True), lab.shape)
    targets[me] = t_col.T[0:8, :]
    with jax.named_scope("statwait"):
        arrive(lambda p: stats.at[p], stat_sem)

    big = stats[0, 0:1, :]
    for p in range(1, n):
        big = jnp.maximum(big, stats[p, 0:1, :])
    total = jnp.zeros_like(big)
    for p in range(n):
        total = total + stats[p, 1:2, :] * jnp.exp(stats[p, 0:1, :] - big)
    inv = 1.0 / (total * rows)
    big_col = jnp.broadcast_to(big, (rows, LANES)).T
    inv_col = jnp.broadcast_to(inv, (rows, LANES)).T
    hit_col = (jnp.exp(t_col - big_col) * inv_col - 1.0 / rows).astype(BF16)
    scale = jnp.exp(m_run[...] - big_col) * inv_col
    home = jnp.where(local - local // LANES * LANES == lane, local // LANES, -1)
    home = jnp.where((local >= 0) & (local < items), home, -1).astype(F32)

    def second_pass(i, carry):
        gs = []
        for f in range(SECOND_TILE // TILE):
            tile = i * (SECOND_TILE // TILE) + f
            here = (home - (tile * chunks).astype(F32)).astype(BF16)
            for c in range(chunks):
                g = (ez[tile * chunks + c] * scale).astype(BF16)
                g = jnp.where(here == jnp.bfloat16(c), hit_col, g)
                g_ref[tile * chunks + c] = g
                gs.append(g)
        base = pl.multiple_of(i * SECOND_TILE, SECOND_TILE)
        part[...] += dot(jnp.concatenate(gs, axis=1), cat[pl.ds(base, SECOND_TILE), :], (1, 0))
        return carry

    with jax.named_scope("pass2"):
        lax.fori_loop(0, items // SECOND_TILE, second_pass, 0)


    part_sends = exchange(lambda p: part.at[rows_of(p)], pieces.at[me], 3, part_sem)
    target_sends = exchange(lambda p: targets.at[me], targets.at[me], 5, target_sem)
    pieces[me] = part[my_rows, :]

    def item_grads(i, carry):
        count = OUT_TILE // LANES
        g = jnp.concatenate([g_ref[i * count + c] for c in range(count)], axis=1)
        cat[pl.ds(pl.multiple_of(i * OUT_TILE, OUT_TILE), OUT_TILE), :] = dot(g, x_ref[...], (0, 0)).astype(BF16)
        return carry

    with jax.named_scope("de1"):
        lax.fori_loop(0, EARLY, item_grads, 0)

    with jax.named_scope("rswait"):
        arrive(lambda p: pieces.at[p], part_sem)

    acc = pieces[0]
    for p in range(1, n):
        acc = acc + pieces[p]
    dx_ref[my_rows, :] = acc.astype(BF16)
    dx_sends = exchange(lambda p: dx_ref.at[my_rows], dx_ref.at[my_rows], 4, dx_sem)
    with jax.named_scope("de2"):
        lax.fori_loop(EARLY, items // OUT_TILE, item_grads, 0)

    with jax.named_scope("agwait"):
        arrive(lambda p: dx_ref.at[rows_of(p)], dx_sem)

    arrive(lambda p: targets.at[p], target_sem)
    target = targets[0, 0:1, :]
    for p in range(1, n):
        target = target + targets[p, 0:1, :]
    loss_ref[...] = jnp.broadcast_to(
        jnp.sum(big + jnp.log(total) - target, axis=1, keepdims=True) / rows, loss_ref.shape)
    with jax.named_scope("sendwait"):
        for copy in target_sends + lab_sends + q_sends + stat_sends + part_sends + dx_sends:
            copy.wait_send()


def grad_kernel(de_ref, dx_ref, h_ref, a_ref, q_ref, w2_ref, loss_ref,
                loss_hbm, de_hbm, dw1_hbm, dw2_hbm, loss, dw1, dw2, out_sem, sem):
    copies = []
    for k in range(de_hbm.shape[0] // LOAD_TILE):
        at = pl.ds(k * LOAD_TILE, LOAD_TILE)
        copies.append(pltpu.make_async_copy(de_ref.at[at], de_hbm.at[at], out_sem.at[k]))
        copies[-1].start()
    with jax.named_scope("bwd"):
        dx = dx_ref[...]
        dw2[...] = dot(h_ref[...], dx, (0, 0)).astype(BF16)
        dh = dot(dx, w2_ref[...], (1, 1))
        da = jnp.where(a_ref[...] > 0.0, dh, 0.0).astype(BF16)
        dw1[...] = dot(q_ref[...], da, (0, 0)).astype(BF16)
        loss[...] = loss_ref[0:1, 0:1]
        copies.append(pltpu.make_async_copy(loss, loss_hbm, sem.at[0]))
        copies.append(pltpu.make_async_copy(dw1, dw1_hbm, sem.at[1]))
        copies.append(pltpu.make_async_copy(dw2, dw2_hbm, sem.at[2]))
        for copy in copies[-3:]:
            copy.start()

    for copy in copies:
        copy.wait()


def solution(mesh):
    n = mesh.shape["tp"]

    def local_step(queries, w_first, w_second, catalogue, log_q, labels):
        own, d_in = queries.shape
        hid, emb = w_second.shape
        items = catalogue.shape[0]
        rows = own * n
        hbm = pl.BlockSpec(memory_space=pl.ANY)
        vmem = pl.BlockSpec(memory_space=pltpu.VMEM)
        dma = pltpu.SemaphoreType.DMA
        held = pl.pallas_call(
            functools.partial(loss_kernel, n),
            name="loss_kernel",
            out_shape=[
                pltpu.VMEM((items, emb), BF16),
                pltpu.VMEM((rows, emb), BF16),
                pltpu.VMEM((rows, hid), BF16),
                pltpu.VMEM((rows, hid), F32),
                pltpu.VMEM((rows, d_in), BF16),
                pltpu.VMEM((hid, emb), BF16),
                pltpu.VMEM((32, LANES), F32),
            ],
            in_specs=[hbm] * 6,
            out_specs=[vmem] * 7,
            scratch_shapes=[
                pltpu.VMEM((rows, emb), BF16),
                pltpu.VMEM((items // LANES, rows, LANES), BF16),
                pltpu.VMEM((items // LANES, rows, LANES), F32),
                pltpu.VMEM((TILE // LANES, rows, LANES), F32),
                pltpu.VMEM((TILE // LANES, rows, LANES), F32),
                pltpu.VMEM((1, items), F32),
                pltpu.VMEM((d_in, hid), BF16),
                pltpu.SMEM((own,), jnp.int32),
                pltpu.VMEM((rows, LANES), jnp.int32),
                pltpu.VMEM((rows, LANES), jnp.int32),
                pltpu.VMEM((rows, LANES), F32),
                pltpu.VMEM((rows, LANES), F32),
                pltpu.VMEM((rows, LANES), F32),
                pltpu.VMEM((items // TILE + 1, rows, LANES), F32),
                pltpu.VMEM((n, 8, LANES), F32),
                pltpu.VMEM((n, 8, LANES), F32),
                pltpu.VMEM((rows, emb), F32),
                pltpu.VMEM((n, own, emb), F32),
                dma((5,)),
                dma((items // LOAD_TILE,)),
                dma((6, n - 1)),
                dma((n,)),
                dma((n,)),
                dma((n,)),
                dma((n,)),
                dma((n,)),
                dma((n,)),
            ],
            compiler_params=pltpu.CompilerParams(collective_id=0, has_side_effects=True, vmem_limit_bytes=44 << 20),
        )(queries, w_first, w_second, catalogue, log_q.reshape(1, items), labels)
        loss, grad_items, grad_first, grad_second = pl.pallas_call(
            grad_kernel,
            name="grad_kernel",
            out_shape=[
                jax.ShapeDtypeStruct((1, 1), F32),
                jax.ShapeDtypeStruct((items, emb), BF16),
                jax.ShapeDtypeStruct((d_in, hid), BF16),
                jax.ShapeDtypeStruct((hid, emb), BF16),
            ],
            in_specs=[vmem] * 7,
            out_specs=[hbm] * 4,
            scratch_shapes=[
                pltpu.VMEM((1, 1), F32),
                pltpu.VMEM((d_in, hid), BF16),
                pltpu.VMEM((hid, emb), BF16),
                dma((items // LOAD_TILE,)),
                dma((3,)),
            ],
            compiler_params=pltpu.CompilerParams(vmem_limit_bytes=24 << 20),
        )(*held)
        return loss.reshape(1), grad_items, grad_first, grad_second

    row_spec = P(("dp", "tp"), None)
    return jax.shard_map(
        local_step, mesh=mesh,
        in_specs=(row_spec, P(None, None), P(None, None), P("tp", None), P("tp"), P(("dp", "tp"))),
        out_specs=(P("dp"), row_spec, P("dp", None), P("dp", None)), check_vma=False)
```

```python
import functools

import jax
import jax.numpy as jnp
from jax import lax
from jax.experimental import pallas as pl
from jax.experimental.pallas import tpu as pltpu
from jax.sharding import PartitionSpec as P

F32, BF16 = jnp.float32, jnp.bfloat16
MESH = pl.DeviceIdType.MESH
LANES = 128
TILE = 4096
DOT_TILE = 512
GROUP = 16
SECOND_TILE = 8192
LOAD_TILE = 4096
OUT_TILE = 4096
EARLY = 5
LOWEST = -3.0e38


def dot(a, b, contract):
    return lax.dot_general(a, b, ((contract[:1], contract[1:]), ((), ())), preferred_element_type=F32)


def loss_kernel(n, q_hbm, w1_hbm, w2_hbm, cat_hbm, lq_hbm, lab_hbm,
                cat, dx_ref, h_ref, a_ref, q_ref, w2_ref, loss_ref,
                x_ref, g_ref, ez, z_even, z_odd, lq, w1, labels, lab, d, m_run, s_run, t_run, m_hist, stats, targets, part, pieces,
                load_sem, cat_sem, send_sem, recv_sem):
    me = lax.axis_index("tp")
    own = q_hbm.shape[0]
    rows = own * n
    items = cat_hbm.shape[0]
    tiles = items // TILE
    chunks = TILE // LANES
    my_rows = pl.ds(pl.multiple_of(me * own, own), own)

    others = pl.ds(0, n - 1)
    other_rows = pl.ds(0, rows - own)

    q_load = pltpu.make_async_copy(q_hbm, q_ref.at[my_rows], load_sem.at[0])
    w1_load = pltpu.make_async_copy(w1_hbm, w1, load_sem.at[1])
    w2_load = pltpu.make_async_copy(w2_hbm, w2_ref, load_sem.at[2])
    lq_load = pltpu.make_async_copy(lq_hbm, lq, load_sem.at[3])
    lab_load = pltpu.make_async_copy(lab_hbm, labels, load_sem.at[4])
    barrier = pltpu.get_barrier_semaphore()
    peers = [lax.rem(me + k, n) for k in range(1, n)]
    for p in peers:
        pl.semaphore_signal(barrier, inc=1, device_id={"tp": p}, device_id_type=MESH)
    for load in (q_load, w1_load, w2_load, lq_load, lab_load):
        load.start()

    def cat_copy(k):
        part_rows = pl.ds(pl.multiple_of(k * LOAD_TILE, LOAD_TILE), LOAD_TILE)
        return pltpu.make_async_copy(cat_hbm.at[part_rows], cat.at[part_rows], cat_sem.at[k])

    with jax.named_scope("bar"):
        pl.semaphore_wait(barrier, n - 1)

    def exchange(src, dst, stage):
        for p in peers:
            pltpu.make_async_remote_copy(
                src_ref=src(p), dst_ref=dst, send_sem=send_sem.at[stage], recv_sem=recv_sem.at[stage],
                device_id={"tp": p}, device_id_type=MESH).start()

    def arrive(others, stage):
        pltpu.make_async_copy(others, others, recv_sem.at[stage]).wait()

    def sent(others, stage):
        pltpu.make_async_copy(others, others, send_sem.at[stage]).wait()

    def rows_of(p):
        return pl.ds(pl.multiple_of(p * own, own), own)

    q_load.wait()
    exchange(lambda p: q_ref.at[my_rows], q_ref.at[my_rows], 1)
    with jax.named_scope("wload"):
        w1_load.wait()
        w2_load.wait()
        lq_load.wait()
        for k in range(items // LOAD_TILE):
            cat_copy(k).start()

    lab_load.wait()
    for r in range(own):
        lab[pl.ds(me * own + r, 1), :] = jnp.full((1, LANES), labels[r], jnp.int32)
    m_run[...] = jnp.full(m_run.shape, LOWEST, F32)
    s_run[...] = jnp.zeros(s_run.shape, F32)
    part[...] = jnp.zeros(part.shape, F32)
    exchange(lambda p: lab.at[my_rows], lab.at[my_rows], 0)
    with jax.named_scope("qgather"):
        arrive(q_ref.at[other_rows], 1)


    with jax.named_scope("tower"):
        a = dot(q_ref[...], w1[...], (1, 0))
        a_ref[...] = a
        h_ref[...] = jnp.maximum(a, 0.0).astype(BF16)
        x_ref[...] = dot(h_ref[...], w2_ref[...], (1, 0)).astype(BF16)
        arrive(lab.at[other_rows], 0)

    local = lab[...] - me * items
    lane = lax.broadcasted_iota(jnp.int32, lab.shape, 1)
    d[...] = local - lane

    def logits(i, z_ref):
        for j in range(TILE // DOT_TILE):
            base = pl.multiple_of(i * TILE + j * DOT_TILE, DOT_TILE)
            z = dot(x_ref[...], cat[pl.ds(base, DOT_TILE), :], (1, 1)) - lq[:, pl.ds(base, DOT_TILE)]
            m = m_run[...]
            for c in range(DOT_TILE // LANES):
                zc = z[:, c * LANES:(c + 1) * LANES]
                z_ref[j * (DOT_TILE // LANES) + c] = zc
                ez[i * chunks + j * (DOT_TILE // LANES) + c] = zc
                m = jnp.maximum(m, zc)
            m_run[...] = m
            yield
        m_hist[i + 1] = m

    def weigh(i, z_ref):
        for r in range(0, rows, GROUP):
            at = slice(r, r + GROUP)
            m = m_hist[i + 1, at, :]
            s = s_run[at, :] * jnp.exp(m_hist[i, at, :] - m)
            for c in range(chunks):
                s = s + jnp.exp(z_ref[c, at, :] - m)
            s_run[at, :] = s
            yield

    def arrived(i):
        for j in range(TILE // LOAD_TILE):
            cat_copy(i * (TILE // LOAD_TILE) + j).wait()

    def together(*parts):
        parts = list(parts)
        while parts:
            parts = [p for p in parts if next(p, parts) is not parts]

    with jax.named_scope("pass1a"):
        m_hist[0] = m_run[...]
        arrived(0)
        together(logits(0, z_even))

    def first_pass(j, carry):
        arrived(2 * j + 1)
        arrived(2 * j + 2)
        together(logits(2 * j + 1, z_odd), weigh(2 * j, z_even))
        together(logits(2 * j + 2, z_even), weigh(2 * j + 1, z_odd))
        return carry

    with jax.named_scope("pass1b"):
        lax.fori_loop(0, tiles // 2 - 1, first_pass, 0)

    with jax.named_scope("pass1c"):
        arrived(tiles - 1)
        together(logits(tiles - 1, z_odd), weigh(tiles - 2, z_even))
        together(weigh(tiles - 1, z_odd))


    m_t = m_run[...].T
    m_row = jnp.max(m_t, axis=0, keepdims=True)
    s_row = jnp.sum(s_run[...].T * jnp.exp(m_t - m_row), axis=0, keepdims=True)
    sub = lax.broadcasted_iota(jnp.int32, (8, LANES), 0)
    stats[me] = jnp.where(sub == 0, m_row, s_row)
    exchange(lambda p: stats.at[me], stats.at[me], 2)
    t_run[...] = jnp.zeros(t_run.shape, F32)

    def weights(i, carry):
        for r in range(0, rows, GROUP):
            at = slice(r, r + GROUP)
            m = m_run[at, :]
            t = t_run[at, :]
            dd = d[at, :] - i * TILE
            for c in range(chunks):
                zc = ez[i * chunks + c, at, :]
                t = jnp.where(dd == c * LANES, zc, t)
                ez[i * chunks + c, at, :] = jnp.exp(zc - m)
            t_run[at, :] = t
        return carry

    with jax.named_scope("weights"):
        lax.fori_loop(0, tiles, weights, 0)

    t_col = jnp.broadcast_to(jnp.sum(t_run[...], axis=1, keepdims=True), lab.shape)
    targets[me] = t_col.T[0:8, :]
    with jax.named_scope("statwait"):
        arrive(stats.at[others], 2)

    big = stats[0, 0:1, :]
    for p in range(1, n):
        big = jnp.maximum(big, stats[p, 0:1, :])
    total = jnp.zeros_like(big)
    for p in range(n):
        total = total + stats[p, 1:2, :] * jnp.exp(stats[p, 0:1, :] - big)
    inv = 1.0 / (total * rows)
    big_col = jnp.broadcast_to(big, (rows, LANES)).T
    inv_col = jnp.broadcast_to(inv, (rows, LANES)).T
    hit_col = (jnp.exp(t_col - big_col) * inv_col - 1.0 / rows).astype(BF16)
    scale = jnp.exp(m_run[...] - big_col) * inv_col
    home = jnp.where(local - local // LANES * LANES == lane, local // LANES, -1)
    home = jnp.where((local >= 0) & (local < items), home, -1).astype(F32)

    def second_pass(i, carry):
        gs = []
        for f in range(SECOND_TILE // TILE):
            tile = i * (SECOND_TILE // TILE) + f
            here = (home - (tile * chunks).astype(F32)).astype(BF16)
            for c in range(chunks):
                g = (ez[tile * chunks + c] * scale).astype(BF16)
                g = jnp.where(here == jnp.bfloat16(c), hit_col, g)
                g_ref[tile * chunks + c] = g
                gs.append(g)
        base = pl.multiple_of(i * SECOND_TILE, SECOND_TILE)
        part[...] += dot(jnp.concatenate(gs, axis=1), cat[pl.ds(base, SECOND_TILE), :], (1, 0))
        return carry

    with jax.named_scope("pass2"):
        lax.fori_loop(0, items // SECOND_TILE, second_pass, 0)

    exchange(lambda p: part.at[rows_of(p)], pieces.at[me], 3)
    pieces[me] = part[my_rows, :]

    def item_grads(i, carry):
        count = OUT_TILE // LANES
        g = jnp.concatenate([g_ref[i * count + c] for c in range(count)], axis=1)
        cat[pl.ds(pl.multiple_of(i * OUT_TILE, OUT_TILE), OUT_TILE), :] = dot(g, x_ref[...], (0, 0)).astype(BF16)
        return carry

    with jax.named_scope("de1"):
        lax.fori_loop(0, EARLY, item_grads, 0)

    with jax.named_scope("rswait"):
        arrive(pieces.at[others], 3)

    acc = pieces[0]
    for p in range(1, n):
        acc = acc + pieces[p]
    dx_ref[my_rows, :] = acc.astype(BF16)
    exchange(lambda p: dx_ref.at[my_rows], dx_ref.at[my_rows], 4)
    exchange(lambda p: targets.at[me], targets.at[me], 5)
    with jax.named_scope("de2"):
        lax.fori_loop(EARLY, items // OUT_TILE, item_grads, 0)

    with jax.named_scope("agwait"):
        arrive(dx_ref.at[other_rows], 4)

    arrive(targets.at[others], 5)
    target = targets[0, 0:1, :]
    for p in range(1, n):
        target = target + targets[p, 0:1, :]
    loss_ref[...] = jnp.broadcast_to(
        jnp.sum(big + jnp.log(total) - target, axis=1, keepdims=True) / rows, loss_ref.shape)
    with jax.named_scope("sendwait"):
        sent(lab.at[other_rows], 0)
        sent(q_ref.at[other_rows], 1)
        sent(stats.at[others], 2)
        sent(pieces.at[others], 3)
        sent(dx_ref.at[other_rows], 4)
        sent(targets.at[others], 5)


def grad_kernel(de_ref, dx_ref, h_ref, a_ref, q_ref, w2_ref, loss_ref,
                loss_hbm, de_hbm, dw1_hbm, dw2_hbm, loss, dw1, dw2, sem):
    copies = []
    for k in range(de_hbm.shape[0] // LOAD_TILE):
        at = pl.ds(k * LOAD_TILE, LOAD_TILE)
        pltpu.make_async_copy(de_ref.at[at], de_hbm.at[at], sem.at[3]).start()
    with jax.named_scope("bwd"):
        dx = dx_ref[...]
        dw2[...] = dot(h_ref[...], dx, (0, 0)).astype(BF16)
        dh = dot(dx, w2_ref[...], (1, 1))
        da = jnp.where(a_ref[...] > 0.0, dh, 0.0).astype(BF16)
        dw1[...] = dot(q_ref[...], da, (0, 0)).astype(BF16)
        loss[...] = loss_ref[0:1, 0:1]
        copies.append(pltpu.make_async_copy(loss, loss_hbm, sem.at[0]))
        copies.append(pltpu.make_async_copy(dw1, dw1_hbm, sem.at[1]))
        copies.append(pltpu.make_async_copy(dw2, dw2_hbm, sem.at[2]))
        for copy in copies[-3:]:
            copy.start()

    for copy in copies:
        copy.wait()
    pltpu.make_async_copy(de_ref, de_hbm, sem.at[3]).wait()


def solution(mesh):
    n = mesh.shape["tp"]

    def local_step(queries, w_first, w_second, catalogue, log_q, labels):
        own, d_in = queries.shape
        hid, emb = w_second.shape
        items = catalogue.shape[0]
        rows = own * n
        hbm = pl.BlockSpec(memory_space=pl.ANY)
        vmem = pl.BlockSpec(memory_space=pltpu.VMEM)
        dma = pltpu.SemaphoreType.DMA
        held = pl.pallas_call(
            functools.partial(loss_kernel, n),
            name="loss_kernel",
            out_shape=[
                pltpu.VMEM((items, emb), BF16),
                pltpu.VMEM((rows, emb), BF16),
                pltpu.VMEM((rows, hid), BF16),
                pltpu.VMEM((rows, hid), F32),
                pltpu.VMEM((rows, d_in), BF16),
                pltpu.VMEM((hid, emb), BF16),
                pltpu.VMEM((32, LANES), F32),
            ],
            in_specs=[hbm] * 6,
            out_specs=[vmem] * 7,
            scratch_shapes=[
                pltpu.VMEM((rows, emb), BF16),
                pltpu.VMEM((items // LANES, rows, LANES), BF16),
                pltpu.VMEM((items // LANES, rows, LANES), F32),
                pltpu.VMEM((TILE // LANES, rows, LANES), F32),
                pltpu.VMEM((TILE // LANES, rows, LANES), F32),
                pltpu.VMEM((1, items), F32),
                pltpu.VMEM((d_in, hid), BF16),
                pltpu.SMEM((own,), jnp.int32),
                pltpu.VMEM((rows, LANES), jnp.int32),
                pltpu.VMEM((rows, LANES), jnp.int32),
                pltpu.VMEM((rows, LANES), F32),
                pltpu.VMEM((rows, LANES), F32),
                pltpu.VMEM((rows, LANES), F32),
                pltpu.VMEM((items // TILE + 1, rows, LANES), F32),
                pltpu.VMEM((n, 8, LANES), F32),
                pltpu.VMEM((n, 8, LANES), F32),
                pltpu.VMEM((rows, emb), F32),
                pltpu.VMEM((n, own, emb), F32),
                dma((5,)),
                dma((items // LOAD_TILE,)),
                dma((6,)),
                dma((6,)),
            ],
            compiler_params=pltpu.CompilerParams(collective_id=0, has_side_effects=True, vmem_limit_bytes=44 << 20),
        )(queries, w_first, w_second, catalogue, log_q.reshape(1, items), labels)
        loss, grad_items, grad_first, grad_second = pl.pallas_call(
            grad_kernel,
            name="grad_kernel",
            out_shape=[
                jax.ShapeDtypeStruct((1, 1), F32),
                jax.ShapeDtypeStruct((items, emb), BF16),
                jax.ShapeDtypeStruct((d_in, hid), BF16),
                jax.ShapeDtypeStruct((hid, emb), BF16),
            ],
            in_specs=[vmem] * 7,
            out_specs=[hbm] * 4,
            scratch_shapes=[
                pltpu.VMEM((1, 1), F32),
                pltpu.VMEM((d_in, hid), BF16),
                pltpu.VMEM((hid, emb), BF16),
                dma((4,)),
            ],
            compiler_params=pltpu.CompilerParams(vmem_limit_bytes=24 << 20),
        )(*held)
        return loss.reshape(1), grad_items, grad_first, grad_second

    row_spec = P(("dp", "tp"), None)
    return jax.shard_map(
        local_step, mesh=mesh,
        in_specs=(row_spec, P(None, None), P(None, None), P("tp", None), P("tp"), P(("dp", "tp"))),
        out_specs=(P("dp"), row_spec, P("dp", None), P("dp", None)), check_vma=False)
```

```python
import functools

import jax
import jax.numpy as jnp
from jax import lax
from jax.experimental import pallas as pl
from jax.experimental.pallas import tpu as pltpu
from jax.sharding import PartitionSpec as P

F32, BF16 = jnp.float32, jnp.bfloat16
MESH = pl.DeviceIdType.MESH
LANES = 128
TILE = 4096
DOT_TILE = 512
GROUP = 16
SECOND_TILE = 8192
LOAD_TILE = 4096
OUT_TILE = 4096
OUT_SLOTS = 4
LOWEST = -3.0e38


def dot(a, b, contract):
    return lax.dot_general(a, b, ((contract[:1], contract[1:]), ((), ())), preferred_element_type=F32)


def loss_kernel(n, q_hbm, w1_hbm, w2_hbm, cat_hbm, lq_hbm, lab_hbm,
                g_ref, x_ref, h_ref, a_ref, q_ref, w2_ref, loss_ref, *rest):
    parts, rest = rest[:n], rest[n:]
    (cat, ez, z_even, z_odd, lq, w1, labels, lab, d, m_run, s_run, t_run, m_hist, stats, targets, part,
     load_sem, cat_sem, send_sem, recv_sem) = rest
    me = lax.axis_index("tp")
    own = q_hbm.shape[0]
    rows = own * n
    items = cat_hbm.shape[0]
    tiles = items // TILE
    chunks = TILE // LANES
    my_rows = pl.ds(pl.multiple_of(me * own, own), own)

    others = pl.ds(0, n - 1)
    other_rows = pl.ds(0, rows - own)

    q_load = pltpu.make_async_copy(q_hbm, q_ref.at[my_rows], load_sem.at[0])
    w1_load = pltpu.make_async_copy(w1_hbm, w1, load_sem.at[1])
    w2_load = pltpu.make_async_copy(w2_hbm, w2_ref, load_sem.at[2])
    lq_load = pltpu.make_async_copy(lq_hbm, lq, load_sem.at[3])
    lab_load = pltpu.make_async_copy(lab_hbm, labels, load_sem.at[4])
    barrier = pltpu.get_barrier_semaphore()
    peers = [lax.rem(me + k, n) for k in range(1, n)]
    for p in peers:
        pl.semaphore_signal(barrier, inc=1, device_id={"tp": p}, device_id_type=MESH)
    for load in (q_load, w1_load, w2_load, lq_load, lab_load):
        load.start()

    def cat_copy(k):
        part_rows = pl.ds(pl.multiple_of(k * LOAD_TILE, LOAD_TILE), LOAD_TILE)
        return pltpu.make_async_copy(cat_hbm.at[part_rows], cat.at[part_rows], cat_sem.at[k])

    pl.semaphore_wait(barrier, n - 1)

    def exchange(src, dst, stage):
        for p in peers:
            pltpu.make_async_remote_copy(
                src_ref=src(p), dst_ref=dst, send_sem=send_sem.at[stage], recv_sem=recv_sem.at[stage],
                device_id={"tp": p}, device_id_type=MESH).start()

    def arrive(others, stage):
        pltpu.make_async_copy(others, others, recv_sem.at[stage]).wait()

    def sent(others, stage):
        pltpu.make_async_copy(others, others, send_sem.at[stage]).wait()

    def rows_of(p):
        return pl.ds(pl.multiple_of(p * own, own), own)

    q_load.wait()
    exchange(lambda p: q_ref.at[my_rows], q_ref.at[my_rows], 1)
    w1_load.wait()
    w2_load.wait()
    lq_load.wait()
    for k in range(items // LOAD_TILE):
        cat_copy(k).start()
    lab_load.wait()
    for r in range(own):
        lab[pl.ds(me * own + r, 1), :] = jnp.full((1, LANES), labels[r], jnp.int32)
    m_run[...] = jnp.full(m_run.shape, LOWEST, F32)
    s_run[...] = jnp.zeros(s_run.shape, F32)
    part[...] = jnp.zeros(part.shape, F32)
    exchange(lambda p: lab.at[my_rows], lab.at[my_rows], 0)
    arrive(q_ref.at[other_rows], 1)

    a = dot(q_ref[...], w1[...], (1, 0))
    a_ref[...] = a
    h_ref[...] = jnp.maximum(a, 0.0).astype(BF16)
    x_ref[...] = dot(h_ref[...], w2_ref[...], (1, 0)).astype(BF16)
    arrive(lab.at[other_rows], 0)
    local = lab[...] - me * items
    lane = lax.broadcasted_iota(jnp.int32, lab.shape, 1)
    d[...] = local - lane

    def logits(i, z_ref):
        for j in range(TILE // DOT_TILE):
            base = pl.multiple_of(i * TILE + j * DOT_TILE, DOT_TILE)
            z = dot(x_ref[...], cat[pl.ds(base, DOT_TILE), :], (1, 1)) - lq[:, pl.ds(base, DOT_TILE)]
            m = m_run[...]
            for c in range(DOT_TILE // LANES):
                zc = z[:, c * LANES:(c + 1) * LANES]
                z_ref[j * (DOT_TILE // LANES) + c] = zc
                ez[i * chunks + j * (DOT_TILE // LANES) + c] = zc
                m = jnp.maximum(m, zc)
            m_run[...] = m
            yield
        m_hist[i + 1] = m

    def weigh(i, z_ref):
        for r in range(0, rows, GROUP):
            at = slice(r, r + GROUP)
            m = m_hist[i + 1, at, :]
            s = s_run[at, :] * jnp.exp(m_hist[i, at, :] - m)
            for c in range(chunks):
                s = s + jnp.exp(z_ref[c, at, :] - m)
            s_run[at, :] = s
            yield

    def arrived(i):
        for j in range(TILE // LOAD_TILE):
            cat_copy(i * (TILE // LOAD_TILE) + j).wait()

    def together(*parts):
        parts = list(parts)
        while parts:
            parts = [p for p in parts if next(p, parts) is not parts]

    m_hist[0] = m_run[...]
    arrived(0)
    together(logits(0, z_even))

    def first_pass(j, carry):
        arrived(2 * j + 1)
        arrived(2 * j + 2)
        together(logits(2 * j + 1, z_odd), weigh(2 * j, z_even))
        together(logits(2 * j + 2, z_even), weigh(2 * j + 1, z_odd))
        return carry

    lax.fori_loop(0, tiles // 2 - 1, first_pass, 0)
    arrived(tiles - 1)
    together(logits(tiles - 1, z_odd), weigh(tiles - 2, z_even))
    together(weigh(tiles - 1, z_odd))

    m_t = m_run[...].T
    m_row = jnp.max(m_t, axis=0, keepdims=True)
    s_row = jnp.sum(s_run[...].T * jnp.exp(m_t - m_row), axis=0, keepdims=True)
    sub = lax.broadcasted_iota(jnp.int32, (8, LANES), 0)
    stats[me] = jnp.where(sub == 0, m_row, s_row)
    exchange(lambda p: stats.at[me], stats.at[me], 2)
    t_run[...] = jnp.zeros(t_run.shape, F32)

    def weights(i, carry):
        for r in range(0, rows, GROUP):
            at = slice(r, r + GROUP)
            m = m_run[at, :]
            t = t_run[at, :]
            dd = d[at, :] - i * TILE
            for c in range(chunks):
                zc = ez[i * chunks + c, at, :]
                t = jnp.where(dd == c * LANES, zc, t)
                ez[i * chunks + c, at, :] = jnp.exp(zc - m)
            t_run[at, :] = t
        return carry

    lax.fori_loop(0, tiles, weights, 0)
    t_col = jnp.broadcast_to(jnp.sum(t_run[...], axis=1, keepdims=True), lab.shape)
    targets[me] = t_col.T[0:8, :]
    exchange(lambda p: targets.at[me], targets.at[me], 3)
    arrive(stats.at[others], 2)
    big = stats[0, 0:1, :]
    for p in range(1, n):
        big = jnp.maximum(big, stats[p, 0:1, :])
    total = jnp.zeros_like(big)
    for p in range(n):
        total = total + stats[p, 1:2, :] * jnp.exp(stats[p, 0:1, :] - big)
    inv = 1.0 / (total * rows)
    big_col = jnp.broadcast_to(big, (rows, LANES)).T
    inv_col = jnp.broadcast_to(inv, (rows, LANES)).T
    hit_col = (jnp.exp(t_col - big_col) * inv_col - 1.0 / rows).astype(BF16)
    scale = jnp.exp(m_run[...] - big_col) * inv_col
    home = jnp.where(local - local // LANES * LANES == lane, local // LANES, -1)
    home = jnp.where((local >= 0) & (local < items), home, -1).astype(F32)

    def second_pass(i, carry):
        gs = []
        for f in range(SECOND_TILE // TILE):
            tile = i * (SECOND_TILE // TILE) + f
            here = (home - (tile * chunks).astype(F32)).astype(BF16)
            for c in range(chunks):
                g = (ez[tile * chunks + c] * scale).astype(BF16)
                g = jnp.where(here == jnp.bfloat16(c), hit_col, g)
                g_ref[tile * chunks + c] = g
                gs.append(g)
        base = pl.multiple_of(i * SECOND_TILE, SECOND_TILE)
        part[...] += dot(jnp.concatenate(gs, axis=1), cat[pl.ds(base, SECOND_TILE), :], (1, 0))
        return carry

    lax.fori_loop(0, items // SECOND_TILE, second_pass, 0)

    parts[0][...] = part[my_rows, :]
    for k, p in enumerate(peers):
        parts[k + 1][...] = part[rows_of(p), :]
    arrive(targets.at[others], 3)
    target = targets[0, 0:1, :]
    for p in range(1, n):
        target = target + targets[p, 0:1, :]
    loss_ref[...] = jnp.broadcast_to(
        jnp.sum(big + jnp.log(total) - target, axis=1, keepdims=True) / rows, loss_ref.shape)
    sent(lab.at[other_rows], 0)
    sent(q_ref.at[other_rows], 1)
    sent(stats.at[others], 2)
    sent(targets.at[others], 3)


def items_kernel(first, g_ref, x_ref, after_ref, de_in, de_hbm, stage, out_sem):
    steps = de_hbm.shape[0] // OUT_TILE // 2
    count = OUT_TILE // LANES
    start = first * steps

    def out_copy(i, slot):
        at = pl.ds(pl.multiple_of((start + i) * OUT_TILE, OUT_TILE), OUT_TILE)
        return pltpu.make_async_copy(stage.at[slot], de_hbm.at[at], out_sem.at[slot])

    for i in range(steps):
        slot = i % OUT_SLOTS
        if i >= OUT_SLOTS:
            out_copy(i - OUT_SLOTS, slot).wait()
        g = jnp.concatenate([g_ref[(start + i) * count + c] for c in range(count)], axis=1)
        stage[slot] = dot(g, x_ref[...], (0, 0)).astype(BF16)
        out_copy(i, slot).start()
    for i in range(max(steps - OUT_SLOTS, 0), steps):
        out_copy(i, i % OUT_SLOTS).wait()


def sum_kernel(*refs):
    acc = refs[0][...]
    for ref in refs[1:-1]:
        acc = acc + ref[...]
    refs[-1][...] = acc.astype(BF16)


def tower_kernel(n, *refs):
    pieces, refs = refs[:n], refs[n:]
    h_ref, a_ref, q_ref, w2_ref, loss_ref, loss_hbm, dw1_hbm, dw2_hbm, dx_ref, loss, dw1, dw2, sem = refs
    me = lax.axis_index("tp")
    own = pieces[0].shape[0]
    loss[...] = loss_ref[0:1, 0:1]
    copies = [pltpu.make_async_copy(loss, loss_hbm, sem.at[0]),
              pltpu.make_async_copy(dw1, dw1_hbm, sem.at[1]),
              pltpu.make_async_copy(dw2, dw2_hbm, sem.at[2])]
    copies[0].start()
    for k in range(n):
        p = lax.rem(me + n - k, n)
        dx_ref[pl.ds(pl.multiple_of(p * own, own), own), :] = pieces[k][...]
    dx = dx_ref[...]
    dw2[...] = dot(h_ref[...], dx, (0, 0)).astype(BF16)
    copies[2].start()
    dh = dot(dx, w2_ref[...], (1, 1))
    da = jnp.where(a_ref[...] > 0.0, dh, 0.0).astype(BF16)
    dw1[...] = dot(q_ref[...], da, (0, 0)).astype(BF16)
    copies[1].start()
    for copy in copies:
        copy.wait()


def solution(mesh):
    n = mesh.shape["tp"]

    def local_step(queries, w_first, w_second, catalogue, log_q, labels):
        own, d_in = queries.shape
        hid, emb = w_second.shape
        items = catalogue.shape[0]
        rows = own * n
        hbm = pl.BlockSpec(memory_space=pl.ANY)
        vmem = pl.BlockSpec(memory_space=pltpu.VMEM)
        dma = pltpu.SemaphoreType.DMA
        g, x, h, a, q, w2, loss_rows, *parts = pl.pallas_call(
            functools.partial(loss_kernel, n),
            name="loss_kernel",
            out_shape=[
                pltpu.VMEM((items // LANES, rows, LANES), BF16),
                pltpu.VMEM((rows, emb), BF16),
                pltpu.VMEM((rows, hid), BF16),
                pltpu.VMEM((rows, hid), F32),
                pltpu.VMEM((rows, d_in), BF16),
                pltpu.VMEM((hid, emb), BF16),
                pltpu.VMEM((32, LANES), F32),
            ] + [pltpu.VMEM((own, emb), F32)] * n,
            in_specs=[hbm] * 6,
            out_specs=[vmem] * (7 + n),
            scratch_shapes=[
                pltpu.VMEM((items, emb), BF16),
                pltpu.VMEM((items // LANES, rows, LANES), F32),
                pltpu.VMEM((TILE // LANES, rows, LANES), F32),
                pltpu.VMEM((TILE // LANES, rows, LANES), F32),
                pltpu.VMEM((1, items), F32),
                pltpu.VMEM((d_in, hid), BF16),
                pltpu.SMEM((own,), jnp.int32),
                pltpu.VMEM((rows, LANES), jnp.int32),
                pltpu.VMEM((rows, LANES), jnp.int32),
                pltpu.VMEM((rows, LANES), F32),
                pltpu.VMEM((rows, LANES), F32),
                pltpu.VMEM((rows, LANES), F32),
                pltpu.VMEM((items // TILE + 1, rows, LANES), F32),
                pltpu.VMEM((n, 8, LANES), F32),
                pltpu.VMEM((n, 8, LANES), F32),
                pltpu.VMEM((rows, emb), F32),
                dma((5,)),
                dma((items // LOAD_TILE,)),
                dma((4,)),
                dma((4,)),
            ],
            compiler_params=pltpu.CompilerParams(collective_id=0, has_side_effects=True, vmem_limit_bytes=50 << 20),
        )(queries, w_first, w_second, catalogue, log_q.reshape(1, items), labels)

        def spread(pieces):
            return [pieces[0]] + [lax.ppermute(pieces[k], "tp", [(i, (i + k) % n) for i in range(n)]) for k in range(1, n)]

        half_cost = pl.CostEstimate(flops=rows * items * emb, bytes_accessed=items * emb, transcendentals=0)

        def item_grads(first, after, de):
            return pl.pallas_call(
                functools.partial(items_kernel, first),
                name=("items_front", "items_back")[first],
                out_shape=jax.ShapeDtypeStruct((items, emb), BF16),
                in_specs=[vmem, vmem, vmem, hbm],
                out_specs=hbm,
                input_output_aliases={3: 0} if first else {},
                scratch_shapes=[pltpu.VMEM((OUT_SLOTS, OUT_TILE, emb), BF16), dma((OUT_SLOTS,))],
                cost_estimate=half_cost,
                compiler_params=pltpu.CompilerParams(vmem_limit_bytes=24 << 20),
            )(g, x, after, de)

        grad_items = item_grads(0, x, x)
        landed = spread(parts)
        grad_own = pl.pallas_call(
            sum_kernel,
            name="sum_kernel",
            out_shape=jax.ShapeDtypeStruct((own, emb), BF16),
            in_specs=[vmem] * n,
            out_specs=vmem,
            compiler_params=pltpu.CompilerParams(vmem_limit_bytes=4 << 20),
        )(*landed)
        grad_items = item_grads(1, grad_own, grad_items)
        loss, grad_first, grad_second = pl.pallas_call(
            functools.partial(tower_kernel, n),
            name="tower_kernel",
            out_shape=[
                jax.ShapeDtypeStruct((1, 1), F32),
                jax.ShapeDtypeStruct((d_in, hid), BF16),
                jax.ShapeDtypeStruct((hid, emb), BF16),
            ],
            in_specs=[vmem] * (n + 5),
            out_specs=[hbm] * 3,
            scratch_shapes=[
                pltpu.VMEM((rows, emb), BF16),
                pltpu.VMEM((1, 1), F32),
                pltpu.VMEM((d_in, hid), BF16),
                pltpu.VMEM((hid, emb), BF16),
                dma((3,)),
            ],
            compiler_params=pltpu.CompilerParams(vmem_limit_bytes=24 << 20),
        )(*spread([grad_own] * n), h, a, q, w2, loss_rows)
        return loss.reshape(1), grad_items, grad_first, grad_second

    row_spec = P(("dp", "tp"), None)
    return jax.shard_map(
        local_step, mesh=mesh,
        in_specs=(row_spec, P(None, None), P(None, None), P("tp", None), P("tp"), P(("dp", "tp"))),
        out_specs=(P("dp"), row_spec, P("dp", None), P("dp", None)), check_vma=False)
```

```python
import functools

import jax
import jax.numpy as jnp
from jax import lax
from jax.experimental import pallas as pl
from jax.experimental.pallas import tpu as pltpu
from jax.sharding import PartitionSpec as P

F32, BF16 = jnp.float32, jnp.bfloat16
MESH = pl.DeviceIdType.MESH
LANES = 128
TILE = 4096
DOT_TILE = 512
GROUP = 16
SECOND_TILE = 8192
LOAD_TILE = 4096
OUT_TILE = 4096
OUT_SLOTS = 4
LOWEST = -3.0e38


def dot(a, b, contract):
    return lax.dot_general(a, b, ((contract[:1], contract[1:]), ((), ())), preferred_element_type=F32)


def loss_kernel(n, q_hbm, w1_hbm, w2_hbm, cat_hbm, lq_hbm, lab_hbm,
                g_ref, x_ref, h_ref, a_ref, q_ref, w2_ref, loss_ref, *rest):
    parts, rest = rest[0], rest[1:]
    (cat, ez, z_even, z_odd, lq, w1, labels, lab, d, m_run, s_run, t_run, m_hist, stats, targets, part,
     load_sem, cat_sem, send_sem, recv_sem) = rest
    me = lax.axis_index("tp")
    own = q_hbm.shape[0]
    rows = own * n
    items = cat_hbm.shape[0]
    tiles = items // TILE
    chunks = TILE // LANES
    my_rows = pl.ds(pl.multiple_of(me * own, own), own)

    others = pl.ds(0, n - 1)
    other_rows = pl.ds(0, rows - own)

    q_load = pltpu.make_async_copy(q_hbm, q_ref.at[my_rows], load_sem.at[0])
    w1_load = pltpu.make_async_copy(w1_hbm, w1, load_sem.at[1])
    w2_load = pltpu.make_async_copy(w2_hbm, w2_ref, load_sem.at[2])
    lq_load = pltpu.make_async_copy(lq_hbm, lq, load_sem.at[3])
    lab_load = pltpu.make_async_copy(lab_hbm, labels, load_sem.at[4])
    barrier = pltpu.get_barrier_semaphore()
    peers = [lax.rem(me + k, n) for k in range(1, n)]
    for p in peers:
        pl.semaphore_signal(barrier, inc=1, device_id={"tp": p}, device_id_type=MESH)
    for load in (q_load, w1_load, w2_load, lq_load, lab_load):
        load.start()

    def cat_copy(k):
        part_rows = pl.ds(pl.multiple_of(k * LOAD_TILE, LOAD_TILE), LOAD_TILE)
        return pltpu.make_async_copy(cat_hbm.at[part_rows], cat.at[part_rows], cat_sem.at[k])

    pl.semaphore_wait(barrier, n - 1)

    def exchange(src, dst, stage):
        for p in peers:
            pltpu.make_async_remote_copy(
                src_ref=src(p), dst_ref=dst, send_sem=send_sem.at[stage], recv_sem=recv_sem.at[stage],
                device_id={"tp": p}, device_id_type=MESH).start()

    def arrive(others, stage):
        pltpu.make_async_copy(others, others, recv_sem.at[stage]).wait()

    def sent(others, stage):
        pltpu.make_async_copy(others, others, send_sem.at[stage]).wait()

    def rows_of(p):
        return pl.ds(pl.multiple_of(p * own, own), own)

    q_load.wait()
    exchange(lambda p: q_ref.at[my_rows], q_ref.at[my_rows], 1)
    w1_load.wait()
    w2_load.wait()
    lq_load.wait()
    for k in range(items // LOAD_TILE):
        cat_copy(k).start()
    lab_load.wait()
    for r in range(own):
        lab[pl.ds(me * own + r, 1), :] = jnp.full((1, LANES), labels[r], jnp.int32)
    m_run[...] = jnp.full(m_run.shape, LOWEST, F32)
    s_run[...] = jnp.zeros(s_run.shape, F32)
    part[...] = jnp.zeros(part.shape, F32)
    exchange(lambda p: lab.at[my_rows], lab.at[my_rows], 0)
    arrive(q_ref.at[other_rows], 1)

    a = dot(q_ref[...], w1[...], (1, 0))
    a_ref[...] = a
    h_ref[...] = jnp.maximum(a, 0.0).astype(BF16)
    x_ref[...] = dot(h_ref[...], w2_ref[...], (1, 0)).astype(BF16)
    arrive(lab.at[other_rows], 0)
    local = lab[...] - me * items
    lane = lax.broadcasted_iota(jnp.int32, lab.shape, 1)
    d[...] = local - lane

    def logits(i, z_ref):
        for j in range(TILE // DOT_TILE):
            base = pl.multiple_of(i * TILE + j * DOT_TILE, DOT_TILE)
            z = dot(x_ref[...], cat[pl.ds(base, DOT_TILE), :], (1, 1)) - lq[:, pl.ds(base, DOT_TILE)]
            m = m_run[...]
            for c in range(DOT_TILE // LANES):
                zc = z[:, c * LANES:(c + 1) * LANES]
                z_ref[j * (DOT_TILE // LANES) + c] = zc
                ez[i * chunks + j * (DOT_TILE // LANES) + c] = zc
                m = jnp.maximum(m, zc)
            m_run[...] = m
            yield
        m_hist[i + 1] = m

    def weigh(i, z_ref):
        for r in range(0, rows, GROUP):
            at = slice(r, r + GROUP)
            m = m_hist[i + 1, at, :]
            s = s_run[at, :] * jnp.exp(m_hist[i, at, :] - m)
            for c in range(chunks):
                s = s + jnp.exp(z_ref[c, at, :] - m)
            s_run[at, :] = s
            yield

    def arrived(i):
        for j in range(TILE // LOAD_TILE):
            cat_copy(i * (TILE // LOAD_TILE) + j).wait()

    def together(*parts):
        parts = list(parts)
        while parts:
            parts = [p for p in parts if next(p, parts) is not parts]

    m_hist[0] = m_run[...]
    arrived(0)
    together(logits(0, z_even))

    def first_pass(j, carry):
        arrived(2 * j + 1)
        arrived(2 * j + 2)
        together(logits(2 * j + 1, z_odd), weigh(2 * j, z_even))
        together(logits(2 * j + 2, z_even), weigh(2 * j + 1, z_odd))
        return carry

    lax.fori_loop(0, tiles // 2 - 1, first_pass, 0)
    arrived(tiles - 1)
    together(logits(tiles - 1, z_odd), weigh(tiles - 2, z_even))
    together(weigh(tiles - 1, z_odd))

    m_t = m_run[...].T
    m_row = jnp.max(m_t, axis=0, keepdims=True)
    s_row = jnp.sum(s_run[...].T * jnp.exp(m_t - m_row), axis=0, keepdims=True)
    sub = lax.broadcasted_iota(jnp.int32, (8, LANES), 0)
    stats[me] = jnp.where(sub == 0, m_row, s_row)
    exchange(lambda p: stats.at[me], stats.at[me], 2)
    t_run[...] = jnp.zeros(t_run.shape, F32)

    def weights(i, carry):
        for r in range(0, rows, GROUP):
            at = slice(r, r + GROUP)
            m = m_run[at, :]
            t = t_run[at, :]
            dd = d[at, :] - i * TILE
            for c in range(chunks):
                zc = ez[i * chunks + c, at, :]
                t = jnp.where(dd == c * LANES, zc, t)
                ez[i * chunks + c, at, :] = jnp.exp(zc - m)
            t_run[at, :] = t
        return carry

    lax.fori_loop(0, tiles, weights, 0)
    t_col = jnp.broadcast_to(jnp.sum(t_run[...], axis=1, keepdims=True), lab.shape)
    targets[me] = t_col.T[0:8, :]
    exchange(lambda p: targets.at[me], targets.at[me], 3)
    arrive(stats.at[others], 2)
    big = stats[0, 0:1, :]
    for p in range(1, n):
        big = jnp.maximum(big, stats[p, 0:1, :])
    total = jnp.zeros_like(big)
    for p in range(n):
        total = total + stats[p, 1:2, :] * jnp.exp(stats[p, 0:1, :] - big)
    inv = 1.0 / (total * rows)
    big_col = jnp.broadcast_to(big, (rows, LANES)).T
    inv_col = jnp.broadcast_to(inv, (rows, LANES)).T
    hit_col = (jnp.exp(t_col - big_col) * inv_col - 1.0 / rows).astype(BF16)
    scale = jnp.exp(m_run[...] - big_col) * inv_col
    home = jnp.where(local - local // LANES * LANES == lane, local // LANES, -1)
    home = jnp.where((local >= 0) & (local < items), home, -1).astype(F32)

    def second_pass(i, carry):
        gs = []
        for f in range(SECOND_TILE // TILE):
            tile = i * (SECOND_TILE // TILE) + f
            here = (home - (tile * chunks).astype(F32)).astype(BF16)
            for c in range(chunks):
                g = (ez[tile * chunks + c] * scale).astype(BF16)
                g = jnp.where(here == jnp.bfloat16(c), hit_col, g)
                g_ref[tile * chunks + c] = g
                gs.append(g)
        base = pl.multiple_of(i * SECOND_TILE, SECOND_TILE)
        part[...] += dot(jnp.concatenate(gs, axis=1), cat[pl.ds(base, SECOND_TILE), :], (1, 0))
        return carry

    lax.fori_loop(0, items // SECOND_TILE, second_pass, 0)

    parts[...] = part[...]
    arrive(targets.at[others], 3)
    target = targets[0, 0:1, :]
    for p in range(1, n):
        target = target + targets[p, 0:1, :]
    loss_ref[...] = jnp.broadcast_to(
        jnp.sum(big + jnp.log(total) - target, axis=1, keepdims=True) / rows, loss_ref.shape)
    sent(lab.at[other_rows], 0)
    sent(q_ref.at[other_rows], 1)
    sent(stats.at[others], 2)
    sent(targets.at[others], 3)


def items_kernel(first, g_ref, x_ref, after_ref, de_in, de_hbm, stage, out_sem):
    steps = de_hbm.shape[0] // OUT_TILE // 2
    count = OUT_TILE // LANES
    start = first * steps

    def out_copy(i, slot):
        at = pl.ds(pl.multiple_of((start + i) * OUT_TILE, OUT_TILE), OUT_TILE)
        return pltpu.make_async_copy(stage.at[slot], de_hbm.at[at], out_sem.at[slot])

    for i in range(steps):
        slot = i % OUT_SLOTS
        if i >= OUT_SLOTS:
            out_copy(i - OUT_SLOTS, slot).wait()
        g = jnp.concatenate([g_ref[(start + i) * count + c] for c in range(count)], axis=1)
        stage[slot] = dot(g, x_ref[...], (0, 0)).astype(BF16)
        out_copy(i, slot).start()
    for i in range(max(steps - OUT_SLOTS, 0), steps):
        out_copy(i, i % OUT_SLOTS).wait()


def sum_kernel(n, pieces, out):
    own = pieces.shape[0] // n
    acc = pieces[0:own, :]
    for k in range(1, n):
        acc = acc + pieces[k * own:(k + 1) * own, :]
    for k in range(n):
        out[k * own:(k + 1) * own, :] = acc.astype(BF16)


def tower_kernel(n, *refs):
    dx_all, refs = refs[0], refs[1:]
    h_ref, a_ref, q_ref, w2_ref, loss_ref, loss_hbm, dw1_hbm, dw2_hbm, dx_ref, loss, dw1, dw2, sem = refs
    me = lax.axis_index("tp")
    loss[...] = loss_ref[0:1, 0:1]
    copies = [pltpu.make_async_copy(loss, loss_hbm, sem.at[0]),
              pltpu.make_async_copy(dw1, dw1_hbm, sem.at[1]),
              pltpu.make_async_copy(dw2, dw2_hbm, sem.at[2])]
    copies[0].start()
    dx = dx_all[...]
    dw2[...] = dot(h_ref[...], dx, (0, 0)).astype(BF16)
    copies[2].start()
    dh = dot(dx, w2_ref[...], (1, 1))
    da = jnp.where(a_ref[...] > 0.0, dh, 0.0).astype(BF16)
    dw1[...] = dot(q_ref[...], da, (0, 0)).astype(BF16)
    copies[1].start()
    for copy in copies:
        copy.wait()


def solution(mesh):
    n = mesh.shape["tp"]

    def local_step(queries, w_first, w_second, catalogue, log_q, labels):
        own, d_in = queries.shape
        hid, emb = w_second.shape
        items = catalogue.shape[0]
        rows = own * n
        hbm = pl.BlockSpec(memory_space=pl.ANY)
        vmem = pl.BlockSpec(memory_space=pltpu.VMEM)
        dma = pltpu.SemaphoreType.DMA
        g, x, h, a, q, w2, loss_rows, parts = pl.pallas_call(
            functools.partial(loss_kernel, n),
            name="loss_kernel",
            out_shape=[
                pltpu.VMEM((items // LANES, rows, LANES), BF16),
                pltpu.VMEM((rows, emb), BF16),
                pltpu.VMEM((rows, hid), BF16),
                pltpu.VMEM((rows, hid), F32),
                pltpu.VMEM((rows, d_in), BF16),
                pltpu.VMEM((hid, emb), BF16),
                pltpu.VMEM((32, LANES), F32),
            ] + [jax.ShapeDtypeStruct((rows, emb), F32)],
            in_specs=[hbm] * 6,
            out_specs=[vmem] * 8,
            scratch_shapes=[
                pltpu.VMEM((items, emb), BF16),
                pltpu.VMEM((items // LANES, rows, LANES), F32),
                pltpu.VMEM((TILE // LANES, rows, LANES), F32),
                pltpu.VMEM((TILE // LANES, rows, LANES), F32),
                pltpu.VMEM((1, items), F32),
                pltpu.VMEM((d_in, hid), BF16),
                pltpu.SMEM((own,), jnp.int32),
                pltpu.VMEM((rows, LANES), jnp.int32),
                pltpu.VMEM((rows, LANES), jnp.int32),
                pltpu.VMEM((rows, LANES), F32),
                pltpu.VMEM((rows, LANES), F32),
                pltpu.VMEM((rows, LANES), F32),
                pltpu.VMEM((items // TILE + 1, rows, LANES), F32),
                pltpu.VMEM((n, 8, LANES), F32),
                pltpu.VMEM((n, 8, LANES), F32),
                pltpu.VMEM((rows, emb), F32),
                dma((5,)),
                dma((items // LOAD_TILE,)),
                dma((4,)),
                dma((4,)),
            ],
            compiler_params=pltpu.CompilerParams(collective_id=0, has_side_effects=True, vmem_limit_bytes=50 << 20),
        )(queries, w_first, w_second, catalogue, log_q.reshape(1, items), labels)

        def spread(pieces):
            return [pieces[0]] + [lax.ppermute(pieces[k], "tp", [(i, (i + k) % n) for i in range(n)]) for k in range(1, n)]

        half_cost = pl.CostEstimate(flops=rows * items * emb, bytes_accessed=items * emb, transcendentals=0)

        def item_grads(first, after, de):
            return pl.pallas_call(
                functools.partial(items_kernel, first),
                name=("items_front", "items_back")[first],
                out_shape=jax.ShapeDtypeStruct((items, emb), BF16),
                in_specs=[vmem, vmem, vmem, hbm],
                out_specs=hbm,
                input_output_aliases={3: 0} if first else {},
                scratch_shapes=[pltpu.VMEM((OUT_SLOTS, OUT_TILE, emb), BF16), dma((OUT_SLOTS,))],
                cost_estimate=half_cost,
                compiler_params=pltpu.CompilerParams(vmem_limit_bytes=24 << 20),
            )(g, x, after, de)

        grad_items = item_grads(0, x, x)
        landed = [lax.all_to_all(parts, "tp", 0, 0, tiled=True)]
        grad_own = pl.pallas_call(
            functools.partial(sum_kernel, n),
            name="sum_kernel",
            out_shape=jax.ShapeDtypeStruct((rows, emb), BF16),
            in_specs=[vmem],
            out_specs=vmem,
            compiler_params=pltpu.CompilerParams(vmem_limit_bytes=4 << 20),
        )(*landed)
        grad_items = item_grads(1, grad_own, grad_items)
        loss, grad_first, grad_second = pl.pallas_call(
            functools.partial(tower_kernel, n),
            name="tower_kernel",
            out_shape=[
                jax.ShapeDtypeStruct((1, 1), F32),
                jax.ShapeDtypeStruct((d_in, hid), BF16),
                jax.ShapeDtypeStruct((hid, emb), BF16),
            ],
            in_specs=[vmem] * 6,
            out_specs=[hbm] * 3,
            scratch_shapes=[
                pltpu.VMEM((rows, emb), BF16),
                pltpu.VMEM((1, 1), F32),
                pltpu.VMEM((d_in, hid), BF16),
                pltpu.VMEM((hid, emb), BF16),
                dma((3,)),
            ],
            compiler_params=pltpu.CompilerParams(vmem_limit_bytes=24 << 20),
        )(lax.all_to_all(grad_own, "tp", 0, 0, tiled=True), h, a, q, w2, loss_rows)
        return loss.reshape(1), grad_items, grad_first, grad_second

    row_spec = P(("dp", "tp"), None)
    return jax.shard_map(
        local_step, mesh=mesh,
        in_specs=(row_spec, P(None, None), P(None, None), P("tp", None), P("tp"), P(("dp", "tp"))),
        out_specs=(P("dp"), row_spec, P("dp", None), P("dp", None)), check_vma=False)
```

```python
import functools

import jax
import jax.numpy as jnp
from jax import lax
from jax.experimental import pallas as pl
from jax.experimental.pallas import tpu as pltpu
from jax.sharding import PartitionSpec as P

F32, BF16 = jnp.float32, jnp.bfloat16
MESH = pl.DeviceIdType.MESH
LANES = 128
TILE = 2048
UNROLL = 4
DOT_TILE = 512
GROUP = 32
WEIGHT_TILE = 4096
WEIGHT_GROUP = 16
SECOND_TILE = 8192
LOAD_TILE = 4096
OUT_TILE = 4096
EARLY = 5
LOWEST = -3.0e38


def dot(a, b, contract):
    return lax.dot_general(a, b, ((contract[:1], contract[1:]), ((), ())), preferred_element_type=F32)


def loss_kernel(n, q_hbm, w1_hbm, w2_hbm, cat_hbm, lq_hbm, lab_hbm,
                cat, dx_ref, h_ref, a_ref, q_ref, w2_ref, loss_ref,
                x_ref, g_ref, ez, z_even, z_odd, lq, w1, labels, lab, d, m_run, s_run, t_run, m_hist, stats, targets, part, pieces,
                load_sem, cat_sem, send_sem, recv_sem):
    me = lax.axis_index("tp")
    own = q_hbm.shape[0]
    rows = own * n
    items = cat_hbm.shape[0]
    tiles = items // TILE
    chunks = TILE // LANES
    my_rows = pl.ds(pl.multiple_of(me * own, own), own)

    others = pl.ds(0, n - 1)
    other_rows = pl.ds(0, rows - own)

    q_load = pltpu.make_async_copy(q_hbm, q_ref.at[my_rows], load_sem.at[0])
    w1_load = pltpu.make_async_copy(w1_hbm, w1, load_sem.at[1])
    w2_load = pltpu.make_async_copy(w2_hbm, w2_ref, load_sem.at[2])
    lq_load = pltpu.make_async_copy(lq_hbm, lq, load_sem.at[3])
    lab_load = pltpu.make_async_copy(lab_hbm, labels, load_sem.at[4])
    for load in (q_load, w1_load, w2_load):
        load.start()
    barrier = pltpu.get_barrier_semaphore()
    peers = [lax.rem(me + k, n) for k in range(1, n)]
    for p in peers:
        pl.semaphore_signal(barrier, inc=1, device_id={"tp": p}, device_id_type=MESH)
    for load in (lq_load, lab_load):
        load.start()

    def cat_copy(k):
        part_rows = pl.ds(pl.multiple_of(k * LOAD_TILE, LOAD_TILE), LOAD_TILE)
        return pltpu.make_async_copy(cat_hbm.at[part_rows], cat.at[part_rows], cat_sem.at[k])

    q_load.wait()
    w1_load.wait()
    w2_load.wait()
    for k in range(items // LOAD_TILE):
        cat_copy(k).start()
    own_hidden = jnp.maximum(dot(q_ref[my_rows, :], w1[...], (1, 0)), 0.0).astype(BF16)
    x_ref[my_rows, :] = dot(own_hidden, w2_ref[...], (1, 0)).astype(BF16)
    with jax.named_scope("bar"):
        pl.semaphore_wait(barrier, n - 1)

    def exchange(src, dst, stage):
        for p in peers:
            pltpu.make_async_remote_copy(
                src_ref=src(p), dst_ref=dst, send_sem=send_sem.at[stage], recv_sem=recv_sem.at[stage],
                device_id={"tp": p}, device_id_type=MESH).start()

    def arrive(others, stage):
        pltpu.make_async_copy(others, others, recv_sem.at[stage]).wait()

    def sent(others, stage):
        pltpu.make_async_copy(others, others, send_sem.at[stage]).wait()

    def rows_of(p):
        return pl.ds(pl.multiple_of(p * own, own), own)

    exchange(lambda p: x_ref.at[my_rows], x_ref.at[my_rows], 1)
    exchange(lambda p: q_ref.at[my_rows], q_ref.at[my_rows], 6)
    lq_load.wait()
    lab_load.wait()
    for r in range(own):
        lab[pl.ds(me * own + r, 1), :] = jnp.full((1, LANES), labels[r], jnp.int32)
    m_run[...] = jnp.full(m_run.shape, LOWEST, F32)
    s_run[...] = jnp.zeros(s_run.shape, F32)
    part[...] = jnp.zeros(part.shape, F32)
    exchange(lambda p: lab.at[my_rows], lab.at[my_rows], 0)
    with jax.named_scope("xgather"):
        arrive(x_ref.at[other_rows], 1)

    def logits(i, z_ref):
        for j in range(TILE // DOT_TILE):
            base = pl.multiple_of(i * TILE + j * DOT_TILE, DOT_TILE)
            z = dot(x_ref[...], cat[pl.ds(base, DOT_TILE), :], (1, 1)) - lq[:, pl.ds(base, DOT_TILE)]
            m = m_run[...]
            for c in range(DOT_TILE // LANES):
                zc = z[:, c * LANES:(c + 1) * LANES]
                z_ref[j * (DOT_TILE // LANES) + c] = zc
                ez[i * chunks + j * (DOT_TILE // LANES) + c] = zc
                m = jnp.maximum(m, zc)
            m_run[...] = m
            yield
        m_hist[i + 1] = m

    def weigh(i, z_ref):
        for r in range(0, rows, GROUP):
            at = slice(r, r + GROUP)
            m = m_hist[i + 1, at, :]
            s = s_run[at, :] * jnp.exp(m_hist[i, at, :] - m)
            for c in range(chunks):
                s = s + jnp.exp(z_ref[c, at, :] - m)
            s_run[at, :] = s
            yield

    def arrived(j):
        for k in range(UNROLL * TILE // LOAD_TILE):
            cat_copy(j * (UNROLL * TILE // LOAD_TILE) + k).wait()

    def together(*parts):
        parts = list(parts)
        while parts:
            parts = [p for p in parts if next(p, parts) is not parts]

    z_refs = (z_even, z_odd)

    def step(i, k):
        together(logits(i + 1, z_refs[(k + 1) % 2]), weigh(i, z_refs[k % 2]))

    with jax.named_scope("pass1a"):
        m_hist[0] = m_run[...]
        arrived(0)
        together(logits(0, z_even))

    def first_pass(j, carry):
        arrived(j + 1)
        for k in range(UNROLL):
            step(j * UNROLL + k, k)
        return carry

    with jax.named_scope("pass1b"):
        lax.fori_loop(0, tiles // UNROLL - 1, first_pass, 0)

    with jax.named_scope("pass1c"):
        for k in range(UNROLL - 1):
            step(tiles - UNROLL + k, k)
        together(weigh(tiles - 1, z_odd))

    m_t = m_run[...].T
    m_row = jnp.max(m_t, axis=0, keepdims=True)
    s_row = jnp.sum(s_run[...].T * jnp.exp(m_t - m_row), axis=0, keepdims=True)
    sub = lax.broadcasted_iota(jnp.int32, (8, LANES), 0)
    stats[me] = jnp.where(sub == 0, m_row, s_row)
    exchange(lambda p: stats.at[me], stats.at[me], 2)
    t_run[...] = jnp.zeros(t_run.shape, F32)
    arrive(lab.at[other_rows], 0)
    local = lab[...] - me * items
    lane = lax.broadcasted_iota(jnp.int32, lab.shape, 1)
    d[...] = local - lane
    wide = WEIGHT_TILE // LANES

    def weights(i, carry):
        for r in range(0, rows, WEIGHT_GROUP):
            at = slice(r, r + WEIGHT_GROUP)
            m = m_run[at, :]
            t = t_run[at, :]
            dd = d[at, :] - i * WEIGHT_TILE
            for c in range(wide):
                zc = ez[i * wide + c, at, :]
                t = jnp.where(dd == c * LANES, zc, t)
                ez[i * wide + c, at, :] = jnp.exp(zc - m)
            t_run[at, :] = t
        return carry

    with jax.named_scope("weights"):
        lax.fori_loop(0, items // WEIGHT_TILE, weights, 0)

    t_col = jnp.broadcast_to(jnp.sum(t_run[...], axis=1, keepdims=True), lab.shape)
    targets[me] = t_col.T[0:8, :]
    with jax.named_scope("statwait"):
        arrive(stats.at[others], 2)

    big = stats[0, 0:1, :]
    for p in range(1, n):
        big = jnp.maximum(big, stats[p, 0:1, :])
    total = jnp.zeros_like(big)
    for p in range(n):
        total = total + stats[p, 1:2, :] * jnp.exp(stats[p, 0:1, :] - big)
    inv = 1.0 / (total * rows)
    big_col = jnp.broadcast_to(big, (rows, LANES)).T
    inv_col = jnp.broadcast_to(inv, (rows, LANES)).T
    hit_col = (jnp.exp(t_col - big_col) * inv_col - 1.0 / rows).astype(BF16)
    scale = jnp.exp(m_run[...] - big_col) * inv_col
    home = jnp.where(local - local // LANES * LANES == lane, local // LANES, -1)
    home = jnp.where((local >= 0) & (local < items), home, -1).astype(F32)

    def second_pass(i, carry):
        gs = []
        count = SECOND_TILE // LANES
        here = (home - (i * count).astype(F32)).astype(BF16)
        for c in range(count):
            g = (ez[i * count + c] * scale).astype(BF16)
            g = jnp.where(here == jnp.bfloat16(c), hit_col, g)
            g_ref[i * count + c] = g
            gs.append(g)
        base = pl.multiple_of(i * SECOND_TILE, SECOND_TILE)
        part[...] += dot(jnp.concatenate(gs, axis=1), cat[pl.ds(base, SECOND_TILE), :], (1, 0))
        return carry

    with jax.named_scope("pass2"):
        lax.fori_loop(0, items // SECOND_TILE, second_pass, 0)

    exchange(lambda p: part.at[rows_of(p)], pieces.at[me], 3)
    pieces[me] = part[my_rows, :]

    def item_grads(i, carry):
        count = OUT_TILE // LANES
        g = jnp.concatenate([g_ref[i * count + c] for c in range(count)], axis=1)
        cat[pl.ds(pl.multiple_of(i * OUT_TILE, OUT_TILE), OUT_TILE), :] = dot(g, x_ref[...], (0, 0)).astype(BF16)
        return carry

    with jax.named_scope("de1"):
        lax.fori_loop(0, EARLY, item_grads, 0)

    exchange(lambda p: targets.at[me], targets.at[me], 5)
    with jax.named_scope("rswait"):
        arrive(pieces.at[others], 3)

    acc = pieces[0]
    for p in range(1, n):
        acc = acc + pieces[p]
    dx_ref[my_rows, :] = acc.astype(BF16)
    exchange(lambda p: dx_ref.at[my_rows], dx_ref.at[my_rows], 4)
    with jax.named_scope("de2"):
        lax.fori_loop(EARLY, items // OUT_TILE, item_grads, 0)

    arrive(q_ref.at[other_rows], 6)
    a = dot(q_ref[...], w1[...], (1, 0))
    a_ref[...] = a
    h_ref[...] = jnp.maximum(a, 0.0).astype(BF16)
    with jax.named_scope("agwait"):
        arrive(dx_ref.at[other_rows], 4)

    arrive(targets.at[others], 5)
    target = targets[0, 0:1, :]
    for p in range(1, n):
        target = target + targets[p, 0:1, :]
    loss_ref[...] = jnp.broadcast_to(
        jnp.sum(big + jnp.log(total) - target, axis=1, keepdims=True) / rows, loss_ref.shape)
    sent(lab.at[other_rows], 0)
    sent(x_ref.at[other_rows], 1)
    sent(q_ref.at[other_rows], 6)
    sent(stats.at[others], 2)
    sent(pieces.at[others], 3)
    sent(dx_ref.at[other_rows], 4)
    sent(targets.at[others], 5)


def grad_kernel(de_ref, dx_ref, h_ref, a_ref, q_ref, w2_ref, loss_ref,
                loss_hbm, de_hbm, dw1_hbm, dw2_hbm, loss, dw1, dw2, sem):
    copies = []
    for k in range(de_hbm.shape[0] // LOAD_TILE):
        at = pl.ds(k * LOAD_TILE, LOAD_TILE)
        pltpu.make_async_copy(de_ref.at[at], de_hbm.at[at], sem.at[3]).start()
    dx = dx_ref[...]
    dw2[...] = dot(h_ref[...], dx, (0, 0)).astype(BF16)
    dh = dot(dx, w2_ref[...], (1, 1))
    da = jnp.where(a_ref[...] > 0.0, dh, 0.0).astype(BF16)
    dw1[...] = dot(q_ref[...], da, (0, 0)).astype(BF16)
    loss[...] = loss_ref[0:1, 0:1]
    copies.append(pltpu.make_async_copy(loss, loss_hbm, sem.at[0]))
    copies.append(pltpu.make_async_copy(dw1, dw1_hbm, sem.at[1]))
    copies.append(pltpu.make_async_copy(dw2, dw2_hbm, sem.at[2]))
    for copy in copies[-3:]:
        copy.start()
    for copy in copies:
        copy.wait()
    pltpu.make_async_copy(de_ref, de_hbm, sem.at[3]).wait()


def solution(mesh):
    n = mesh.shape["tp"]

    def local_step(queries, w_first, w_second, catalogue, log_q, labels):
        own, d_in = queries.shape
        hid, emb = w_second.shape
        items = catalogue.shape[0]
        rows = own * n
        hbm = pl.BlockSpec(memory_space=pl.ANY)
        vmem = pl.BlockSpec(memory_space=pltpu.VMEM)
        dma = pltpu.SemaphoreType.DMA
        held = pl.pallas_call(
            functools.partial(loss_kernel, n),
            name="loss_kernel",
            out_shape=[
                pltpu.VMEM((items, emb), BF16),
                pltpu.VMEM((rows, emb), BF16),
                pltpu.VMEM((rows, hid), BF16),
                pltpu.VMEM((rows, hid), F32),
                pltpu.VMEM((rows, d_in), BF16),
                pltpu.VMEM((hid, emb), BF16),
                pltpu.VMEM((32, LANES), F32),
            ],
            in_specs=[hbm] * 6,
            out_specs=[vmem] * 7,
            scratch_shapes=[
                pltpu.VMEM((rows, emb), BF16),
                pltpu.VMEM((items // LANES, rows, LANES), BF16),
                pltpu.VMEM((items // LANES, rows, LANES), F32),
                pltpu.VMEM((TILE // LANES, rows, LANES), F32),
                pltpu.VMEM((TILE // LANES, rows, LANES), F32),
                pltpu.VMEM((1, items), F32),
                pltpu.VMEM((d_in, hid), BF16),
                pltpu.SMEM((own,), jnp.int32),
                pltpu.VMEM((rows, LANES), jnp.int32),
                pltpu.VMEM((rows, LANES), jnp.int32),
                pltpu.VMEM((rows, LANES), F32),
                pltpu.VMEM((rows, LANES), F32),
                pltpu.VMEM((rows, LANES), F32),
                pltpu.VMEM((items // TILE + 1, rows, LANES), F32),
                pltpu.VMEM((n, 8, LANES), F32),
                pltpu.VMEM((n, 8, LANES), F32),
                pltpu.VMEM((rows, emb), F32),
                pltpu.VMEM((n, own, emb), F32),
                dma((5,)),
                dma((items // LOAD_TILE,)),
                dma((7,)),
                dma((7,)),
            ],
            compiler_params=pltpu.CompilerParams(collective_id=0, has_side_effects=True, vmem_limit_bytes=44 << 20),
        )(queries, w_first, w_second, catalogue, log_q.reshape(1, items), labels)
        loss, grad_items, grad_first, grad_second = pl.pallas_call(
            grad_kernel,
            name="grad_kernel",
            out_shape=[
                jax.ShapeDtypeStruct((1, 1), F32),
                jax.ShapeDtypeStruct((items, emb), BF16),
                jax.ShapeDtypeStruct((d_in, hid), BF16),
                jax.ShapeDtypeStruct((hid, emb), BF16),
            ],
            in_specs=[vmem] * 7,
            out_specs=[hbm] * 4,
            scratch_shapes=[
                pltpu.VMEM((1, 1), F32),
                pltpu.VMEM((d_in, hid), BF16),
                pltpu.VMEM((hid, emb), BF16),
                dma((4,)),
            ],
            compiler_params=pltpu.CompilerParams(vmem_limit_bytes=24 << 20),
        )(*held)
        return loss.reshape(1), grad_items, grad_first, grad_second

    row_spec = P(("dp", "tp"), None)
    return jax.shard_map(
        local_step, mesh=mesh,
        in_specs=(row_spec, P(None, None), P(None, None), P("tp", None), P("tp"), P(("dp", "tp"))),
        out_specs=(P("dp"), row_spec, P("dp", None), P("dp", None)), check_vma=False)
```

```python
import functools

import jax
import jax.numpy as jnp
from jax import lax
from jax.experimental import pallas as pl
from jax.experimental.pallas import tpu as pltpu
from jax.sharding import PartitionSpec as P

F32, BF16 = jnp.float32, jnp.bfloat16
MESH = pl.DeviceIdType.MESH
LANES = 128
TILE = 2048
UNROLL = 4
DOT_TILE = 512
GROUP = 32
WEIGHT_TILE = 4096
WEIGHT_GROUP = 16
SECOND_TILE = 8192
LOAD_TILE = 4096
OUT_TILE = 4096
EARLY = 5
WARM = 3
LOWEST = -3.0e38


def dot(a, b, contract):
    return lax.dot_general(a, b, ((contract[:1], contract[1:]), ((), ())), preferred_element_type=F32)


def loss_kernel(n, q_hbm, w1_hbm, w2_hbm, cat_hbm, lq_hbm, lab_hbm,
                cat, dx_ref, h_ref, a_ref, q_ref, w2_ref, loss_ref,
                x_ref, g_ref, ez, z_even, z_odd, lq, w1, labels, lab, d, m_run, s_run, t_run, m_hist, stats, targets, part, pieces,
                load_sem, cat_sem, send_sem, recv_sem):
    me = lax.axis_index("tp")
    own = q_hbm.shape[0]
    rows = own * n
    items = cat_hbm.shape[0]
    tiles = items // TILE
    chunks = TILE // LANES
    my_rows = pl.ds(pl.multiple_of(me * own, own), own)

    others = pl.ds(0, n - 1)
    other_rows = pl.ds(0, rows - own)

    q_load = pltpu.make_async_copy(q_hbm, q_ref.at[my_rows], load_sem.at[0])
    w1_load = pltpu.make_async_copy(w1_hbm, w1, load_sem.at[1])
    w2_load = pltpu.make_async_copy(w2_hbm, w2_ref, load_sem.at[2])
    lq_load = pltpu.make_async_copy(lq_hbm, lq, load_sem.at[3])
    lab_load = pltpu.make_async_copy(lab_hbm, labels, load_sem.at[4])
    for load in (q_load, w1_load, w2_load):
        load.start()
    barrier = pltpu.get_barrier_semaphore()
    peers = [lax.rem(me + k, n) for k in range(1, n)]
    for p in peers:
        pl.semaphore_signal(barrier, inc=1, device_id={"tp": p}, device_id_type=MESH)
    for load in (lq_load, lab_load):
        load.start()

    def cat_copy(k):
        part_rows = pl.ds(pl.multiple_of(k * LOAD_TILE, LOAD_TILE), LOAD_TILE)
        return pltpu.make_async_copy(cat_hbm.at[part_rows], cat.at[part_rows], cat_sem.at[k])

    q_load.wait()
    w1_load.wait()
    w2_load.wait()
    for k in range(items // LOAD_TILE):
        cat_copy(k).start()
    own_hidden = jnp.maximum(dot(q_ref[my_rows, :], w1[...], (1, 0)), 0.0).astype(BF16)
    x_ref[my_rows, :] = dot(own_hidden, w2_ref[...], (1, 0)).astype(BF16)
    with jax.named_scope("bar"):
        pl.semaphore_wait(barrier, n - 1)

    def exchange(src, dst, stage):
        for p in peers:
            pltpu.make_async_remote_copy(
                src_ref=src(p), dst_ref=dst, send_sem=send_sem.at[stage], recv_sem=recv_sem.at[stage],
                device_id={"tp": p}, device_id_type=MESH).start()

    def arrive(others, stage):
        pltpu.make_async_copy(others, others, recv_sem.at[stage]).wait()

    def sent(others, stage):
        pltpu.make_async_copy(others, others, send_sem.at[stage]).wait()

    def rows_of(p):
        return pl.ds(pl.multiple_of(p * own, own), own)

    exchange(lambda p: x_ref.at[my_rows], x_ref.at[my_rows], 1)
    exchange(lambda p: q_ref.at[my_rows], q_ref.at[my_rows], 6)
    lq_load.wait()
    lab_load.wait()
    for r in range(own):
        lab[pl.ds(me * own + r, 1), :] = jnp.full((1, LANES), labels[r], jnp.int32)
    m_run[...] = jnp.full(m_run.shape, LOWEST, F32)
    s_run[...] = jnp.zeros(s_run.shape, F32)
    part[...] = jnp.zeros(part.shape, F32)
    exchange(lambda p: lab.at[my_rows], lab.at[my_rows], 0)

    def warm(k, carry):
        for j in range(0, w1.shape[1], 2 * LANES):
            r = dot(w2_ref[...], w1[:, j:j + 2 * LANES], (1, 0))
            for i in range(TILE // LANES // 2):
                z_even[2 * i] = r[i * LANES:(i + 1) * LANES, :LANES]
                z_even[2 * i + 1] = r[i * LANES:(i + 1) * LANES, LANES:]
        return carry

    lax.fori_loop(0, WARM, warm, 0)
    with jax.named_scope("xgather"):
        arrive(x_ref.at[other_rows], 1)

    def logits(i, z_ref):
        for j in range(TILE // DOT_TILE):
            base = pl.multiple_of(i * TILE + j * DOT_TILE, DOT_TILE)
            z = dot(x_ref[...], cat[pl.ds(base, DOT_TILE), :], (1, 1)) - lq[:, pl.ds(base, DOT_TILE)]
            m = m_run[...]
            for c in range(DOT_TILE // LANES):
                zc = z[:, c * LANES:(c + 1) * LANES]
                z_ref[j * (DOT_TILE // LANES) + c] = zc
                ez[i * chunks + j * (DOT_TILE // LANES) + c] = zc
                m = jnp.maximum(m, zc)
            m_run[...] = m
            yield
        m_hist[i + 1] = m

    def weigh(i, z_ref):
        for r in range(0, rows, GROUP):
            at = slice(r, r + GROUP)
            m = m_hist[i + 1, at, :]
            s = s_run[at, :] * jnp.exp(m_hist[i, at, :] - m)
            for c in range(chunks):
                s = s + jnp.exp(z_ref[c, at, :] - m)
            s_run[at, :] = s
            yield

    def arrived(j):
        for k in range(UNROLL * TILE // LOAD_TILE):
            cat_copy(j * (UNROLL * TILE // LOAD_TILE) + k).wait()

    def together(*parts):
        parts = list(parts)
        while parts:
            parts = [p for p in parts if next(p, parts) is not parts]

    z_refs = (z_even, z_odd)

    def step(i, k):
        together(logits(i + 1, z_refs[(k + 1) % 2]), weigh(i, z_refs[k % 2]))

    with jax.named_scope("pass1a"):
        m_hist[0] = m_run[...]
        arrived(0)
        together(logits(0, z_even))

    def first_pass(j, carry):
        arrived(j + 1)
        for k in range(UNROLL):
            step(j * UNROLL + k, k)
        return carry

    with jax.named_scope("pass1b"):
        lax.fori_loop(0, tiles // UNROLL - 1, first_pass, 0)

    with jax.named_scope("pass1c"):
        for k in range(UNROLL - 1):
            step(tiles - UNROLL + k, k)
        together(weigh(tiles - 1, z_odd))

    m_t = m_run[...].T
    m_row = jnp.max(m_t, axis=0, keepdims=True)
    s_row = jnp.sum(s_run[...].T * jnp.exp(m_t - m_row), axis=0, keepdims=True)
    sub = lax.broadcasted_iota(jnp.int32, (8, LANES), 0)
    stats[me] = jnp.where(sub == 0, m_row, s_row)
    exchange(lambda p: stats.at[me], stats.at[me], 2)
    t_run[...] = jnp.zeros(t_run.shape, F32)
    arrive(lab.at[other_rows], 0)
    local = lab[...] - me * items
    lane = lax.broadcasted_iota(jnp.int32, lab.shape, 1)
    d[...] = local - lane
    wide = WEIGHT_TILE // LANES

    def weights(i, carry):
        for r in range(0, rows, WEIGHT_GROUP):
            at = slice(r, r + WEIGHT_GROUP)
            m = m_run[at, :]
            t = t_run[at, :]
            dd = d[at, :] - i * WEIGHT_TILE
            for c in range(wide):
                zc = ez[i * wide + c, at, :]
                t = jnp.where(dd == c * LANES, zc, t)
                ez[i * wide + c, at, :] = jnp.exp(zc - m)
            t_run[at, :] = t
        return carry

    with jax.named_scope("weights"):
        lax.fori_loop(0, items // WEIGHT_TILE, weights, 0)

    t_col = jnp.broadcast_to(jnp.sum(t_run[...], axis=1, keepdims=True), lab.shape)
    targets[me] = t_col.T[0:8, :]
    with jax.named_scope("statwait"):
        arrive(stats.at[others], 2)

    big = stats[0, 0:1, :]
    for p in range(1, n):
        big = jnp.maximum(big, stats[p, 0:1, :])
    total = jnp.zeros_like(big)
    for p in range(n):
        total = total + stats[p, 1:2, :] * jnp.exp(stats[p, 0:1, :] - big)
    inv = 1.0 / (total * rows)
    big_col = jnp.broadcast_to(big, (rows, LANES)).T
    inv_col = jnp.broadcast_to(inv, (rows, LANES)).T
    hit_col = (jnp.exp(t_col - big_col) * inv_col - 1.0 / rows).astype(BF16)
    scale = jnp.exp(m_run[...] - big_col) * inv_col
    home = jnp.where(local - local // LANES * LANES == lane, local // LANES, -1)
    home = jnp.where((local >= 0) & (local < items), home, -1).astype(F32)

    def second_pass(i, carry):
        gs = []
        count = SECOND_TILE // LANES
        here = (home - (i * count).astype(F32)).astype(BF16)
        for c in range(count):
            g = (ez[i * count + c] * scale).astype(BF16)
            g = jnp.where(here == jnp.bfloat16(c), hit_col, g)
            g_ref[i * count + c] = g
            gs.append(g)
        base = pl.multiple_of(i * SECOND_TILE, SECOND_TILE)
        part[...] += dot(jnp.concatenate(gs, axis=1), cat[pl.ds(base, SECOND_TILE), :], (1, 0))
        return carry

    with jax.named_scope("pass2"):
        lax.fori_loop(0, items // SECOND_TILE, second_pass, 0)

    exchange(lambda p: part.at[rows_of(p)], pieces.at[me], 3)
    pieces[me] = part[my_rows, :]

    def item_grads(i, carry):
        count = OUT_TILE // LANES
        g = jnp.concatenate([g_ref[i * count + c] for c in range(count)], axis=1)
        cat[pl.ds(pl.multiple_of(i * OUT_TILE, OUT_TILE), OUT_TILE), :] = dot(g, x_ref[...], (0, 0)).astype(BF16)
        return carry

    with jax.named_scope("de1"):
        lax.fori_loop(0, EARLY, item_grads, 0)

    exchange(lambda p: targets.at[me], targets.at[me], 5)
    with jax.named_scope("rswait"):
        arrive(pieces.at[others], 3)

    acc = pieces[0]
    for p in range(1, n):
        acc = acc + pieces[p]
    dx_ref[my_rows, :] = acc.astype(BF16)
    exchange(lambda p: dx_ref.at[my_rows], dx_ref.at[my_rows], 4)
    with jax.named_scope("de2"):
        lax.fori_loop(EARLY, items // OUT_TILE, item_grads, 0)

    arrive(q_ref.at[other_rows], 6)
    a = dot(q_ref[...], w1[...], (1, 0))
    a_ref[...] = a
    h_ref[...] = jnp.maximum(a, 0.0).astype(BF16)
    with jax.named_scope("agwait"):
        arrive(dx_ref.at[other_rows], 4)

    arrive(targets.at[others], 5)
    target = targets[0, 0:1, :]
    for p in range(1, n):
        target = target + targets[p, 0:1, :]
    loss_ref[...] = jnp.broadcast_to(
        jnp.sum(big + jnp.log(total) - target, axis=1, keepdims=True) / rows, loss_ref.shape)
    sent(lab.at[other_rows], 0)
    sent(x_ref.at[other_rows], 1)
    sent(q_ref.at[other_rows], 6)
    sent(stats.at[others], 2)
    sent(pieces.at[others], 3)
    sent(dx_ref.at[other_rows], 4)
    sent(targets.at[others], 5)


def grad_kernel(de_ref, dx_ref, h_ref, a_ref, q_ref, w2_ref, loss_ref,
                loss_hbm, de_hbm, dw1_hbm, dw2_hbm, loss, dw1, dw2, sem):
    copies = []
    for k in range(de_hbm.shape[0] // LOAD_TILE):
        at = pl.ds(k * LOAD_TILE, LOAD_TILE)
        pltpu.make_async_copy(de_ref.at[at], de_hbm.at[at], sem.at[3]).start()
    dx = dx_ref[...]
    dw2[...] = dot(h_ref[...], dx, (0, 0)).astype(BF16)
    dh = dot(dx, w2_ref[...], (1, 1))
    da = jnp.where(a_ref[...] > 0.0, dh, 0.0).astype(BF16)
    dw1[...] = dot(q_ref[...], da, (0, 0)).astype(BF16)
    loss[...] = loss_ref[0:1, 0:1]
    copies.append(pltpu.make_async_copy(loss, loss_hbm, sem.at[0]))
    copies.append(pltpu.make_async_copy(dw1, dw1_hbm, sem.at[1]))
    copies.append(pltpu.make_async_copy(dw2, dw2_hbm, sem.at[2]))
    for copy in copies[-3:]:
        copy.start()
    for copy in copies:
        copy.wait()
    pltpu.make_async_copy(de_ref, de_hbm, sem.at[3]).wait()


def solution(mesh):
    n = mesh.shape["tp"]

    def local_step(queries, w_first, w_second, catalogue, log_q, labels):
        own, d_in = queries.shape
        hid, emb = w_second.shape
        items = catalogue.shape[0]
        rows = own * n
        hbm = pl.BlockSpec(memory_space=pl.ANY)
        vmem = pl.BlockSpec(memory_space=pltpu.VMEM)
        dma = pltpu.SemaphoreType.DMA
        held = pl.pallas_call(
            functools.partial(loss_kernel, n),
            name="loss_kernel",
            out_shape=[
                pltpu.VMEM((items, emb), BF16),
                pltpu.VMEM((rows, emb), BF16),
                pltpu.VMEM((rows, hid), BF16),
                pltpu.VMEM((rows, hid), F32),
                pltpu.VMEM((rows, d_in), BF16),
                pltpu.VMEM((hid, emb), BF16),
                pltpu.VMEM((32, LANES), F32),
            ],
            in_specs=[hbm] * 6,
            out_specs=[vmem] * 7,
            scratch_shapes=[
                pltpu.VMEM((rows, emb), BF16),
                pltpu.VMEM((items // LANES, rows, LANES), BF16),
                pltpu.VMEM((items // LANES, rows, LANES), F32),
                pltpu.VMEM((TILE // LANES, rows, LANES), F32),
                pltpu.VMEM((TILE // LANES, rows, LANES), F32),
                pltpu.VMEM((1, items), F32),
                pltpu.VMEM((d_in, hid), BF16),
                pltpu.SMEM((own,), jnp.int32),
                pltpu.VMEM((rows, LANES), jnp.int32),
                pltpu.VMEM((rows, LANES), jnp.int32),
                pltpu.VMEM((rows, LANES), F32),
                pltpu.VMEM((rows, LANES), F32),
                pltpu.VMEM((rows, LANES), F32),
                pltpu.VMEM((items // TILE + 1, rows, LANES), F32),
                pltpu.VMEM((n, 8, LANES), F32),
                pltpu.VMEM((n, 8, LANES), F32),
                pltpu.VMEM((rows, emb), F32),
                pltpu.VMEM((n, own, emb), F32),
                dma((5,)),
                dma((items // LOAD_TILE,)),
                dma((7,)),
                dma((7,)),
            ],
            compiler_params=pltpu.CompilerParams(collective_id=0, has_side_effects=True, vmem_limit_bytes=44 << 20),
        )(queries, w_first, w_second, catalogue, log_q.reshape(1, items), labels)
        loss, grad_items, grad_first, grad_second = pl.pallas_call(
            grad_kernel,
            name="grad_kernel",
            out_shape=[
                jax.ShapeDtypeStruct((1, 1), F32),
                jax.ShapeDtypeStruct((items, emb), BF16),
                jax.ShapeDtypeStruct((d_in, hid), BF16),
                jax.ShapeDtypeStruct((hid, emb), BF16),
            ],
            in_specs=[vmem] * 7,
            out_specs=[hbm] * 4,
            scratch_shapes=[
                pltpu.VMEM((1, 1), F32),
                pltpu.VMEM((d_in, hid), BF16),
                pltpu.VMEM((hid, emb), BF16),
                dma((4,)),
            ],
            compiler_params=pltpu.CompilerParams(vmem_limit_bytes=24 << 20),
        )(*held)
        return loss.reshape(1), grad_items, grad_first, grad_second

    row_spec = P(("dp", "tp"), None)
    return jax.shard_map(
        local_step, mesh=mesh,
        in_specs=(row_spec, P(None, None), P(None, None), P("tp", None), P("tp"), P(("dp", "tp"))),
        out_specs=(P("dp"), row_spec, P("dp", None), P("dp", None)), check_vma=False)
```

```python
import functools

import jax
import jax.numpy as jnp
from jax import lax
from jax.experimental import pallas as pl
from jax.experimental.pallas import tpu as pltpu
from jax.sharding import PartitionSpec as P

F32, BF16 = jnp.float32, jnp.bfloat16
MESH = pl.DeviceIdType.MESH
LANES = 128
TILE = 2048
UNROLL = 4
DOT_TILE = 512
GROUP = 32
WEIGHT_TILE = 4096
WEIGHT_GROUP = 16
SECOND_TILE = 8192
LOAD_TILE = 4096
OUT_TILE = 4096
EARLY = 5
SHIFT = 16
LOWEST = -3.0e38


def dot(a, b, contract):
    return lax.dot_general(a, b, ((contract[:1], contract[1:]), ((), ())), preferred_element_type=F32)


def loss_kernel(n, q_hbm, w1_hbm, w2_hbm, cat_hbm, lq_hbm, lab_hbm,
                cat, dx_ref, h_ref, a_ref, q_ref, w2_ref, loss_ref,
                x_ref, g_ref, ez, z_even, z_odd, lq, w1, labels, lab, d, m_run, s_run, t_run, m_hist, stats, targets, part, pieces,
                load_sem, cat_sem, send_sem, recv_sem):
    me = lax.axis_index("tp")
    own = q_hbm.shape[0]
    rows = own * n
    items = cat_hbm.shape[0]
    tiles = items // TILE
    chunks = TILE // LANES
    my_rows = pl.ds(pl.multiple_of(me * own, own), own)

    others = pl.ds(0, n - 1)
    other_rows = pl.ds(0, rows - own)

    q_load = pltpu.make_async_copy(q_hbm, q_ref.at[my_rows], load_sem.at[0])
    w1_load = pltpu.make_async_copy(w1_hbm, w1, load_sem.at[1])
    w2_load = pltpu.make_async_copy(w2_hbm, w2_ref, load_sem.at[2])
    lq_load = pltpu.make_async_copy(lq_hbm, lq, load_sem.at[3])
    lab_load = pltpu.make_async_copy(lab_hbm, labels, load_sem.at[4])
    for load in (q_load, w1_load, w2_load):
        load.start()
    barrier = pltpu.get_barrier_semaphore()
    peers = [lax.rem(me + k, n) for k in range(1, n)]
    for p in peers:
        pl.semaphore_signal(barrier, inc=1, device_id={"tp": p}, device_id_type=MESH)
    for load in (lq_load, lab_load):
        load.start()

    def cat_copy(k):
        part_rows = pl.ds(pl.multiple_of(k * LOAD_TILE, LOAD_TILE), LOAD_TILE)
        return pltpu.make_async_copy(cat_hbm.at[part_rows], cat.at[part_rows], cat_sem.at[k])

    q_load.wait()
    w1_load.wait()
    w2_load.wait()
    for k in range(items // LOAD_TILE):
        cat_copy(k).start()
    own_hidden = jnp.maximum(dot(q_ref[my_rows, :], w1[...], (1, 0)), 0.0).astype(BF16)
    x_ref[my_rows, :] = dot(own_hidden, w2_ref[...], (1, 0)).astype(BF16)
    with jax.named_scope("bar"):
        pl.semaphore_wait(barrier, n - 1)

    def exchange(src, dst, stage):
        for p in peers:
            pltpu.make_async_remote_copy(
                src_ref=src(p), dst_ref=dst, send_sem=send_sem.at[stage], recv_sem=recv_sem.at[stage],
                device_id={"tp": p}, device_id_type=MESH).start()

    def arrive(others, stage):
        pltpu.make_async_copy(others, others, recv_sem.at[stage]).wait()

    def sent(others, stage):
        pltpu.make_async_copy(others, others, send_sem.at[stage]).wait()

    def rows_of(p):
        return pl.ds(pl.multiple_of(p * own, own), own)

    exchange(lambda p: x_ref.at[my_rows], x_ref.at[my_rows], 1)
    exchange(lambda p: q_ref.at[my_rows], q_ref.at[my_rows], 6)
    lq_load.wait()
    lab_load.wait()
    for r in range(own):
        lab[pl.ds(me * own + r, 1), :] = jnp.full((1, LANES), labels[r], jnp.int32)
    m_run[...] = jnp.full(m_run.shape, LOWEST, F32)
    s_run[...] = jnp.zeros(s_run.shape, F32)
    part[...] = jnp.zeros(part.shape, F32)
    exchange(lambda p: lab.at[my_rows], lab.at[my_rows], 0)
    with jax.named_scope("xgather"):
        arrive(x_ref.at[other_rows], 1)

    def logits(i, z_ref):
        for j in range(TILE // DOT_TILE):
            base = pl.multiple_of(i * TILE + j * DOT_TILE, DOT_TILE)
            z = dot(x_ref[...], cat[pl.ds(base, DOT_TILE), :], (1, 1)) - lq[:, pl.ds(base, DOT_TILE)]
            m = m_run[...]
            for c in range(DOT_TILE // LANES):
                zc = z[:, c * LANES:(c + 1) * LANES]
                z_ref[pl.ds(SHIFT + (j * (DOT_TILE // LANES) + c) * rows, rows), :] = zc
                ez[i * chunks + j * (DOT_TILE // LANES) + c] = zc
                m = jnp.maximum(m, zc)
            m_run[...] = m
            yield
        m_hist[i + 1] = m

    def weigh(i, z_ref):
        for r in range(0, rows, GROUP):
            at = slice(r, r + GROUP)
            m = m_hist[i + 1, at, :]
            s = s_run[at, :] * jnp.exp(m_hist[i, at, :] - m)
            for c in range(chunks):
                s = s + jnp.exp(z_ref[pl.ds(SHIFT + c * rows + r, GROUP), :] - m)
            s_run[at, :] = s
            yield

    def arrived(j):
        for k in range(UNROLL * TILE // LOAD_TILE):
            cat_copy(j * (UNROLL * TILE // LOAD_TILE) + k).wait()

    def together(*parts):
        parts = list(parts)
        while parts:
            parts = [p for p in parts if next(p, parts) is not parts]

    z_refs = (z_even, z_odd)

    def step(i, k):
        together(logits(i + 1, z_refs[(k + 1) % 2]), weigh(i, z_refs[k % 2]))

    with jax.named_scope("pass1a"):
        m_hist[0] = m_run[...]
        arrived(0)
        together(logits(0, z_even))

    def first_pass(j, carry):
        arrived(j + 1)
        for k in range(UNROLL):
            step(j * UNROLL + k, k)
        return carry

    with jax.named_scope("pass1b"):
        lax.fori_loop(0, tiles // UNROLL - 1, first_pass, 0)

    with jax.named_scope("pass1c"):
        for k in range(UNROLL - 1):
            step(tiles - UNROLL + k, k)
        together(weigh(tiles - 1, z_odd))

    m_t = m_run[...].T
    m_row = jnp.max(m_t, axis=0, keepdims=True)
    s_row = jnp.sum(s_run[...].T * jnp.exp(m_t - m_row), axis=0, keepdims=True)
    sub = lax.broadcasted_iota(jnp.int32, (8, LANES), 0)
    stats[me] = jnp.where(sub == 0, m_row, s_row)
    exchange(lambda p: stats.at[me], stats.at[me], 2)
    t_run[...] = jnp.zeros(t_run.shape, F32)
    arrive(lab.at[other_rows], 0)
    local = lab[...] - me * items
    lane = lax.broadcasted_iota(jnp.int32, lab.shape, 1)
    d[...] = local - lane
    wide = WEIGHT_TILE // LANES

    def weights(i, carry):
        for r in range(0, rows, WEIGHT_GROUP):
            at = slice(r, r + WEIGHT_GROUP)
            m = m_run[at, :]
            t = t_run[at, :]
            dd = d[at, :] - i * WEIGHT_TILE
            for c in range(wide):
                zc = ez[i * wide + c, at, :]
                t = jnp.where(dd == c * LANES, zc, t)
                ez[i * wide + c, at, :] = jnp.exp(zc - m)
            t_run[at, :] = t
        return carry

    with jax.named_scope("weights"):
        lax.fori_loop(0, items // WEIGHT_TILE, weights, 0)

    t_col = jnp.broadcast_to(jnp.sum(t_run[...], axis=1, keepdims=True), lab.shape)
    targets[me] = t_col.T[0:8, :]
    with jax.named_scope("statwait"):
        arrive(stats.at[others], 2)

    big = stats[0, 0:1, :]
    for p in range(1, n):
        big = jnp.maximum(big, stats[p, 0:1, :])
    total = jnp.zeros_like(big)
    for p in range(n):
        total = total + stats[p, 1:2, :] * jnp.exp(stats[p, 0:1, :] - big)
    inv = 1.0 / (total * rows)
    big_col = jnp.broadcast_to(big, (rows, LANES)).T
    inv_col = jnp.broadcast_to(inv, (rows, LANES)).T
    hit_col = (jnp.exp(t_col - big_col) * inv_col - 1.0 / rows).astype(BF16)
    scale = jnp.exp(m_run[...] - big_col) * inv_col
    home = jnp.where(local - local // LANES * LANES == lane, local // LANES, -1)
    home = jnp.where((local >= 0) & (local < items), home, -1).astype(F32)

    def second_pass(i, carry):
        gs = []
        count = SECOND_TILE // LANES
        here = (home - (i * count).astype(F32)).astype(BF16)
        for c in range(count):
            g = (ez[i * count + c] * scale).astype(BF16)
            g = jnp.where(here == jnp.bfloat16(c), hit_col, g)
            g_ref[i * count + c, :rows, :] = g
            gs.append(g)
        base = pl.multiple_of(i * SECOND_TILE, SECOND_TILE)
        part[...] += dot(jnp.concatenate(gs, axis=1), cat[pl.ds(base, SECOND_TILE), :], (1, 0))
        return carry

    with jax.named_scope("pass2"):
        lax.fori_loop(0, items // SECOND_TILE, second_pass, 0)

    exchange(lambda p: part.at[rows_of(p)], pieces.at[me], 3)
    pieces[me] = part[my_rows, :]

    def item_grads(i, carry):
        count = OUT_TILE // LANES
        g = jnp.concatenate([g_ref[i * count + c, :rows, :] for c in range(count)], axis=1)
        cat[pl.ds(pl.multiple_of(i * OUT_TILE, OUT_TILE), OUT_TILE), :] = dot(g, x_ref[...], (0, 0)).astype(BF16)
        return carry

    with jax.named_scope("de1"):
        lax.fori_loop(0, EARLY, item_grads, 0)

    exchange(lambda p: targets.at[me], targets.at[me], 5)
    with jax.named_scope("rswait"):
        arrive(pieces.at[others], 3)

    acc = pieces[0]
    for p in range(1, n):
        acc = acc + pieces[p]
    dx_ref[my_rows, :] = acc.astype(BF16)
    exchange(lambda p: dx_ref.at[my_rows], dx_ref.at[my_rows], 4)
    with jax.named_scope("de2"):
        lax.fori_loop(EARLY, items // OUT_TILE, item_grads, 0)

    arrive(q_ref.at[other_rows], 6)
    a = dot(q_ref[...], w1[...], (1, 0))
    a_ref[...] = a
    h_ref[...] = jnp.maximum(a, 0.0).astype(BF16)
    with jax.named_scope("agwait"):
        arrive(dx_ref.at[other_rows], 4)

    arrive(targets.at[others], 5)
    target = targets[0, 0:1, :]
    for p in range(1, n):
        target = target + targets[p, 0:1, :]
    loss_ref[...] = jnp.broadcast_to(
        jnp.sum(big + jnp.log(total) - target, axis=1, keepdims=True) / rows, loss_ref.shape)
    sent(lab.at[other_rows], 0)
    sent(x_ref.at[other_rows], 1)
    sent(q_ref.at[other_rows], 6)
    sent(stats.at[others], 2)
    sent(pieces.at[others], 3)
    sent(dx_ref.at[other_rows], 4)
    sent(targets.at[others], 5)


def grad_kernel(de_ref, dx_ref, h_ref, a_ref, q_ref, w2_ref, loss_ref,
                loss_hbm, de_hbm, dw1_hbm, dw2_hbm, loss, dw1, dw2, sem):
    copies = []
    for k in range(de_hbm.shape[0] // LOAD_TILE):
        at = pl.ds(k * LOAD_TILE, LOAD_TILE)
        pltpu.make_async_copy(de_ref.at[at], de_hbm.at[at], sem.at[3]).start()
    dx = dx_ref[...]
    dw2[...] = dot(h_ref[...], dx, (0, 0)).astype(BF16)
    dh = dot(dx, w2_ref[...], (1, 1))
    da = jnp.where(a_ref[...] > 0.0, dh, 0.0).astype(BF16)
    dw1[...] = dot(q_ref[...], da, (0, 0)).astype(BF16)
    loss[...] = loss_ref[0:1, 0:1]
    copies.append(pltpu.make_async_copy(loss, loss_hbm, sem.at[0]))
    copies.append(pltpu.make_async_copy(dw1, dw1_hbm, sem.at[1]))
    copies.append(pltpu.make_async_copy(dw2, dw2_hbm, sem.at[2]))
    for copy in copies[-3:]:
        copy.start()
    for copy in copies:
        copy.wait()
    pltpu.make_async_copy(de_ref, de_hbm, sem.at[3]).wait()


def solution(mesh):
    n = mesh.shape["tp"]

    def local_step(queries, w_first, w_second, catalogue, log_q, labels):
        own, d_in = queries.shape
        hid, emb = w_second.shape
        items = catalogue.shape[0]
        rows = own * n
        hbm = pl.BlockSpec(memory_space=pl.ANY)
        vmem = pl.BlockSpec(memory_space=pltpu.VMEM)
        dma = pltpu.SemaphoreType.DMA
        held = pl.pallas_call(
            functools.partial(loss_kernel, n),
            name="loss_kernel",
            out_shape=[
                pltpu.VMEM((items, emb), BF16),
                pltpu.VMEM((rows, emb), BF16),
                pltpu.VMEM((rows, hid), BF16),
                pltpu.VMEM((rows, hid), F32),
                pltpu.VMEM((rows, d_in), BF16),
                pltpu.VMEM((hid, emb), BF16),
                pltpu.VMEM((32, LANES), F32),
            ],
            in_specs=[hbm] * 6,
            out_specs=[vmem] * 7,
            scratch_shapes=[
                pltpu.VMEM((rows, emb), BF16),
                pltpu.VMEM((items // LANES, rows + SHIFT, LANES), BF16),
                pltpu.VMEM((items // LANES, rows, LANES), F32),
                pltpu.VMEM((2 * SHIFT + TILE // LANES * rows, LANES), F32),
                pltpu.VMEM((2 * SHIFT + TILE // LANES * rows, LANES), F32),
                pltpu.VMEM((1, items), F32),
                pltpu.VMEM((d_in, hid), BF16),
                pltpu.SMEM((own,), jnp.int32),
                pltpu.VMEM((rows, LANES), jnp.int32),
                pltpu.VMEM((rows, LANES), jnp.int32),
                pltpu.VMEM((rows, LANES), F32),
                pltpu.VMEM((rows, LANES), F32),
                pltpu.VMEM((rows, LANES), F32),
                pltpu.VMEM((items // TILE + 1, rows, LANES), F32),
                pltpu.VMEM((n, 8, LANES), F32),
                pltpu.VMEM((n, 8, LANES), F32),
                pltpu.VMEM((rows, emb), F32),
                pltpu.VMEM((n, own, emb), F32),
                dma((5,)),
                dma((items // LOAD_TILE,)),
                dma((7,)),
                dma((7,)),
            ],
            compiler_params=pltpu.CompilerParams(collective_id=0, has_side_effects=True, vmem_limit_bytes=44 << 20),
        )(queries, w_first, w_second, catalogue, log_q.reshape(1, items), labels)
        loss, grad_items, grad_first, grad_second = pl.pallas_call(
            grad_kernel,
            name="grad_kernel",
            out_shape=[
                jax.ShapeDtypeStruct((1, 1), F32),
                jax.ShapeDtypeStruct((items, emb), BF16),
                jax.ShapeDtypeStruct((d_in, hid), BF16),
                jax.ShapeDtypeStruct((hid, emb), BF16),
            ],
            in_specs=[vmem] * 7,
            out_specs=[hbm] * 4,
            scratch_shapes=[
                pltpu.VMEM((1, 1), F32),
                pltpu.VMEM((d_in, hid), BF16),
                pltpu.VMEM((hid, emb), BF16),
                dma((4,)),
            ],
            compiler_params=pltpu.CompilerParams(vmem_limit_bytes=24 << 20),
        )(*held)
        return loss.reshape(1), grad_items, grad_first, grad_second

    row_spec = P(("dp", "tp"), None)
    return jax.shard_map(
        local_step, mesh=mesh,
        in_specs=(row_spec, P(None, None), P(None, None), P("tp", None), P("tp"), P(("dp", "tp"))),
        out_specs=(P("dp"), row_spec, P("dp", None), P("dp", None)), check_vma=False)
```

```python
import functools

import jax
import jax.numpy as jnp
from jax import lax
from jax.experimental import pallas as pl
from jax.experimental.pallas import tpu as pltpu
from jax.sharding import PartitionSpec as P

F32, BF16 = jnp.float32, jnp.bfloat16
MESH = pl.DeviceIdType.MESH
LANES = 128
TILE = 2048
UNROLL = 4
DOT_TILE = 512
GROUP = 32
WEIGHT_TILE = 4096
WEIGHT_GROUP = 16
SECOND_TILE = 8192
LOAD_TILE = 4096
OUT_TILE = 4096
EARLY = 5
SHIFT = 16
LOWEST = -3.0e38


def dot(a, b, contract):
    return lax.dot_general(a, b, ((contract[:1], contract[1:]), ((), ())), preferred_element_type=F32)


def loss_kernel(n, q_hbm, w1_hbm, w2_hbm, cat_hbm, lq_hbm, lab_hbm,
                cat, dx_ref, h_ref, a_ref, q_ref, w2_ref, loss_ref,
                x_ref, g_ref, ez, z_even, z_odd, lq, w1, labels, lab, d, m_run, s_run, t_run, m_hist, stats, targets, part, pieces,
                load_sem, cat_sem, send_sem, recv_sem):
    me = lax.axis_index("tp")
    own = q_hbm.shape[0]
    rows = own * n
    items = cat_hbm.shape[0]
    tiles = items // TILE
    chunks = TILE // LANES
    my_rows = pl.ds(pl.multiple_of(me * own, own), own)

    others = pl.ds(0, n - 1)
    other_rows = pl.ds(0, rows - own)

    q_load = pltpu.make_async_copy(q_hbm, q_ref.at[my_rows], load_sem.at[0])
    w1_load = pltpu.make_async_copy(w1_hbm, w1, load_sem.at[1])
    w2_load = pltpu.make_async_copy(w2_hbm, w2_ref, load_sem.at[2])
    lq_load = pltpu.make_async_copy(lq_hbm, lq, load_sem.at[3])
    lab_load = pltpu.make_async_copy(lab_hbm, labels, load_sem.at[4])
    for load in (q_load, w1_load, w2_load):
        load.start()
    barrier = pltpu.get_barrier_semaphore()
    peers = [lax.rem(me + k, n) for k in range(1, n)]
    for p in peers:
        pl.semaphore_signal(barrier, inc=1, device_id={"tp": p}, device_id_type=MESH)
    for load in (lq_load, lab_load):
        load.start()

    def cat_copy(k):
        part_rows = pl.ds(pl.multiple_of(k * LOAD_TILE, LOAD_TILE), LOAD_TILE)
        return pltpu.make_async_copy(cat_hbm.at[part_rows], cat.at[part_rows], cat_sem.at[k])

    q_load.wait()
    w1_load.wait()
    w2_load.wait()
    for k in range(items // LOAD_TILE):
        cat_copy(k).start()
    own_hidden = jnp.maximum(dot(q_ref[my_rows, :], w1[...], (1, 0)), 0.0).astype(BF16)
    x_ref[my_rows, :] = dot(own_hidden, w2_ref[...], (1, 0)).astype(BF16)
    pl.semaphore_wait(barrier, n - 1)

    def exchange(src, dst, stage):
        for p in peers:
            pltpu.make_async_remote_copy(
                src_ref=src(p), dst_ref=dst, send_sem=send_sem.at[stage], recv_sem=recv_sem.at[stage],
                device_id={"tp": p}, device_id_type=MESH).start()

    def arrive(others, stage):
        pltpu.make_async_copy(others, others, recv_sem.at[stage]).wait()

    def sent(others, stage):
        pltpu.make_async_copy(others, others, send_sem.at[stage]).wait()

    def rows_of(p):
        return pl.ds(pl.multiple_of(p * own, own), own)

    exchange(lambda p: x_ref.at[my_rows], x_ref.at[my_rows], 1)
    lq_load.wait()
    lab_load.wait()
    for r in range(own):
        lab[pl.ds(me * own + r, 1), :] = jnp.full((1, LANES), labels[r], jnp.int32)
    m_run[...] = jnp.full(m_run.shape, LOWEST, F32)
    s_run[...] = jnp.zeros(s_run.shape, F32)
    part[...] = jnp.zeros(part.shape, F32)
    arrive(x_ref.at[other_rows], 1)

    def logits(i, z_ref):
        for j in range(TILE // DOT_TILE):
            base = pl.multiple_of(i * TILE + j * DOT_TILE, DOT_TILE)
            z = dot(x_ref[...], cat[pl.ds(base, DOT_TILE), :], (1, 1)) - lq[:, pl.ds(base, DOT_TILE)]
            m = m_run[...]
            for c in range(DOT_TILE // LANES):
                zc = z[:, c * LANES:(c + 1) * LANES]
                z_ref[pl.ds(SHIFT + (j * (DOT_TILE // LANES) + c) * rows, rows), :] = zc
                ez[i * chunks + j * (DOT_TILE // LANES) + c] = zc
                m = jnp.maximum(m, zc)
            m_run[...] = m
            yield
        m_hist[i + 1] = m

    def weigh(i, z_ref):
        for r in range(0, rows, GROUP):
            at = slice(r, r + GROUP)
            m = m_hist[i + 1, at, :]
            s = s_run[at, :] * jnp.exp(m_hist[i, at, :] - m)
            for c in range(chunks):
                s = s + jnp.exp(z_ref[pl.ds(SHIFT + c * rows + r, GROUP), :] - m)
            s_run[at, :] = s
            yield

    def arrived(j):
        for k in range(UNROLL * TILE // LOAD_TILE):
            cat_copy(j * (UNROLL * TILE // LOAD_TILE) + k).wait()

    def together(*parts):
        parts = list(parts)
        while parts:
            parts = [p for p in parts if next(p, parts) is not parts]

    z_refs = (z_even, z_odd)

    def step(i, k):
        together(logits(i + 1, z_refs[(k + 1) % 2]), weigh(i, z_refs[k % 2]))

    m_hist[0] = m_run[...]
    arrived(0)
    together(logits(0, z_even))
    exchange(lambda p: lab.at[my_rows], lab.at[my_rows], 0)
    exchange(lambda p: q_ref.at[my_rows], q_ref.at[my_rows], 6)

    def first_pass(j, carry):
        arrived(j + 1)
        for k in range(UNROLL):
            step(j * UNROLL + k, k)
        return carry

    lax.fori_loop(0, tiles // UNROLL - 1, first_pass, 0)
    for k in range(UNROLL - 1):
        step(tiles - UNROLL + k, k)
    together(weigh(tiles - 1, z_odd))

    m_t = m_run[...].T
    m_row = jnp.max(m_t, axis=0, keepdims=True)
    s_row = jnp.sum(s_run[...].T * jnp.exp(m_t - m_row), axis=0, keepdims=True)
    sub = lax.broadcasted_iota(jnp.int32, (8, LANES), 0)
    stats[me] = jnp.where(sub == 0, m_row, s_row)
    exchange(lambda p: stats.at[me], stats.at[me], 2)
    t_run[...] = jnp.zeros(t_run.shape, F32)
    arrive(lab.at[other_rows], 0)
    local = lab[...] - me * items
    lane = lax.broadcasted_iota(jnp.int32, lab.shape, 1)
    d[...] = local - lane
    wide = WEIGHT_TILE // LANES

    def weights(i, carry):
        for r in range(0, rows, WEIGHT_GROUP):
            at = slice(r, r + WEIGHT_GROUP)
            m = m_run[at, :]
            t = t_run[at, :]
            dd = d[at, :] - i * WEIGHT_TILE
            for c in range(wide):
                zc = ez[i * wide + c, at, :]
                t = jnp.where(dd == c * LANES, zc, t)
                ez[i * wide + c, at, :] = jnp.exp(zc - m)
            t_run[at, :] = t
        return carry

    lax.fori_loop(0, items // WEIGHT_TILE, weights, 0)
    t_col = jnp.broadcast_to(jnp.sum(t_run[...], axis=1, keepdims=True), lab.shape)
    targets[me] = t_col.T[0:8, :]
    arrive(stats.at[others], 2)
    big = stats[0, 0:1, :]
    for p in range(1, n):
        big = jnp.maximum(big, stats[p, 0:1, :])
    total = jnp.zeros_like(big)
    for p in range(n):
        total = total + stats[p, 1:2, :] * jnp.exp(stats[p, 0:1, :] - big)
    inv = 1.0 / (total * rows)
    big_col = jnp.broadcast_to(big, (rows, LANES)).T
    inv_col = jnp.broadcast_to(inv, (rows, LANES)).T
    hit_col = (jnp.exp(t_col - big_col) * inv_col - 1.0 / rows).astype(BF16)
    scale = jnp.exp(m_run[...] - big_col) * inv_col
    home = jnp.where(local - local // LANES * LANES == lane, local // LANES, -1)
    home = jnp.where((local >= 0) & (local < items), home, -1).astype(F32)

    def second_pass(i, carry):
        gs = []
        count = SECOND_TILE // LANES
        here = (home - (i * count).astype(F32)).astype(BF16)
        for c in range(count):
            g = (ez[i * count + c] * scale).astype(BF16)
            g = jnp.where(here == jnp.bfloat16(c), hit_col, g)
            g_ref[i * count + c, :rows, :] = g
            gs.append(g)
        base = pl.multiple_of(i * SECOND_TILE, SECOND_TILE)
        part[...] += dot(jnp.concatenate(gs, axis=1), cat[pl.ds(base, SECOND_TILE), :], (1, 0))
        return carry

    lax.fori_loop(0, items // SECOND_TILE, second_pass, 0)

    exchange(lambda p: part.at[rows_of(p)], pieces.at[me], 3)
    pieces[me] = part[my_rows, :]

    def item_grads(i, carry):
        count = OUT_TILE // LANES
        g = jnp.concatenate([g_ref[i * count + c, :rows, :] for c in range(count)], axis=1)
        cat[pl.ds(pl.multiple_of(i * OUT_TILE, OUT_TILE), OUT_TILE), :] = dot(g, x_ref[...], (0, 0)).astype(BF16)
        return carry

    lax.fori_loop(0, EARLY, item_grads, 0)
    exchange(lambda p: targets.at[me], targets.at[me], 5)
    arrive(pieces.at[others], 3)
    acc = pieces[0]
    for p in range(1, n):
        acc = acc + pieces[p]
    dx_ref[my_rows, :] = acc.astype(BF16)
    exchange(lambda p: dx_ref.at[my_rows], dx_ref.at[my_rows], 4)
    lax.fori_loop(EARLY, items // OUT_TILE, item_grads, 0)
    arrive(q_ref.at[other_rows], 6)
    a = dot(q_ref[...], w1[...], (1, 0))
    a_ref[...] = a
    h_ref[...] = jnp.maximum(a, 0.0).astype(BF16)
    arrive(dx_ref.at[other_rows], 4)
    arrive(targets.at[others], 5)
    target = targets[0, 0:1, :]
    for p in range(1, n):
        target = target + targets[p, 0:1, :]
    loss_ref[...] = jnp.broadcast_to(
        jnp.sum(big + jnp.log(total) - target, axis=1, keepdims=True) / rows, loss_ref.shape)
    sent(lab.at[other_rows], 0)
    sent(x_ref.at[other_rows], 1)
    sent(q_ref.at[other_rows], 6)
    sent(stats.at[others], 2)
    sent(pieces.at[others], 3)
    sent(dx_ref.at[other_rows], 4)
    sent(targets.at[others], 5)


def grad_kernel(de_ref, dx_ref, h_ref, a_ref, q_ref, w2_ref, loss_ref,
                loss_hbm, de_hbm, dw1_hbm, dw2_hbm, loss, dw1, dw2, sem):
    copies = []
    for k in range(de_hbm.shape[0] // LOAD_TILE):
        at = pl.ds(k * LOAD_TILE, LOAD_TILE)
        pltpu.make_async_copy(de_ref.at[at], de_hbm.at[at], sem.at[3]).start()
    dx = dx_ref[...]
    dw2[...] = dot(h_ref[...], dx, (0, 0)).astype(BF16)
    dh = dot(dx, w2_ref[...], (1, 1))
    da = jnp.where(a_ref[...] > 0.0, dh, 0.0).astype(BF16)
    dw1[...] = dot(q_ref[...], da, (0, 0)).astype(BF16)
    loss[...] = loss_ref[0:1, 0:1]
    copies.append(pltpu.make_async_copy(loss, loss_hbm, sem.at[0]))
    copies.append(pltpu.make_async_copy(dw1, dw1_hbm, sem.at[1]))
    copies.append(pltpu.make_async_copy(dw2, dw2_hbm, sem.at[2]))
    for copy in copies[-3:]:
        copy.start()
    for copy in copies:
        copy.wait()
    pltpu.make_async_copy(de_ref, de_hbm, sem.at[3]).wait()


def solution(mesh):
    n = mesh.shape["tp"]

    def local_step(queries, w_first, w_second, catalogue, log_q, labels):
        own, d_in = queries.shape
        hid, emb = w_second.shape
        items = catalogue.shape[0]
        rows = own * n
        hbm = pl.BlockSpec(memory_space=pl.ANY)
        vmem = pl.BlockSpec(memory_space=pltpu.VMEM)
        dma = pltpu.SemaphoreType.DMA
        held = pl.pallas_call(
            functools.partial(loss_kernel, n),
            name="loss_kernel",
            out_shape=[
                pltpu.VMEM((items, emb), BF16),
                pltpu.VMEM((rows, emb), BF16),
                pltpu.VMEM((rows, hid), BF16),
                pltpu.VMEM((rows, hid), F32),
                pltpu.VMEM((rows, d_in), BF16),
                pltpu.VMEM((hid, emb), BF16),
                pltpu.VMEM((32, LANES), F32),
            ],
            in_specs=[hbm] * 6,
            out_specs=[vmem] * 7,
            scratch_shapes=[
                pltpu.VMEM((rows, emb), BF16),
                pltpu.VMEM((items // LANES, rows + SHIFT, LANES), BF16),
                pltpu.VMEM((items // LANES, rows, LANES), F32),
                pltpu.VMEM((2 * SHIFT + TILE // LANES * rows, LANES), F32),
                pltpu.VMEM((2 * SHIFT + TILE // LANES * rows, LANES), F32),
                pltpu.VMEM((1, items), F32),
                pltpu.VMEM((d_in, hid), BF16),
                pltpu.SMEM((own,), jnp.int32),
                pltpu.VMEM((rows, LANES), jnp.int32),
                pltpu.VMEM((rows, LANES), jnp.int32),
                pltpu.VMEM((rows, LANES), F32),
                pltpu.VMEM((rows, LANES), F32),
                pltpu.VMEM((rows, LANES), F32),
                pltpu.VMEM((items // TILE + 1, rows, LANES), F32),
                pltpu.VMEM((n, 8, LANES), F32),
                pltpu.VMEM((n, 8, LANES), F32),
                pltpu.VMEM((rows, emb), F32),
                pltpu.VMEM((n, own, emb), F32),
                dma((5,)),
                dma((items // LOAD_TILE,)),
                dma((7,)),
                dma((7,)),
            ],
            compiler_params=pltpu.CompilerParams(collective_id=0, has_side_effects=True, vmem_limit_bytes=44 << 20),
        )(queries, w_first, w_second, catalogue, log_q.reshape(1, items), labels)
        loss, grad_items, grad_first, grad_second = pl.pallas_call(
            grad_kernel,
            name="grad_kernel",
            out_shape=[
                jax.ShapeDtypeStruct((1, 1), F32),
                jax.ShapeDtypeStruct((items, emb), BF16),
                jax.ShapeDtypeStruct((d_in, hid), BF16),
                jax.ShapeDtypeStruct((hid, emb), BF16),
            ],
            in_specs=[vmem] * 7,
            out_specs=[hbm] * 4,
            scratch_shapes=[
                pltpu.VMEM((1, 1), F32),
                pltpu.VMEM((d_in, hid), BF16),
                pltpu.VMEM((hid, emb), BF16),
                dma((4,)),
            ],
            compiler_params=pltpu.CompilerParams(vmem_limit_bytes=24 << 20),
        )(*held)
        return loss.reshape(1), grad_items, grad_first, grad_second

    row_spec = P(("dp", "tp"), None)
    return jax.shard_map(
        local_step, mesh=mesh,
        in_specs=(row_spec, P(None, None), P(None, None), P("tp", None), P("tp"), P(("dp", "tp"))),
        out_specs=(P("dp"), row_spec, P("dp", None), P("dp", None)), check_vma=False)
```

```python
import functools

import jax
import jax.numpy as jnp
from jax import lax
from jax.experimental import pallas as pl
from jax.experimental.pallas import tpu as pltpu
from jax.sharding import PartitionSpec as P

F32, BF16 = jnp.float32, jnp.bfloat16
MESH = pl.DeviceIdType.MESH
LANES = 128
TILE = 2048
UNROLL = 4
DOT_TILE = 512
GROUP = 32
WEIGHT_TILE = 4096
WEIGHT_GROUP = 16
SECOND_TILE = 8192
LOAD_TILE = 4096
OUT_TILE = 4096
EARLY = 5
SHIFT = 16
LOWEST = -3.0e38


def dot(a, b, contract):
    return lax.dot_general(a, b, ((contract[:1], contract[1:]), ((), ())), preferred_element_type=F32)


def loss_kernel(n, q_hbm, w1_hbm, w2_hbm, cat_hbm, lq_hbm, lab_hbm,
                cat, dx_ref, h_ref, a_ref, q_ref, w2_ref, loss_ref,
                x_ref, g_ref, ez, z_even, z_odd, lq, w1, labels, lab, d, m_run, s_run, t_run, m_hist, stats, targets, part, pieces,
                load_sem, cat_sem, send_sem, recv_sem):
    me = lax.axis_index("tp")
    own = q_hbm.shape[0]
    rows = own * n
    items = cat_hbm.shape[0]
    tiles = items // TILE
    chunks = TILE // LANES
    my_rows = pl.ds(pl.multiple_of(me * own, own), own)

    others = pl.ds(0, n - 1)
    other_rows = pl.ds(0, rows - own)

    q_load = pltpu.make_async_copy(q_hbm, q_ref.at[my_rows], load_sem.at[0])
    w1_load = pltpu.make_async_copy(w1_hbm, w1, load_sem.at[1])
    w2_load = pltpu.make_async_copy(w2_hbm, w2_ref, load_sem.at[2])
    lq_load = pltpu.make_async_copy(lq_hbm, lq, load_sem.at[3])
    lab_load = pltpu.make_async_copy(lab_hbm, labels, load_sem.at[4])
    for load in (q_load, w1_load, w2_load):
        load.start()
    barrier = pltpu.get_barrier_semaphore()
    peers = [lax.rem(me + k, n) for k in sorted(range(1, n), key=lambda k: -min(k, n - k))]
    for p in peers:
        pl.semaphore_signal(barrier, inc=1, device_id={"tp": p}, device_id_type=MESH)
    for load in (lq_load, lab_load):
        load.start()

    def cat_copy(k):
        part_rows = pl.ds(pl.multiple_of(k * LOAD_TILE, LOAD_TILE), LOAD_TILE)
        return pltpu.make_async_copy(cat_hbm.at[part_rows], cat.at[part_rows], cat_sem.at[k])

    q_load.wait()
    w1_load.wait()
    w2_load.wait()
    for k in range(items // LOAD_TILE):
        cat_copy(k).start()
    own_hidden = jnp.maximum(dot(q_ref[my_rows, :], w1[...], (1, 0)), 0.0).astype(BF16)
    x_ref[my_rows, :] = dot(own_hidden, w2_ref[...], (1, 0)).astype(BF16)
    pl.semaphore_wait(barrier, n - 1)

    def exchange(src, dst, stage):
        for p in peers:
            pltpu.make_async_remote_copy(
                src_ref=src(p), dst_ref=dst, send_sem=send_sem.at[stage], recv_sem=recv_sem.at[stage],
                device_id={"tp": p}, device_id_type=MESH).start()

    def arrive(others, stage):
        pltpu.make_async_copy(others, others, recv_sem.at[stage]).wait()

    def sent(others, stage):
        pltpu.make_async_copy(others, others, send_sem.at[stage]).wait()

    def rows_of(p):
        return pl.ds(pl.multiple_of(p * own, own), own)

    exchange(lambda p: x_ref.at[my_rows], x_ref.at[my_rows], 1)
    lq_load.wait()
    lab_load.wait()
    for r in range(own):
        lab[pl.ds(me * own + r, 1), :] = jnp.full((1, LANES), labels[r], jnp.int32)
    m_run[...] = jnp.full(m_run.shape, LOWEST, F32)
    s_run[...] = jnp.zeros(s_run.shape, F32)
    part[...] = jnp.zeros(part.shape, F32)
    arrive(x_ref.at[other_rows], 1)

    def logits(i, z_ref):
        for j in range(TILE // DOT_TILE):
            base = pl.multiple_of(i * TILE + j * DOT_TILE, DOT_TILE)
            z = dot(x_ref[...], cat[pl.ds(base, DOT_TILE), :], (1, 1)) - lq[:, pl.ds(base, DOT_TILE)]
            m = m_run[...]
            for c in range(DOT_TILE // LANES):
                zc = z[:, c * LANES:(c + 1) * LANES]
                z_ref[pl.ds(SHIFT + (j * (DOT_TILE // LANES) + c) * rows, rows), :] = zc
                ez[i * chunks + j * (DOT_TILE // LANES) + c] = zc
                m = jnp.maximum(m, zc)
            m_run[...] = m
            yield
        m_hist[i + 1] = m

    def weigh(i, z_ref):
        for r in range(0, rows, GROUP):
            at = slice(r, r + GROUP)
            m = m_hist[i + 1, at, :]
            s = s_run[at, :] * jnp.exp(m_hist[i, at, :] - m)
            for c in range(chunks):
                s = s + jnp.exp(z_ref[pl.ds(SHIFT + c * rows + r, GROUP), :] - m)
            s_run[at, :] = s
            yield

    def arrived(j):
        for k in range(UNROLL * TILE // LOAD_TILE):
            cat_copy(j * (UNROLL * TILE // LOAD_TILE) + k).wait()

    def together(*parts):
        parts = list(parts)
        while parts:
            parts = [p for p in parts if next(p, parts) is not parts]

    z_refs = (z_even, z_odd)

    def step(i, k):
        together(logits(i + 1, z_refs[(k + 1) % 2]), weigh(i, z_refs[k % 2]))

    m_hist[0] = m_run[...]
    arrived(0)
    together(logits(0, z_even))
    exchange(lambda p: lab.at[my_rows], lab.at[my_rows], 0)
    exchange(lambda p: q_ref.at[my_rows], q_ref.at[my_rows], 6)

    def first_pass(j, carry):
        arrived(j + 1)
        for k in range(UNROLL):
            step(j * UNROLL + k, k)
        return carry

    lax.fori_loop(0, tiles // UNROLL - 1, first_pass, 0)
    for k in range(UNROLL - 1):
        step(tiles - UNROLL + k, k)
    together(weigh(tiles - 1, z_odd))

    m_t = m_run[...].T
    m_row = jnp.max(m_t, axis=0, keepdims=True)
    s_row = jnp.sum(s_run[...].T * jnp.exp(m_t - m_row), axis=0, keepdims=True)
    sub = lax.broadcasted_iota(jnp.int32, (8, LANES), 0)
    stats[me] = jnp.where(sub == 0, m_row, s_row)
    exchange(lambda p: stats.at[me], stats.at[me], 2)
    t_run[...] = jnp.zeros(t_run.shape, F32)
    arrive(lab.at[other_rows], 0)
    local = lab[...] - me * items
    lane = lax.broadcasted_iota(jnp.int32, lab.shape, 1)
    d[...] = local - lane
    wide = WEIGHT_TILE // LANES

    def weights(i, carry):
        for r in range(0, rows, WEIGHT_GROUP):
            at = slice(r, r + WEIGHT_GROUP)
            m = m_run[at, :]
            t = t_run[at, :]
            dd = d[at, :] - i * WEIGHT_TILE
            for c in range(wide):
                zc = ez[i * wide + c, at, :]
                t = jnp.where(dd == c * LANES, zc, t)
                ez[i * wide + c, at, :] = jnp.exp(zc - m)
            t_run[at, :] = t
        return carry

    lax.fori_loop(0, items // WEIGHT_TILE, weights, 0)
    t_col = jnp.broadcast_to(jnp.sum(t_run[...], axis=1, keepdims=True), lab.shape)
    targets[me] = t_col.T[0:8, :]
    arrive(stats.at[others], 2)
    big = stats[0, 0:1, :]
    for p in range(1, n):
        big = jnp.maximum(big, stats[p, 0:1, :])
    total = jnp.zeros_like(big)
    for p in range(n):
        total = total + stats[p, 1:2, :] * jnp.exp(stats[p, 0:1, :] - big)
    inv = 1.0 / (total * rows)
    big_col = jnp.broadcast_to(big, (rows, LANES)).T
    inv_col = jnp.broadcast_to(inv, (rows, LANES)).T
    hit_col = (jnp.exp(t_col - big_col) * inv_col - 1.0 / rows).astype(BF16)
    scale = jnp.exp(m_run[...] - big_col) * inv_col
    home = jnp.where(local - local // LANES * LANES == lane, local // LANES, -1)
    home = jnp.where((local >= 0) & (local < items), home, -1).astype(F32)

    def second_pass(i, carry):
        gs = []
        count = SECOND_TILE // LANES
        here = (home - (i * count).astype(F32)).astype(BF16)
        for c in range(count):
            g = (ez[i * count + c] * scale).astype(BF16)
            g = jnp.where(here == jnp.bfloat16(c), hit_col, g)
            g_ref[i * count + c, :rows, :] = g
            gs.append(g)
        base = pl.multiple_of(i * SECOND_TILE, SECOND_TILE)
        part[...] += dot(jnp.concatenate(gs, axis=1), cat[pl.ds(base, SECOND_TILE), :], (1, 0))
        return carry

    lax.fori_loop(0, items // SECOND_TILE, second_pass, 0)

    exchange(lambda p: part.at[rows_of(p)], pieces.at[me], 3)
    pieces[me] = part[my_rows, :]

    def item_grads(i, carry):
        count = OUT_TILE // LANES
        g = jnp.concatenate([g_ref[i * count + c, :rows, :] for c in range(count)], axis=1)
        cat[pl.ds(pl.multiple_of(i * OUT_TILE, OUT_TILE), OUT_TILE), :] = dot(g, x_ref[...], (0, 0)).astype(BF16)
        return carry

    lax.fori_loop(0, EARLY, item_grads, 0)
    exchange(lambda p: targets.at[me], targets.at[me], 5)
    arrive(pieces.at[others], 3)
    acc = pieces[0]
    for p in range(1, n):
        acc = acc + pieces[p]
    dx_ref[my_rows, :] = acc.astype(BF16)
    exchange(lambda p: dx_ref.at[my_rows], dx_ref.at[my_rows], 4)
    lax.fori_loop(EARLY, items // OUT_TILE, item_grads, 0)
    arrive(q_ref.at[other_rows], 6)
    a = dot(q_ref[...], w1[...], (1, 0))
    a_ref[...] = a
    h_ref[...] = jnp.maximum(a, 0.0).astype(BF16)
    arrive(dx_ref.at[other_rows], 4)
    arrive(targets.at[others], 5)
    target = targets[0, 0:1, :]
    for p in range(1, n):
        target = target + targets[p, 0:1, :]
    loss_ref[...] = jnp.broadcast_to(
        jnp.sum(big + jnp.log(total) - target, axis=1, keepdims=True) / rows, loss_ref.shape)
    sent(lab.at[other_rows], 0)
    sent(x_ref.at[other_rows], 1)
    sent(q_ref.at[other_rows], 6)
    sent(stats.at[others], 2)
    sent(pieces.at[others], 3)
    sent(dx_ref.at[other_rows], 4)
    sent(targets.at[others], 5)


def grad_kernel(de_ref, dx_ref, h_ref, a_ref, q_ref, w2_ref, loss_ref,
                loss_hbm, de_hbm, dw1_hbm, dw2_hbm, loss, dw1, dw2, sem):
    copies = []

    def start_copy(k, carry):
        at = pl.ds(pl.multiple_of(k * LOAD_TILE, LOAD_TILE), LOAD_TILE)
        pltpu.make_async_copy(de_ref.at[at], de_hbm.at[at], sem.at[3]).start()
        return carry

    lax.fori_loop(0, de_hbm.shape[0] // LOAD_TILE, start_copy, 0)
    dx = dx_ref[...]
    dw2[...] = dot(h_ref[...], dx, (0, 0)).astype(BF16)
    dh = dot(dx, w2_ref[...], (1, 1))
    da = jnp.where(a_ref[...] > 0.0, dh, 0.0).astype(BF16)
    dw1[...] = dot(q_ref[...], da, (0, 0)).astype(BF16)
    loss[...] = loss_ref[0:1, 0:1]
    copies.append(pltpu.make_async_copy(loss, loss_hbm, sem.at[0]))
    copies.append(pltpu.make_async_copy(dw1, dw1_hbm, sem.at[1]))
    copies.append(pltpu.make_async_copy(dw2, dw2_hbm, sem.at[2]))
    for copy in copies[-3:]:
        copy.start()
    for copy in copies:
        copy.wait()
    pltpu.make_async_copy(de_ref, de_hbm, sem.at[3]).wait()


def solution(mesh):
    n = mesh.shape["tp"]

    def local_step(queries, w_first, w_second, catalogue, log_q, labels):
        own, d_in = queries.shape
        hid, emb = w_second.shape
        items = catalogue.shape[0]
        rows = own * n
        hbm = pl.BlockSpec(memory_space=pl.ANY)
        vmem = pl.BlockSpec(memory_space=pltpu.VMEM)
        dma = pltpu.SemaphoreType.DMA
        held = pl.pallas_call(
            functools.partial(loss_kernel, n),
            name="loss_kernel",
            out_shape=[
                pltpu.VMEM((items, emb), BF16),
                pltpu.VMEM((rows, emb), BF16),
                pltpu.VMEM((rows, hid), BF16),
                pltpu.VMEM((rows, hid), F32),
                pltpu.VMEM((rows, d_in), BF16),
                pltpu.VMEM((hid, emb), BF16),
                pltpu.VMEM((32, LANES), F32),
            ],
            in_specs=[hbm] * 6,
            out_specs=[vmem] * 7,
            scratch_shapes=[
                pltpu.VMEM((rows, emb), BF16),
                pltpu.VMEM((items // LANES, rows + SHIFT, LANES), BF16),
                pltpu.VMEM((items // LANES, rows, LANES), F32),
                pltpu.VMEM((2 * SHIFT + TILE // LANES * rows, LANES), F32),
                pltpu.VMEM((2 * SHIFT + TILE // LANES * rows, LANES), F32),
                pltpu.VMEM((1, items), F32),
                pltpu.VMEM((d_in, hid), BF16),
                pltpu.SMEM((own,), jnp.int32),
                pltpu.VMEM((rows, LANES), jnp.int32),
                pltpu.VMEM((rows, LANES), jnp.int32),
                pltpu.VMEM((rows, LANES), F32),
                pltpu.VMEM((rows, LANES), F32),
                pltpu.VMEM((rows, LANES), F32),
                pltpu.VMEM((items // TILE + 1, rows, LANES), F32),
                pltpu.VMEM((n, 8, LANES), F32),
                pltpu.VMEM((n, 8, LANES), F32),
                pltpu.VMEM((rows, emb), F32),
                pltpu.VMEM((n, own, emb), F32),
                dma((5,)),
                dma((items // LOAD_TILE,)),
                dma((7,)),
                dma((7,)),
            ],
            compiler_params=pltpu.CompilerParams(collective_id=0, has_side_effects=True, vmem_limit_bytes=44 << 20),
        )(queries, w_first, w_second, catalogue, log_q.reshape(1, items), labels)
        loss, grad_items, grad_first, grad_second = pl.pallas_call(
            grad_kernel,
            name="grad_kernel",
            out_shape=[
                jax.ShapeDtypeStruct((1, 1), F32),
                jax.ShapeDtypeStruct((items, emb), BF16),
                jax.ShapeDtypeStruct((d_in, hid), BF16),
                jax.ShapeDtypeStruct((hid, emb), BF16),
            ],
            in_specs=[vmem] * 7,
            out_specs=[hbm] * 4,
            scratch_shapes=[
                pltpu.VMEM((1, 1), F32),
                pltpu.VMEM((d_in, hid), BF16),
                pltpu.VMEM((hid, emb), BF16),
                dma((4,)),
            ],
            compiler_params=pltpu.CompilerParams(vmem_limit_bytes=24 << 20),
        )(*held)
        return loss.reshape(1), grad_items, grad_first, grad_second

    row_spec = P(("dp", "tp"), None)
    return jax.shard_map(
        local_step, mesh=mesh,
        in_specs=(row_spec, P(None, None), P(None, None), P("tp", None), P("tp"), P(("dp", "tp"))),
        out_specs=(P("dp"), row_spec, P("dp", None), P("dp", None)), check_vma=False)
```

```python
import functools

import jax
import jax.numpy as jnp
from jax import lax
from jax.experimental import pallas as pl
from jax.experimental.pallas import tpu as pltpu
from jax.sharding import PartitionSpec as P

F32, BF16 = jnp.float32, jnp.bfloat16
MESH = pl.DeviceIdType.MESH
LANES = 128
TILE = 2048
UNROLL = 4
DOT_TILE = 512
GROUP = 16
WEIGHT_TILE = 4096
WEIGHT_GROUP = 16
SECOND_TILE = 16384
LOAD_TILE = 4096
OUT_TILE = 4096
EARLY = 5
SHIFT = 16
LOWEST = -3.0e38


def dot(a, b, contract):
    return lax.dot_general(a, b, ((contract[:1], contract[1:]), ((), ())), preferred_element_type=F32)


def loss_kernel(n, q_hbm, w1_hbm, w2_hbm, cat_hbm, lq_hbm, lab_hbm,
                cat, dx_ref, h_ref, a_ref, q_ref, w2_ref, loss_ref,
                x_ref, g_ref, ez, lq, w1, labels, lab, d, m_run, s_run, t_run, m_hist, stats, targets, part, pieces,
                load_sem, cat_sem, send_sem, recv_sem):
    me = lax.axis_index("tp")
    own = q_hbm.shape[0]
    rows = own * n
    items = cat_hbm.shape[0]
    tiles = items // TILE
    chunks = TILE // LANES
    my_rows = pl.ds(pl.multiple_of(me * own, own), own)

    others = pl.ds(0, n - 1)
    other_rows = pl.ds(0, rows - own)

    q_load = pltpu.make_async_copy(q_hbm, q_ref.at[my_rows], load_sem.at[0])
    w1_load = pltpu.make_async_copy(w1_hbm, w1, load_sem.at[1])
    w2_load = pltpu.make_async_copy(w2_hbm, w2_ref, load_sem.at[2])
    lq_load = pltpu.make_async_copy(lq_hbm, lq, load_sem.at[3])
    lab_load = pltpu.make_async_copy(lab_hbm, labels, load_sem.at[4])
    for load in (q_load, w1_load, w2_load):
        load.start()
    barrier = pltpu.get_barrier_semaphore()
    peers = [lax.rem(me + k, n) for k in sorted(range(1, n), key=lambda k: -min(k, n - k))]
    for p in peers:
        pl.semaphore_signal(barrier, inc=1, device_id={"tp": p}, device_id_type=MESH)
    for load in (lq_load, lab_load):
        load.start()

    def cat_copy(k):
        part_rows = pl.ds(pl.multiple_of(k * LOAD_TILE, LOAD_TILE), LOAD_TILE)
        return pltpu.make_async_copy(cat_hbm.at[part_rows], cat.at[part_rows], cat_sem.at[k])

    q_load.wait()
    w1_load.wait()
    w2_load.wait()
    for k in range(items // LOAD_TILE):
        cat_copy(k).start()
    own_hidden = jnp.maximum(dot(q_ref[my_rows, :], w1[...], (1, 0)), 0.0).astype(BF16)
    x_ref[my_rows, :] = dot(own_hidden, w2_ref[...], (1, 0)).astype(BF16)
    pl.semaphore_wait(barrier, n - 1)

    def exchange(src, dst, stage):
        for p in peers:
            pltpu.make_async_remote_copy(
                src_ref=src(p), dst_ref=dst, send_sem=send_sem.at[stage], recv_sem=recv_sem.at[stage],
                device_id={"tp": p}, device_id_type=MESH).start()

    def arrive(others, stage):
        pltpu.make_async_copy(others, others, recv_sem.at[stage]).wait()

    def sent(others, stage):
        pltpu.make_async_copy(others, others, send_sem.at[stage]).wait()

    def rows_of(p):
        return pl.ds(pl.multiple_of(p * own, own), own)

    exchange(lambda p: x_ref.at[my_rows], x_ref.at[my_rows], 1)
    lq_load.wait()
    lab_load.wait()
    for r in range(own):
        lab[pl.ds(me * own + r, 1), :] = jnp.full((1, LANES), labels[r], jnp.int32)
    m_run[...] = jnp.full(m_run.shape, LOWEST, F32)
    s_run[...] = jnp.zeros(s_run.shape, F32)
    part[...] = jnp.zeros(part.shape, F32)
    arrive(x_ref.at[other_rows], 1)

    def logits(j, k):
        for p in range(TILE // DOT_TILE):
            items_at = pl.ds(pl.multiple_of(j * UNROLL * TILE, TILE) + (k * TILE + p * DOT_TILE), DOT_TILE)
            z = dot(x_ref[...], cat[items_at, :], (1, 1)) - lq[:, items_at]
            m = m_run[...]
            for c in range(DOT_TILE // LANES):
                zc = z[:, c * LANES:(c + 1) * LANES]
                ez[j * UNROLL * chunks + (k * chunks + p * (DOT_TILE // LANES) + c)] = zc
                m = jnp.maximum(m, zc)
            m_run[...] = m
            yield
        m_hist[j * UNROLL + (k + 1)] = m

    def weigh(j, k):
        for r in range(0, rows, GROUP):
            at = slice(r, r + GROUP)
            m = m_hist[j * UNROLL + (k + 1), at, :]
            s = s_run[at, :] * jnp.exp(m_hist[j * UNROLL + k, at, :] - m)
            for c in range(chunks):
                s = s + jnp.exp(ez[j * UNROLL * chunks + (k * chunks + c), at, :] - m)
            s_run[at, :] = s
            yield

    def arrived(j):
        for k in range(UNROLL * TILE // LOAD_TILE):
            cat_copy(j * (UNROLL * TILE // LOAD_TILE) + k).wait()

    def together(*parts):
        parts = list(parts)
        while parts:
            parts = [p for p in parts if next(p, parts) is not parts]

    m_hist[0] = m_run[...]
    arrived(0)
    together(logits(0, 0))
    exchange(lambda p: lab.at[my_rows], lab.at[my_rows], 0)
    exchange(lambda p: q_ref.at[my_rows], q_ref.at[my_rows], 6)

    def first_pass(j, carry):
        arrived(j + 1)
        for k in range(UNROLL):
            together(logits(j, k + 1), weigh(j, k))
        return carry

    trips = tiles // UNROLL - 1
    lax.fori_loop(0, trips, first_pass, 0)
    for k in range(UNROLL - 1):
        together(logits(trips, k + 1), weigh(trips, k))
    together(weigh(trips, UNROLL - 1))

    m_t = m_run[...].T
    m_row = jnp.max(m_t, axis=0, keepdims=True)
    s_row = jnp.sum(s_run[...].T * jnp.exp(m_t - m_row), axis=0, keepdims=True)
    sub = lax.broadcasted_iota(jnp.int32, (8, LANES), 0)
    stats[me] = jnp.where(sub == 0, m_row, s_row)
    exchange(lambda p: stats.at[me], stats.at[me], 2)
    t_run[...] = jnp.zeros(t_run.shape, F32)
    arrive(lab.at[other_rows], 0)
    local = lab[...] - me * items
    lane = lax.broadcasted_iota(jnp.int32, lab.shape, 1)
    d[...] = local - lane
    wide = WEIGHT_TILE // LANES

    def weights(i, carry):
        for r in range(0, rows, WEIGHT_GROUP):
            at = slice(r, r + WEIGHT_GROUP)
            m = m_run[at, :]
            t = t_run[at, :]
            dd = d[at, :] - i * WEIGHT_TILE
            for c in range(wide):
                zc = ez[i * wide + c, at, :]
                t = jnp.where(dd == c * LANES, zc, t)
                ez[i * wide + c, at, :] = jnp.exp(zc - m)
            t_run[at, :] = t
        return carry

    lax.fori_loop(0, items // WEIGHT_TILE, weights, 0)
    t_col = jnp.broadcast_to(jnp.sum(t_run[...], axis=1, keepdims=True), lab.shape)
    targets[me] = t_col.T[0:8, :]
    arrive(stats.at[others], 2)
    big = stats[0, 0:1, :]
    for p in range(1, n):
        big = jnp.maximum(big, stats[p, 0:1, :])
    total = jnp.zeros_like(big)
    for p in range(n):
        total = total + stats[p, 1:2, :] * jnp.exp(stats[p, 0:1, :] - big)
    inv = 1.0 / (total * rows)
    big_col = jnp.broadcast_to(big, (rows, LANES)).T
    inv_col = jnp.broadcast_to(inv, (rows, LANES)).T
    hit_col = (jnp.exp(t_col - big_col) * inv_col - 1.0 / rows).astype(BF16)
    scale = jnp.exp(m_run[...] - big_col) * inv_col
    home = jnp.where(local - local // LANES * LANES == lane, local // LANES, -1)
    home = jnp.where((local >= 0) & (local < items), home, -1).astype(F32)

    def second_pass(i, carry):
        gs = []
        count = SECOND_TILE // LANES
        here = (home - (i * count).astype(F32)).astype(BF16)
        for c in range(count):
            g = (ez[i * count + c] * scale).astype(BF16)
            g = jnp.where(here == jnp.bfloat16(c), hit_col, g)
            g_ref[i * count + c, :rows, :] = g
            gs.append(g)
        base = pl.multiple_of(i * SECOND_TILE, SECOND_TILE)
        part[...] += dot(jnp.concatenate(gs, axis=1), cat[pl.ds(base, SECOND_TILE), :], (1, 0))
        return carry

    lax.fori_loop(0, items // SECOND_TILE, second_pass, 0)

    exchange(lambda p: part.at[rows_of(p)], pieces.at[me], 3)
    pieces[me] = part[my_rows, :]

    def item_grads(i, carry):
        count = OUT_TILE // LANES
        g = jnp.concatenate([g_ref[i * count + c, :rows, :] for c in range(count)], axis=1)
        cat[pl.ds(pl.multiple_of(i * OUT_TILE, OUT_TILE), OUT_TILE), :] = dot(g, x_ref[...], (0, 0)).astype(BF16)
        return carry

    lax.fori_loop(0, EARLY, item_grads, 0)
    exchange(lambda p: targets.at[me], targets.at[me], 5)
    arrive(pieces.at[others], 3)
    acc = pieces[0]
    for p in range(1, n):
        acc = acc + pieces[p]
    dx_ref[my_rows, :] = acc.astype(BF16)
    exchange(lambda p: dx_ref.at[my_rows], dx_ref.at[my_rows], 4)
    lax.fori_loop(EARLY, items // OUT_TILE, item_grads, 0)
    arrive(q_ref.at[other_rows], 6)
    a = dot(q_ref[...], w1[...], (1, 0))
    a_ref[...] = a
    h_ref[...] = jnp.maximum(a, 0.0).astype(BF16)
    arrive(dx_ref.at[other_rows], 4)
    arrive(targets.at[others], 5)
    target = targets[0, 0:1, :]
    for p in range(1, n):
        target = target + targets[p, 0:1, :]
    loss_ref[...] = jnp.broadcast_to(
        jnp.sum(big + jnp.log(total) - target, axis=1, keepdims=True) / rows, loss_ref.shape)
    sent(lab.at[other_rows], 0)
    sent(x_ref.at[other_rows], 1)
    sent(q_ref.at[other_rows], 6)
    sent(stats.at[others], 2)
    sent(pieces.at[others], 3)
    sent(dx_ref.at[other_rows], 4)
    sent(targets.at[others], 5)


def grad_kernel(de_ref, dx_ref, h_ref, a_ref, q_ref, w2_ref, loss_ref,
                loss_hbm, de_hbm, dw1_hbm, dw2_hbm, loss, dw1, dw2, sem):
    copies = []

    def start_copy(k, carry):
        at = pl.ds(pl.multiple_of(k * LOAD_TILE, LOAD_TILE), LOAD_TILE)
        pltpu.make_async_copy(de_ref.at[at], de_hbm.at[at], sem.at[3]).start()
        return carry

    lax.fori_loop(0, de_hbm.shape[0] // LOAD_TILE, start_copy, 0)
    dx = dx_ref[...]
    dw2[...] = dot(h_ref[...], dx, (0, 0)).astype(BF16)
    dh = dot(dx, w2_ref[...], (1, 1))
    da = jnp.where(a_ref[...] > 0.0, dh, 0.0).astype(BF16)
    dw1[...] = dot(q_ref[...], da, (0, 0)).astype(BF16)
    loss[...] = loss_ref[0:1, 0:1]
    copies.append(pltpu.make_async_copy(loss, loss_hbm, sem.at[0]))
    copies.append(pltpu.make_async_copy(dw1, dw1_hbm, sem.at[1]))
    copies.append(pltpu.make_async_copy(dw2, dw2_hbm, sem.at[2]))
    for copy in copies[-3:]:
        copy.start()
    for copy in copies:
        copy.wait()
    pltpu.make_async_copy(de_ref, de_hbm, sem.at[3]).wait()


def solution(mesh):
    n = mesh.shape["tp"]

    def local_step(queries, w_first, w_second, catalogue, log_q, labels):
        own, d_in = queries.shape
        hid, emb = w_second.shape
        items = catalogue.shape[0]
        rows = own * n
        hbm = pl.BlockSpec(memory_space=pl.ANY)
        vmem = pl.BlockSpec(memory_space=pltpu.VMEM)
        dma = pltpu.SemaphoreType.DMA
        held = pl.pallas_call(
            functools.partial(loss_kernel, n),
            name="loss_kernel",
            out_shape=[
                pltpu.VMEM((items, emb), BF16),
                pltpu.VMEM((rows, emb), BF16),
                pltpu.VMEM((rows, hid), BF16),
                pltpu.VMEM((rows, hid), F32),
                pltpu.VMEM((rows, d_in), BF16),
                pltpu.VMEM((hid, emb), BF16),
                pltpu.VMEM((32, LANES), F32),
            ],
            in_specs=[hbm] * 6,
            out_specs=[vmem] * 7,
            scratch_shapes=[
                pltpu.VMEM((rows, emb), BF16),
                pltpu.VMEM((items // LANES, rows + SHIFT, LANES), BF16),
                pltpu.VMEM((items // LANES, rows, LANES), F32),
                pltpu.VMEM((1, items), F32),
                pltpu.VMEM((d_in, hid), BF16),
                pltpu.SMEM((own,), jnp.int32),
                pltpu.VMEM((rows, LANES), jnp.int32),
                pltpu.VMEM((rows, LANES), jnp.int32),
                pltpu.VMEM((rows, LANES), F32),
                pltpu.VMEM((rows, LANES), F32),
                pltpu.VMEM((rows, LANES), F32),
                pltpu.VMEM((items // TILE + 1, rows, LANES), F32),
                pltpu.VMEM((n, 8, LANES), F32),
                pltpu.VMEM((n, 8, LANES), F32),
                pltpu.VMEM((rows, emb), F32),
                pltpu.VMEM((n, own, emb), F32),
                dma((5,)),
                dma((items // LOAD_TILE,)),
                dma((7,)),
                dma((7,)),
            ],
            compiler_params=pltpu.CompilerParams(collective_id=0, has_side_effects=True, vmem_limit_bytes=44 << 20),
        )(queries, w_first, w_second, catalogue, log_q.reshape(1, items), labels)
        loss, grad_items, grad_first, grad_second = pl.pallas_call(
            grad_kernel,
            name="grad_kernel",
            out_shape=[
                jax.ShapeDtypeStruct((1, 1), F32),
                jax.ShapeDtypeStruct((items, emb), BF16),
                jax.ShapeDtypeStruct((d_in, hid), BF16),
                jax.ShapeDtypeStruct((hid, emb), BF16),
            ],
            in_specs=[vmem] * 7,
            out_specs=[hbm] * 4,
            scratch_shapes=[
                pltpu.VMEM((1, 1), F32),
                pltpu.VMEM((d_in, hid), BF16),
                pltpu.VMEM((hid, emb), BF16),
                dma((4,)),
            ],
            compiler_params=pltpu.CompilerParams(vmem_limit_bytes=24 << 20),
        )(*held)
        return loss.reshape(1), grad_items, grad_first, grad_second

    row_spec = P(("dp", "tp"), None)
    return jax.shard_map(
        local_step, mesh=mesh,
        in_specs=(row_spec, P(None, None), P(None, None), P("tp", None), P("tp"), P(("dp", "tp"))),
        out_specs=(P("dp"), row_spec, P("dp", None), P("dp", None)), check_vma=False)
```

```python
import functools

import jax
import jax.numpy as jnp
from jax import lax
from jax.experimental import pallas as pl
from jax.experimental.pallas import tpu as pltpu
from jax.sharding import PartitionSpec as P

F32, BF16 = jnp.float32, jnp.bfloat16
MESH = pl.DeviceIdType.MESH
LANES = 128
TILE = 2048
UNROLL = 4
DOT_TILE = 512
GROUP = 32
WEIGHT_TILE = 4096
WEIGHT_GROUP = 16
SECOND_TILE = 16384
LOAD_TILE = 4096
OUT_TILE = 4096
EARLY = 4
SHIFT = 16
LOWEST = -3.0e38


def dot(a, b, contract):
    return lax.dot_general(a, b, ((contract[:1], contract[1:]), ((), ())), preferred_element_type=F32)


def loss_kernel(n, q_hbm, w1_hbm, w2_hbm, cat_hbm, lq_hbm, lab_hbm,
                cat, dx_ref, h_ref, a_ref, q_ref, w2_ref, loss_ref,
                x_ref, g_ref, ez, z_even, z_odd, lq, w1, labels, lab, d, m_run, s_run, t_run, m_hist, stats, targets, part, pieces,
                load_sem, cat_sem, send_sem, recv_sem):
    me = lax.axis_index("tp")
    own = q_hbm.shape[0]
    rows = own * n
    items = cat_hbm.shape[0]
    tiles = items // TILE
    chunks = TILE // LANES
    my_rows = pl.ds(pl.multiple_of(me * own, own), own)

    others = pl.ds(0, n - 1)
    other_rows = pl.ds(0, rows - own)

    q_load = pltpu.make_async_copy(q_hbm, q_ref.at[my_rows], load_sem.at[0])
    w1_load = pltpu.make_async_copy(w1_hbm, w1, load_sem.at[1])
    w2_load = pltpu.make_async_copy(w2_hbm, w2_ref, load_sem.at[2])
    lq_load = pltpu.make_async_copy(lq_hbm, lq, load_sem.at[3])
    lab_load = pltpu.make_async_copy(lab_hbm, labels, load_sem.at[4])
    for load in (q_load, w1_load, w2_load):
        load.start()
    barrier = pltpu.get_barrier_semaphore()
    peers = [lax.rem(me + k, n) for k in sorted(range(1, n), key=lambda k: -min(k, n - k))]
    for p in peers:
        pl.semaphore_signal(barrier, inc=1, device_id={"tp": p}, device_id_type=MESH)
    for load in (lq_load, lab_load):
        load.start()

    def cat_copy(k):
        part_rows = pl.ds(pl.multiple_of(k * LOAD_TILE, LOAD_TILE), LOAD_TILE)
        return pltpu.make_async_copy(cat_hbm.at[part_rows], cat.at[part_rows], cat_sem.at[k])

    q_load.wait()
    w1_load.wait()
    w2_load.wait()
    for k in range(items // LOAD_TILE):
        cat_copy(k).start()
    own_hidden = jnp.maximum(dot(q_ref[my_rows, :], w1[...], (1, 0)), 0.0).astype(BF16)
    x_ref[my_rows, :] = dot(own_hidden, w2_ref[...], (1, 0)).astype(BF16)
    pl.semaphore_wait(barrier, n - 1)

    def exchange(src, dst, stage):
        for p in peers:
            pltpu.make_async_remote_copy(
                src_ref=src(p), dst_ref=dst, send_sem=send_sem.at[stage], recv_sem=recv_sem.at[stage],
                device_id={"tp": p}, device_id_type=MESH).start()

    def arrive(others, stage):
        pltpu.make_async_copy(others, others, recv_sem.at[stage]).wait()

    def sent(others, stage):
        pltpu.make_async_copy(others, others, send_sem.at[stage]).wait()

    def rows_of(p):
        return pl.ds(pl.multiple_of(p * own, own), own)

    exchange(lambda p: x_ref.at[my_rows], x_ref.at[my_rows], 1)
    lq_load.wait()
    lab_load.wait()
    for r in range(own):
        lab[pl.ds(me * own + r, 1), :] = jnp.full((1, LANES), labels[r], jnp.int32)
    m_run[...] = jnp.full(m_run.shape, LOWEST, F32)
    s_run[...] = jnp.zeros(s_run.shape, F32)
    part[...] = jnp.zeros(part.shape, F32)
    arrive(x_ref.at[other_rows], 1)

    def logits(i, z_ref):
        for j in range(TILE // DOT_TILE):
            base = pl.multiple_of(i * TILE + j * DOT_TILE, DOT_TILE)
            z = dot(x_ref[...], cat[pl.ds(base, DOT_TILE), :], (1, 1)) - lq[:, pl.ds(base, DOT_TILE)]
            m = m_run[...]
            for c in range(DOT_TILE // LANES):
                zc = z[:, c * LANES:(c + 1) * LANES]
                z_ref[pl.ds(SHIFT + (j * (DOT_TILE // LANES) + c) * rows, rows), :] = zc
                ez[i * chunks + j * (DOT_TILE // LANES) + c] = zc
                m = jnp.maximum(m, zc)
            m_run[...] = m
            yield
        m_hist[i + 1] = m

    def weigh(i, z_ref):
        for r in range(0, rows, GROUP):
            at = slice(r, r + GROUP)
            m = m_hist[i + 1, at, :]
            s = s_run[at, :] * jnp.exp(m_hist[i, at, :] - m)
            for c in range(chunks):
                s = s + jnp.exp(z_ref[pl.ds(SHIFT + c * rows + r, GROUP), :] - m)
            s_run[at, :] = s
            yield

    def arrived(j):
        for k in range(UNROLL * TILE // LOAD_TILE):
            cat_copy(j * (UNROLL * TILE // LOAD_TILE) + k).wait()

    def together(*parts):
        parts = list(parts)
        while parts:
            parts = [p for p in parts if next(p, parts) is not parts]

    z_refs = (z_even, z_odd)

    def step(i, k):
        together(logits(i + 1, z_refs[(k + 1) % 2]), weigh(i, z_refs[k % 2]))

    m_hist[0] = m_run[...]
    arrived(0)
    together(logits(0, z_even))
    exchange(lambda p: lab.at[my_rows], lab.at[my_rows], 0)
    exchange(lambda p: q_ref.at[my_rows], q_ref.at[my_rows], 6)

    def first_pass(j, carry):
        arrived(j + 1)
        for k in range(UNROLL):
            step(j * UNROLL + k, k)
        return carry

    lax.fori_loop(0, tiles // UNROLL - 1, first_pass, 0)
    for k in range(UNROLL - 1):
        step(tiles - UNROLL + k, k)
    together(weigh(tiles - 1, z_odd))

    m_t = m_run[...].T
    m_row = jnp.max(m_t, axis=0, keepdims=True)
    s_row = jnp.sum(s_run[...].T * jnp.exp(m_t - m_row), axis=0, keepdims=True)
    sub = lax.broadcasted_iota(jnp.int32, (8, LANES), 0)
    stats[me] = jnp.where(sub == 0, m_row, s_row)
    exchange(lambda p: stats.at[me], stats.at[me], 2)
    t_run[...] = jnp.zeros(t_run.shape, F32)
    arrive(lab.at[other_rows], 0)
    local = lab[...] - me * items
    lane = lax.broadcasted_iota(jnp.int32, lab.shape, 1)
    d[...] = local - lane
    wide = WEIGHT_TILE // LANES

    def weights(i, carry):
        for r in range(0, rows, WEIGHT_GROUP):
            at = slice(r, r + WEIGHT_GROUP)
            m = m_run[at, :]
            t = t_run[at, :]
            dd = d[at, :] - i * WEIGHT_TILE
            for c in range(wide):
                zc = ez[i * wide + c, at, :]
                t = jnp.where(dd == c * LANES, zc, t)
                ez[i * wide + c, at, :] = jnp.exp(zc - m)
            t_run[at, :] = t
        return carry

    lax.fori_loop(0, items // WEIGHT_TILE, weights, 0)
    t_col = jnp.broadcast_to(jnp.sum(t_run[...], axis=1, keepdims=True), lab.shape)
    targets[me] = t_col.T[0:8, :]
    arrive(stats.at[others], 2)
    big = stats[0, 0:1, :]
    for p in range(1, n):
        big = jnp.maximum(big, stats[p, 0:1, :])
    total = jnp.zeros_like(big)
    for p in range(n):
        total = total + stats[p, 1:2, :] * jnp.exp(stats[p, 0:1, :] - big)
    inv = 1.0 / (total * rows)
    big_col = jnp.broadcast_to(big, (rows, LANES)).T
    inv_col = jnp.broadcast_to(inv, (rows, LANES)).T
    hit_col = (jnp.exp(t_col - big_col) * inv_col - 1.0 / rows).astype(BF16)
    scale = jnp.exp(m_run[...] - big_col) * inv_col
    home = jnp.where(local - local // LANES * LANES == lane, local // LANES, -1)
    home = jnp.where((local >= 0) & (local < items), home, -1).astype(F32)

    def second_pass(i, carry):
        gs = []
        count = SECOND_TILE // LANES
        here = (home - (i * count).astype(F32)).astype(BF16)
        for c in range(count):
            g = (ez[i * count + c] * scale).astype(BF16)
            g = jnp.where(here == jnp.bfloat16(c), hit_col, g)
            g_ref[i * count + c, :rows, :] = g
            gs.append(g)
        base = pl.multiple_of(i * SECOND_TILE, SECOND_TILE)
        part[...] += dot(jnp.concatenate(gs, axis=1), cat[pl.ds(base, SECOND_TILE), :], (1, 0))
        return carry

    lax.fori_loop(0, items // SECOND_TILE, second_pass, 0)

    exchange(lambda p: part.at[rows_of(p)], pieces.at[me], 3)
    pieces[me] = part[my_rows, :]

    def item_grads(i, carry):
        count = OUT_TILE // LANES
        g = jnp.concatenate([g_ref[i * count + c, :rows, :] for c in range(count)], axis=1)
        cat[pl.ds(pl.multiple_of(i * OUT_TILE, OUT_TILE), OUT_TILE), :] = dot(g, x_ref[...], (0, 0)).astype(BF16)
        return carry

    lax.fori_loop(0, EARLY, item_grads, 0)
    exchange(lambda p: targets.at[me], targets.at[me], 5)
    arrive(pieces.at[others], 3)
    acc = pieces[0]
    for p in range(1, n):
        acc = acc + pieces[p]
    dx_ref[my_rows, :] = acc.astype(BF16)
    exchange(lambda p: dx_ref.at[my_rows], dx_ref.at[my_rows], 4)
    lax.fori_loop(EARLY, items // OUT_TILE, item_grads, 0)
    arrive(q_ref.at[other_rows], 6)
    a = dot(q_ref[...], w1[...], (1, 0))
    a_ref[...] = a
    h_ref[...] = jnp.maximum(a, 0.0).astype(BF16)
    arrive(dx_ref.at[other_rows], 4)
    arrive(targets.at[others], 5)
    target = targets[0, 0:1, :]
    for p in range(1, n):
        target = target + targets[p, 0:1, :]
    loss_ref[...] = jnp.broadcast_to(
        jnp.sum(big + jnp.log(total) - target, axis=1, keepdims=True) / rows, loss_ref.shape)
    sent(lab.at[other_rows], 0)
    sent(x_ref.at[other_rows], 1)
    sent(q_ref.at[other_rows], 6)
    sent(stats.at[others], 2)
    sent(pieces.at[others], 3)
    sent(dx_ref.at[other_rows], 4)
    sent(targets.at[others], 5)


def grad_kernel(de_ref, dx_ref, h_ref, a_ref, q_ref, w2_ref, loss_ref,
                loss_hbm, de_hbm, dw1_hbm, dw2_hbm, loss, dw1, dw2, sem):
    copies = []

    def start_copy(k, carry):
        at = pl.ds(pl.multiple_of(k * LOAD_TILE, LOAD_TILE), LOAD_TILE)
        pltpu.make_async_copy(de_ref.at[at], de_hbm.at[at], sem.at[3]).start()
        return carry

    lax.fori_loop(0, de_hbm.shape[0] // LOAD_TILE, start_copy, 0)
    dx = dx_ref[...]
    dw2[...] = dot(h_ref[...], dx, (0, 0)).astype(BF16)
    dh = dot(dx, w2_ref[...], (1, 1))
    da = jnp.where(a_ref[...] > 0.0, dh, 0.0).astype(BF16)
    dw1[...] = dot(q_ref[...], da, (0, 0)).astype(BF16)
    loss[...] = loss_ref[0:1, 0:1]
    copies.append(pltpu.make_async_copy(loss, loss_hbm, sem.at[0]))
    copies.append(pltpu.make_async_copy(dw1, dw1_hbm, sem.at[1]))
    copies.append(pltpu.make_async_copy(dw2, dw2_hbm, sem.at[2]))
    for copy in copies[-3:]:
        copy.start()
    for copy in copies:
        copy.wait()
    pltpu.make_async_copy(de_ref, de_hbm, sem.at[3]).wait()


def solution(mesh):
    n = mesh.shape["tp"]

    def local_step(queries, w_first, w_second, catalogue, log_q, labels):
        own, d_in = queries.shape
        hid, emb = w_second.shape
        items = catalogue.shape[0]
        rows = own * n
        hbm = pl.BlockSpec(memory_space=pl.ANY)
        vmem = pl.BlockSpec(memory_space=pltpu.VMEM)
        dma = pltpu.SemaphoreType.DMA
        held = pl.pallas_call(
            functools.partial(loss_kernel, n),
            name="loss_kernel",
            out_shape=[
                pltpu.VMEM((items, emb), BF16),
                pltpu.VMEM((rows, emb), BF16),
                pltpu.VMEM((rows, hid), BF16),
                pltpu.VMEM((rows, hid), F32),
                pltpu.VMEM((rows, d_in), BF16),
                pltpu.VMEM((hid, emb), BF16),
                pltpu.VMEM((32, LANES), F32),
            ],
            in_specs=[hbm] * 6,
            out_specs=[vmem] * 7,
            scratch_shapes=[
                pltpu.VMEM((rows, emb), BF16),
                pltpu.VMEM((items // LANES, rows + SHIFT, LANES), BF16),
                pltpu.VMEM((items // LANES, rows, LANES), F32),
                pltpu.VMEM((2 * SHIFT + TILE // LANES * rows, LANES), F32),
                pltpu.VMEM((2 * SHIFT + TILE // LANES * rows, LANES), F32),
                pltpu.VMEM((1, items), F32),
                pltpu.VMEM((d_in, hid), BF16),
                pltpu.SMEM((own,), jnp.int32),
                pltpu.VMEM((rows, LANES), jnp.int32),
                pltpu.VMEM((rows, LANES), jnp.int32),
                pltpu.VMEM((rows, LANES), F32),
                pltpu.VMEM((rows, LANES), F32),
                pltpu.VMEM((rows, LANES), F32),
                pltpu.VMEM((items // TILE + 1, rows, LANES), F32),
                pltpu.VMEM((n, 8, LANES), F32),
                pltpu.VMEM((n, 8, LANES), F32),
                pltpu.VMEM((rows, emb), F32),
                pltpu.VMEM((n, own, emb), F32),
                dma((5,)),
                dma((items // LOAD_TILE,)),
                dma((7,)),
                dma((7,)),
            ],
            compiler_params=pltpu.CompilerParams(collective_id=0, has_side_effects=True, vmem_limit_bytes=44 << 20),
        )(queries, w_first, w_second, catalogue, log_q.reshape(1, items), labels)
        loss, grad_items, grad_first, grad_second = pl.pallas_call(
            grad_kernel,
            name="grad_kernel",
            out_shape=[
                jax.ShapeDtypeStruct((1, 1), F32),
                jax.ShapeDtypeStruct((items, emb), BF16),
                jax.ShapeDtypeStruct((d_in, hid), BF16),
                jax.ShapeDtypeStruct((hid, emb), BF16),
            ],
            in_specs=[vmem] * 7,
            out_specs=[hbm] * 4,
            scratch_shapes=[
                pltpu.VMEM((1, 1), F32),
                pltpu.VMEM((d_in, hid), BF16),
                pltpu.VMEM((hid, emb), BF16),
                dma((4,)),
            ],
            compiler_params=pltpu.CompilerParams(vmem_limit_bytes=24 << 20),
        )(*held)
        return loss.reshape(1), grad_items, grad_first, grad_second

    row_spec = P(("dp", "tp"), None)
    return jax.shard_map(
        local_step, mesh=mesh,
        in_specs=(row_spec, P(None, None), P(None, None), P("tp", None), P("tp"), P(("dp", "tp"))),
        out_specs=(P("dp"), row_spec, P("dp", None), P("dp", None)), check_vma=False)
```

```python
import functools

import jax
import jax.numpy as jnp
from jax import lax
from jax.experimental import pallas as pl
from jax.experimental.pallas import tpu as pltpu
from jax.sharding import PartitionSpec as P

F32, BF16 = jnp.float32, jnp.bfloat16
MESH = pl.DeviceIdType.MESH
LANES = 128
TILE = 2048
UNROLL = 4
DOT_TILE = 512
GROUP = 32
WEIGHT_TILE = 4096
WEIGHT_GROUP = 16
SECOND_TILE = 16384
LOAD_TILE = 4096
OUT_TILE = 8192
EARLY = 2
SHIFT = 16
LOWEST = -3.0e38


def dot(a, b, contract):
    return lax.dot_general(a, b, ((contract[:1], contract[1:]), ((), ())), preferred_element_type=F32)


def loss_kernel(n, q_hbm, w1_hbm, w2_hbm, cat_hbm, lq_hbm, lab_hbm,
                cat, dx_ref, h_ref, a_ref, q_ref, w2_ref, loss_ref,
                x_ref, g_ref, ez, z_even, z_odd, lq, w1, labels, lab, d, m_run, s_run, t_run, m_hist, stats, targets, part, pieces,
                load_sem, cat_sem, send_sem, recv_sem):
    me = lax.axis_index("tp")
    own = q_hbm.shape[0]
    rows = own * n
    items = cat_hbm.shape[0]
    tiles = items // TILE
    chunks = TILE // LANES
    my_rows = pl.ds(pl.multiple_of(me * own, own), own)

    others = pl.ds(0, n - 1)
    other_rows = pl.ds(0, rows - own)

    q_load = pltpu.make_async_copy(q_hbm, q_ref.at[my_rows], load_sem.at[0])
    w1_load = pltpu.make_async_copy(w1_hbm, w1, load_sem.at[1])
    w2_load = pltpu.make_async_copy(w2_hbm, w2_ref, load_sem.at[2])
    lq_load = pltpu.make_async_copy(lq_hbm, lq, load_sem.at[3])
    lab_load = pltpu.make_async_copy(lab_hbm, labels, load_sem.at[4])
    for load in (q_load, w1_load, w2_load):
        load.start()
    barrier = pltpu.get_barrier_semaphore()
    peers = [lax.rem(me + k, n) for k in sorted(range(1, n), key=lambda k: -min(k, n - k))]
    for p in peers:
        pl.semaphore_signal(barrier, inc=1, device_id={"tp": p}, device_id_type=MESH)
    for load in (lq_load, lab_load):
        load.start()

    def cat_copy(k):
        part_rows = pl.ds(pl.multiple_of(k * LOAD_TILE, LOAD_TILE), LOAD_TILE)
        return pltpu.make_async_copy(cat_hbm.at[part_rows], cat.at[part_rows], cat_sem.at[k])

    q_load.wait()
    w1_load.wait()
    w2_load.wait()
    for k in range(items // LOAD_TILE):
        cat_copy(k).start()
    own_hidden = jnp.maximum(dot(q_ref[my_rows, :], w1[...], (1, 0)), 0.0).astype(BF16)
    x_ref[my_rows, :] = dot(own_hidden, w2_ref[...], (1, 0)).astype(BF16)
    pl.semaphore_wait(barrier, n - 1)

    def exchange(src, dst, stage):
        for p in peers:
            pltpu.make_async_remote_copy(
                src_ref=src(p), dst_ref=dst, send_sem=send_sem.at[stage], recv_sem=recv_sem.at[stage],
                device_id={"tp": p}, device_id_type=MESH).start()

    def arrive(others, stage):
        pltpu.make_async_copy(others, others, recv_sem.at[stage]).wait()

    def sent(others, stage):
        pltpu.make_async_copy(others, others, send_sem.at[stage]).wait()

    def rows_of(p):
        return pl.ds(pl.multiple_of(p * own, own), own)

    exchange(lambda p: x_ref.at[my_rows], x_ref.at[my_rows], 1)
    lq_load.wait()
    lab_load.wait()
    for r in range(own):
        lab[pl.ds(me * own + r, 1), :] = jnp.full((1, LANES), labels[r], jnp.int32)
    m_run[...] = jnp.full(m_run.shape, LOWEST, F32)
    s_run[...] = jnp.zeros(s_run.shape, F32)
    part[...] = jnp.zeros(part.shape, F32)
    arrive(x_ref.at[other_rows], 1)

    def logits(i, z_ref):
        for j in range(TILE // DOT_TILE):
            base = pl.multiple_of(i * TILE + j * DOT_TILE, DOT_TILE)
            z = dot(x_ref[...], cat[pl.ds(base, DOT_TILE), :], (1, 1)) - lq[:, pl.ds(base, DOT_TILE)]
            m = m_run[...]
            for c in range(DOT_TILE // LANES):
                zc = z[:, c * LANES:(c + 1) * LANES]
                z_ref[pl.ds(SHIFT + (j * (DOT_TILE // LANES) + c) * rows, rows), :] = zc
                ez[i * chunks + j * (DOT_TILE // LANES) + c] = zc
                m = jnp.maximum(m, zc)
            m_run[...] = m
            yield
        m_hist[i + 1] = m

    def weigh(i, z_ref):
        for r in range(0, rows, GROUP):
            at = slice(r, r + GROUP)
            m = m_hist[i + 1, at, :]
            s = s_run[at, :] * jnp.exp(m_hist[i, at, :] - m)
            for c in range(chunks):
                s = s + jnp.exp(z_ref[pl.ds(SHIFT + c * rows + r, GROUP), :] - m)
            s_run[at, :] = s
            yield

    def arrived(j):
        for k in range(UNROLL * TILE // LOAD_TILE):
            cat_copy(j * (UNROLL * TILE // LOAD_TILE) + k).wait()

    def together(*parts):
        parts = list(parts)
        while parts:
            parts = [p for p in parts if next(p, parts) is not parts]

    z_refs = (z_even, z_odd)

    def step(i, k):
        together(logits(i + 1, z_refs[(k + 1) % 2]), weigh(i, z_refs[k % 2]))

    m_hist[0] = m_run[...]
    arrived(0)
    together(logits(0, z_even))
    exchange(lambda p: lab.at[my_rows], lab.at[my_rows], 0)
    exchange(lambda p: q_ref.at[my_rows], q_ref.at[my_rows], 6)

    def first_pass(j, carry):
        arrived(j + 1)
        for k in range(UNROLL):
            step(j * UNROLL + k, k)
        return carry

    lax.fori_loop(0, tiles // UNROLL - 1, first_pass, 0)
    for k in range(UNROLL - 1):
        step(tiles - UNROLL + k, k)
    together(weigh(tiles - 1, z_odd))

    m_t = m_run[...].T
    m_row = jnp.max(m_t, axis=0, keepdims=True)
    s_row = jnp.sum(s_run[...].T * jnp.exp(m_t - m_row), axis=0, keepdims=True)
    sub = lax.broadcasted_iota(jnp.int32, (8, LANES), 0)
    stats[me] = jnp.where(sub == 0, m_row, s_row)
    exchange(lambda p: stats.at[me], stats.at[me], 2)
    t_run[...] = jnp.zeros(t_run.shape, F32)
    arrive(lab.at[other_rows], 0)
    local = lab[...] - me * items
    lane = lax.broadcasted_iota(jnp.int32, lab.shape, 1)
    d[...] = local - lane
    wide = WEIGHT_TILE // LANES

    def weights(i, carry):
        for r in range(0, rows, WEIGHT_GROUP):
            at = slice(r, r + WEIGHT_GROUP)
            m = m_run[at, :]
            t = t_run[at, :]
            dd = d[at, :] - i * WEIGHT_TILE
            for c in range(wide):
                zc = ez[i * wide + c, at, :]
                t = jnp.where(dd == c * LANES, zc, t)
                ez[i * wide + c, at, :] = jnp.exp(zc - m)
            t_run[at, :] = t
        return carry

    lax.fori_loop(0, items // WEIGHT_TILE, weights, 0)
    t_col = jnp.broadcast_to(jnp.sum(t_run[...], axis=1, keepdims=True), lab.shape)
    targets[me] = t_col.T[0:8, :]
    arrive(stats.at[others], 2)
    big = stats[0, 0:1, :]
    for p in range(1, n):
        big = jnp.maximum(big, stats[p, 0:1, :])
    total = jnp.zeros_like(big)
    for p in range(n):
        total = total + stats[p, 1:2, :] * jnp.exp(stats[p, 0:1, :] - big)
    inv = 1.0 / (total * rows)
    big_col = jnp.broadcast_to(big, (rows, LANES)).T
    inv_col = jnp.broadcast_to(inv, (rows, LANES)).T
    hit_col = (jnp.exp(t_col - big_col) * inv_col - 1.0 / rows).astype(BF16)
    scale = jnp.exp(m_run[...] - big_col) * inv_col
    home = jnp.where(local - local // LANES * LANES == lane, local // LANES, -1)
    home = jnp.where((local >= 0) & (local < items), home, -1).astype(F32)

    def second_pass(i, carry):
        gs = []
        count = SECOND_TILE // LANES
        here = (home - (i * count).astype(F32)).astype(BF16)
        for c in range(count):
            g = (ez[i * count + c] * scale).astype(BF16)
            g = jnp.where(here == jnp.bfloat16(c), hit_col, g)
            g_ref[i * count + c, :rows, :] = g
            gs.append(g)
        base = pl.multiple_of(i * SECOND_TILE, SECOND_TILE)
        part[...] += dot(jnp.concatenate(gs, axis=1), cat[pl.ds(base, SECOND_TILE), :], (1, 0))
        return carry

    lax.fori_loop(0, items // SECOND_TILE, second_pass, 0)

    exchange(lambda p: part.at[rows_of(p)], pieces.at[me], 3)
    pieces[me] = part[my_rows, :]

    def item_grads(i, carry):
        count = OUT_TILE // LANES
        g = jnp.concatenate([g_ref[i * count + c, :rows, :] for c in range(count)], axis=1)
        cat[pl.ds(pl.multiple_of(i * OUT_TILE, OUT_TILE), OUT_TILE), :] = dot(g, x_ref[...], (0, 0)).astype(BF16)
        return carry

    lax.fori_loop(0, EARLY, item_grads, 0)
    exchange(lambda p: targets.at[me], targets.at[me], 5)
    arrive(pieces.at[others], 3)
    acc = pieces[0]
    for p in range(1, n):
        acc = acc + pieces[p]
    dx_ref[my_rows, :] = acc.astype(BF16)
    exchange(lambda p: dx_ref.at[my_rows], dx_ref.at[my_rows], 4)
    lax.fori_loop(EARLY, items // OUT_TILE, item_grads, 0)
    arrive(q_ref.at[other_rows], 6)
    a = dot(q_ref[...], w1[...], (1, 0))
    a_ref[...] = a
    h_ref[...] = jnp.maximum(a, 0.0).astype(BF16)
    arrive(dx_ref.at[other_rows], 4)
    arrive(targets.at[others], 5)
    target = targets[0, 0:1, :]
    for p in range(1, n):
        target = target + targets[p, 0:1, :]
    loss_ref[...] = jnp.broadcast_to(
        jnp.sum(big + jnp.log(total) - target, axis=1, keepdims=True) / rows, loss_ref.shape)
    sent(lab.at[other_rows], 0)
    sent(x_ref.at[other_rows], 1)
    sent(q_ref.at[other_rows], 6)
    sent(stats.at[others], 2)
    sent(pieces.at[others], 3)
    sent(dx_ref.at[other_rows], 4)
    sent(targets.at[others], 5)


def grad_kernel(de_ref, dx_ref, h_ref, a_ref, q_ref, w2_ref, loss_ref,
                loss_hbm, de_hbm, dw1_hbm, dw2_hbm, loss, dw1, dw2, sem):
    copies = []

    def start_copy(k, carry):
        at = pl.ds(pl.multiple_of(k * LOAD_TILE, LOAD_TILE), LOAD_TILE)
        pltpu.make_async_copy(de_ref.at[at], de_hbm.at[at], sem.at[3]).start()
        return carry

    lax.fori_loop(0, de_hbm.shape[0] // LOAD_TILE, start_copy, 0)
    dx = dx_ref[...]
    dw2[...] = dot(h_ref[...], dx, (0, 0)).astype(BF16)
    dh = dot(dx, w2_ref[...], (1, 1))
    da = jnp.where(a_ref[...] > 0.0, dh, 0.0).astype(BF16)
    dw1[...] = dot(q_ref[...], da, (0, 0)).astype(BF16)
    loss[...] = loss_ref[0:1, 0:1]
    copies.append(pltpu.make_async_copy(loss, loss_hbm, sem.at[0]))
    copies.append(pltpu.make_async_copy(dw1, dw1_hbm, sem.at[1]))
    copies.append(pltpu.make_async_copy(dw2, dw2_hbm, sem.at[2]))
    for copy in copies[-3:]:
        copy.start()
    for copy in copies:
        copy.wait()
    pltpu.make_async_copy(de_ref, de_hbm, sem.at[3]).wait()


def solution(mesh):
    n = mesh.shape["tp"]

    def local_step(queries, w_first, w_second, catalogue, log_q, labels):
        own, d_in = queries.shape
        hid, emb = w_second.shape
        items = catalogue.shape[0]
        rows = own * n
        hbm = pl.BlockSpec(memory_space=pl.ANY)
        vmem = pl.BlockSpec(memory_space=pltpu.VMEM)
        dma = pltpu.SemaphoreType.DMA
        held = pl.pallas_call(
            functools.partial(loss_kernel, n),
            name="loss_kernel",
            out_shape=[
                pltpu.VMEM((items, emb), BF16),
                pltpu.VMEM((rows, emb), BF16),
                pltpu.VMEM((rows, hid), BF16),
                pltpu.VMEM((rows, hid), F32),
                pltpu.VMEM((rows, d_in), BF16),
                pltpu.VMEM((hid, emb), BF16),
                pltpu.VMEM((32, LANES), F32),
            ],
            in_specs=[hbm] * 6,
            out_specs=[vmem] * 7,
            scratch_shapes=[
                pltpu.VMEM((rows, emb), BF16),
                pltpu.VMEM((items // LANES, rows + SHIFT, LANES), BF16),
                pltpu.VMEM((items // LANES, rows, LANES), F32),
                pltpu.VMEM((2 * SHIFT + TILE // LANES * rows, LANES), F32),
                pltpu.VMEM((2 * SHIFT + TILE // LANES * rows, LANES), F32),
                pltpu.VMEM((1, items), F32),
                pltpu.VMEM((d_in, hid), BF16),
                pltpu.SMEM((own,), jnp.int32),
                pltpu.VMEM((rows, LANES), jnp.int32),
                pltpu.VMEM((rows, LANES), jnp.int32),
                pltpu.VMEM((rows, LANES), F32),
                pltpu.VMEM((rows, LANES), F32),
                pltpu.VMEM((rows, LANES), F32),
                pltpu.VMEM((items // TILE + 1, rows, LANES), F32),
                pltpu.VMEM((n, 8, LANES), F32),
                pltpu.VMEM((n, 8, LANES), F32),
                pltpu.VMEM((rows, emb), F32),
                pltpu.VMEM((n, own, emb), F32),
                dma((5,)),
                dma((items // LOAD_TILE,)),
                dma((7,)),
                dma((7,)),
            ],
            compiler_params=pltpu.CompilerParams(collective_id=0, has_side_effects=True, vmem_limit_bytes=44 << 20),
        )(queries, w_first, w_second, catalogue, log_q.reshape(1, items), labels)
        loss, grad_items, grad_first, grad_second = pl.pallas_call(
            grad_kernel,
            name="grad_kernel",
            out_shape=[
                jax.ShapeDtypeStruct((1, 1), F32),
                jax.ShapeDtypeStruct((items, emb), BF16),
                jax.ShapeDtypeStruct((d_in, hid), BF16),
                jax.ShapeDtypeStruct((hid, emb), BF16),
            ],
            in_specs=[vmem] * 7,
            out_specs=[hbm] * 4,
            scratch_shapes=[
                pltpu.VMEM((1, 1), F32),
                pltpu.VMEM((d_in, hid), BF16),
                pltpu.VMEM((hid, emb), BF16),
                dma((4,)),
            ],
            compiler_params=pltpu.CompilerParams(vmem_limit_bytes=24 << 20),
        )(*held)
        return loss.reshape(1), grad_items, grad_first, grad_second

    row_spec = P(("dp", "tp"), None)
    return jax.shard_map(
        local_step, mesh=mesh,
        in_specs=(row_spec, P(None, None), P(None, None), P("tp", None), P("tp"), P(("dp", "tp"))),
        out_specs=(P("dp"), row_spec, P("dp", None), P("dp", None)), check_vma=False)
```
